8 devices in a mesh: replica: 2 (over z, y), model: 4 (over x, core).
Axes of the slice: x: 2, y: 2, z: 1, core: 2. Of those that a mesh axis runs over, the one named last changes fastest.
Arguments:
- x: bfloat16 [128, 8192], P('replica'), parts along dimension 0
- cache_len: int32 [128], P('replica'), parts along dimension 0
- w_query: bfloat16 [2, 8192, 8192], P(None, None, 'model')
- w_key: bfloat16 [2, 8192, 128], replicated
- w_value: bfloat16 [2, 8192, 128], replicated
- w_out: bfloat16 [2, 8192, 8192], P(None, 'model')
- k_cache: bfloat16 [2, 128, 2048, 128], P(None, ('replica', 'model')), parts along dimension 1
- v_cache: bfloat16 [2, 128, 2048, 128], P(None, ('replica', 'model')), parts along dimension 1
Outputs:
- output 1: bfloat16 [128, 8192], P('replica'), parts along dimension 0
- output 2: bfloat16 [2, 128, 2048, 128], P(None, ('replica', 'model')), parts along dimension 1
- output 3: bfloat16 [2, 128, 2048, 128], P(None, ('replica', 'model')), parts along dimension 1
There are 2 independent parts. The reference program is written for one: setup_inputs(seed, part) draws one part's arguments, and reference() takes and returns one part's arrays. A program takes and returns all parts, laid end to end along the dimension named above; an argument that names none is the same for every part.
All inputs are finite; a program needn't handle non-finite values.
Results may differ from the reference program's by a relative error of at most 0.00572.
Values are sent between devices in bfloat16 or wider.
A program may use at most 1 GiB of HBM per device.

```python
import jax
import jax.numpy as jnp
from jax import lax

LAYERS = 2
BATCH = 64
D_MODEL = 8192
NUM_HEADS = 64
HEAD_DIM = 128
SEQ_LEN = 2048

SEQ_BITS = SEQ_LEN.bit_length() - 1
Q_WIDTH = NUM_HEADS * HEAD_DIM


def setup_inputs(seed: int = 0, part: int = 0) -> dict:
    root_key = jax.random.key(seed)
    shared = jax.random.split(root_key, 4)
    part_keys = jax.random.split(jax.random.fold_in(root_key, part), 6)
    x = jax.random.normal(part_keys[0], (BATCH, D_MODEL), jnp.float32).astype(jnp.bfloat16)
    raw_len = jax.random.randint(part_keys[1], (BATCH,), 0, SEQ_LEN)
    shift_by = jax.random.randint(part_keys[2], (BATCH,), 0, SEQ_BITS + 1)
    row_order = jax.random.permutation(part_keys[3], BATCH)
    cache_len = jnp.right_shift(raw_len, shift_by)
    cache_len = cache_len.at[row_order[0]].set(SEQ_LEN - 1).at[row_order[1]].set(0)
    w_query = (1.5 * D_MODEL ** -0.5) * jax.random.normal(shared[0], (LAYERS, D_MODEL, Q_WIDTH), jnp.float32)
    w_key = (1.5 * D_MODEL ** -0.5) * jax.random.normal(shared[1], (LAYERS, D_MODEL, HEAD_DIM), jnp.float32)
    w_value = (D_MODEL ** -0.5) * jax.random.normal(shared[2], (LAYERS, D_MODEL, HEAD_DIM), jnp.float32)
    w_out = (2.0 * Q_WIDTH ** -0.5) * jax.random.normal(shared[3], (LAYERS, Q_WIDTH, D_MODEL), jnp.float32)
    k_cache = 1.5 * jax.random.normal(part_keys[4], (LAYERS, BATCH, SEQ_LEN, HEAD_DIM), jnp.float32)
    v_cache = jax.random.normal(part_keys[5], (LAYERS, BATCH, SEQ_LEN, HEAD_DIM), jnp.float32)
    return {
        "x": x,
        "cache_len": cache_len,
        "w_query": w_query.astype(jnp.bfloat16),
        "w_key": w_key.astype(jnp.bfloat16),
        "w_value": w_value.astype(jnp.bfloat16),
        "w_out": w_out.astype(jnp.bfloat16),
        "k_cache": k_cache.astype(jnp.bfloat16),
        "v_cache": v_cache.astype(jnp.bfloat16),
    }


def attend_layer(hidden, cache_len, query_w, key_w, value_w, out_w, k_layer, v_layer):
    query = jnp.dot(hidden, query_w, preferred_element_type=jnp.float32).astype(jnp.bfloat16)
    query = query.reshape(BATCH, NUM_HEADS, HEAD_DIM)
    k_new = jnp.dot(hidden, key_w, preferred_element_type=jnp.float32).astype(jnp.bfloat16)
    v_new = jnp.dot(hidden, value_w, preferred_element_type=jnp.float32).astype(jnp.bfloat16)
    write_here = jnp.arange(SEQ_LEN)[None, :, None] == cache_len[:, None, None]
    k_layer = jnp.where(write_here, k_new[:, None, :], k_layer)
    v_layer = jnp.where(write_here, v_new[:, None, :], v_layer)

    def one_row(row_items):
        q_row, k_row, v_row, row_len = row_items
        scores = jnp.dot(q_row, k_row.T, preferred_element_type=jnp.float32) * (HEAD_DIM ** -0.5)
        visible = jnp.arange(SEQ_LEN)[None, :] <= row_len
        scores = jnp.where(visible, scores, -jnp.inf)
        weights = jax.nn.softmax(scores, axis=-1).astype(jnp.bfloat16)
        context = jnp.dot(weights, v_row, preferred_element_type=jnp.float32)
        return context.astype(jnp.bfloat16)

    context = lax.map(one_row, (query, k_layer, v_layer, cache_len))
    update = jnp.dot(context.reshape(BATCH, Q_WIDTH), out_w, preferred_element_type=jnp.float32)
    hidden = (hidden.astype(jnp.float32) + update).astype(jnp.bfloat16)
    return hidden, k_layer, v_layer


def reference(x, cache_len, w_query, w_key, w_value, w_out, k_cache, v_cache):
    def layer_step(hidden, params):
        query_w, key_w, value_w, out_w, k_layer, v_layer = params
        hidden, k_layer, v_layer = attend_layer(hidden, cache_len, query_w, key_w, value_w, out_w, k_layer, v_layer)
        return hidden, (k_layer, v_layer)

    out, (k_all, v_all) = lax.scan(layer_step, x, (w_query, w_key, w_value, w_out, k_cache, v_cache))
    return out, k_all, v_all
```

```python
import functools

import jax
import jax.numpy as jnp
from jax import lax
from jax.experimental import pallas as pl
from jax.experimental.pallas import tpu as pltpu
from jax.sharding import PartitionSpec as P

F32 = jnp.float32
BF16 = jnp.bfloat16
MIB = 1 << 20

GROUPS = 4
ROWS = 64
MINE = 16
D = 8192
HD = 128
LH = 16
QW = LH * HD
SEQ = 2048
CH = 512
NJ = QW // CH
QKV = QW + 2 * HD
WO_SLOTS = 8
BLK = 256
VM = pltpu.VMEM
VSPEC = pl.BlockSpec(memory_space=pltpu.VMEM)
ASPEC = pl.BlockSpec(memory_space=pl.ANY)
SSPEC = pl.BlockSpec(memory_space=pltpu.SMEM)


def sds(shape, dtype=BF16):
    return jax.ShapeDtypeStruct(shape, dtype)


def qkv_copies(layer, chunk, slot, wq, wk, wv, buf, sems):
    rows = pl.ds(pl.multiple_of(chunk * CH, CH), CH)
    return (
        pltpu.make_async_copy(wq.at[layer, rows, :], buf.at[slot, :, pl.ds(0, QW)], sems.at[0, slot]),
        pltpu.make_async_copy(wk.at[layer, rows, :], buf.at[slot, :, pl.ds(QW, HD)], sems.at[1, slot]),
        pltpu.make_async_copy(wv.at[layer, rows, :], buf.at[slot, :, pl.ds(QW + HD, HD)], sems.at[2, slot]),
    )


def write_qkv(me, acc, q_outs, k_new, v_new):
    for i, q_out in enumerate(q_outs):
        other = xor_id(me, i)
        q_out[...] = acc[pl.ds(pl.multiple_of(other * MINE, MINE), MINE), 0:QW].astype(BF16)
    mine = pl.ds(pl.multiple_of(me * MINE, MINE), MINE)
    k_new[...] = acc[mine, QW:QW + HD].astype(BF16)
    v_new[...] = acc[mine, QW + HD:QKV].astype(BF16)


def xor_id(me, i):
    core = lax.rem(me, 2)
    other = me
    if i & 1:
        other = other + 1 - 2 * core
    if i & 2:
        other = lax.rem(other + 2, GROUPS)
    return other


def first_qkv_kernel(x, wq, wk, wv, q0, q1, q2, q3, k_new, v_new, buf, acc, sems):
    me = lax.axis_index("model")
    chunks = D // CH

    def start(c, _):
        for cp in qkv_copies(0, c, c, wq, wk, wv, buf, sems):
            cp.start()
        return 0

    lax.fori_loop(0, chunks, start, 0)
    acc[...] = jnp.zeros_like(acc)

    def step(c, _):
        for cp in qkv_copies(0, c, c, wq, wk, wv, buf, sems):
            cp.wait()
        cols = pl.ds(pl.multiple_of(c * CH, CH), CH)
        acc[...] += jnp.dot(x[:, cols], buf[c], preferred_element_type=F32)
        return 0

    lax.fori_loop(0, chunks, step, 0)
    write_qkv(me, acc, (q0, q1, q2, q3), k_new, v_new)


def first_qkv(x, wq, wk, wv):
    n = D // CH
    return pl.pallas_call(
        first_qkv_kernel,
        out_shape=[sds((MINE, QW))] * 4 + [sds((MINE, HD))] * 2,
        in_specs=[VSPEC, ASPEC, ASPEC, ASPEC],
        out_specs=[VSPEC] * 6,
        scratch_shapes=[
            VM((n, CH, QKV), BF16),
            VM((ROWS, QKV), F32),
            pltpu.SemaphoreType.DMA((3, n)),
        ],
        compiler_params=pltpu.CompilerParams(vmem_limit_bytes=50 * MIB),
        cost_estimate=pl.CostEstimate(flops=2 * ROWS * D * QKV, bytes_accessed=2 * D * QKV, transcendentals=0),
        name="first_qkv",
    )(x, wq, wk, wv)


def put_row(buf, b, length, row):
    base = pl.multiple_of((length // 16) * 16, 16)
    here = lax.broadcasted_iota(jnp.int32, (16, HD), 0) == length - base
    buf[b, pl.ds(base, 16), :] = jnp.where(here, row, buf[b, pl.ds(base, 16), :])


def copy_kernel(layer, n_in, *refs):
    lens, new, src = refs[:3]
    dst, buf, in_sems, out_sems = refs[n_in:]
    me = lax.axis_index("model")

    def take(b):
        return pltpu.make_async_copy(src.at[layer, b], buf.at[b], in_sems.at[b])

    def give(b):
        return pltpu.make_async_copy(buf.at[b], dst.at[layer, b], out_sems.at[b])

    for b in range(MINE):
        take(b).start()
    for b in range(MINE):
        take(b).wait()
        put_row(buf, b, lens[me * MINE + b], new[pl.ds(b, 1), :])
        if b:
            give(b - 1).start()
    give(MINE - 1).start()
    for b in range(MINE):
        give(b).wait()


def copy_cache(layer, lens, new, src, prior):
    args = [lens, new, src] + ([prior] if prior is not None else [])
    return pl.pallas_call(
        functools.partial(copy_kernel, layer, len(args)),
        out_shape=sds(src.shape),
        in_specs=[SSPEC, VSPEC, ASPEC] + ([ASPEC] if prior is not None else []),
        out_specs=ASPEC,
        input_output_aliases={3: 0} if prior is not None else {},
        scratch_shapes=[
            VM((MINE, SEQ, HD), BF16),
            pltpu.SemaphoreType.DMA((MINE,)),
            pltpu.SemaphoreType.DMA((MINE,)),
        ],
        compiler_params=pltpu.CompilerParams(vmem_limit_bytes=16 * MIB),
        cost_estimate=pl.CostEstimate(flops=5_000_000_000, bytes_accessed=4 * MINE * SEQ * HD, transcendentals=0),
        name=f"copy_cache_{layer}",
    )(*args)


GRP = 4


def attend_kernel(layer, lens, r0, r1, r2, r3, k_new, v_new, k_cache, v_cache, c0, c1, c2, c3,
                  kbuf, vbuf, qbuf, sbuf, cbuf, ksems, vsems):
    me = lax.axis_index("model")
    length = [lens[me * MINE + b] for b in range(MINE)]
    n_groups = MINE // GRP
    n_blocks = []
    for g in range(n_groups):
        longest = length[g * GRP]
        for b in range(g * GRP + 1, (g + 1) * GRP):
            longest = jnp.maximum(longest, length[b])
        n_blocks.append(longest // BLK + 1)

    def block(t):
        return pl.ds(pl.multiple_of(t * BLK, BLK), BLK)

    def k_copy(b, t):
        return pltpu.make_async_copy(k_cache.at[layer, b, block(t), :], kbuf.at[b, block(t), :], ksems.at[b, t])

    def v_copy(b, t):
        return pltpu.make_async_copy(v_cache.at[layer, b, block(t), :], vbuf.at[b, block(t), :], vsems.at[b, t])

    for g in range(n_groups):
        def start(t, _, g=g):
            for b in range(g * GRP, (g + 1) * GRP):
                k_copy(b, t).start()
            for b in range(g * GRP, (g + 1) * GRP):
                v_copy(b, t).start()
            return 0
        lax.fori_loop(0, n_blocks[g], start, 0)

    for i, r in enumerate((r0, r1, r2, r3)):
        for h in range(LH):
            qbuf[:, i * LH + h, :] = r[:, h * HD:(h + 1) * HD].astype(F32)

    n_heads = 4 * LH
    scale = HD ** -0.5
    for g in range(n_groups):
        seqs = range(g * GRP, (g + 1) * GRP)
        nb = n_blocks[g]

        def wait_k(t, _, seqs=seqs):
            for b in seqs:
                k_copy(b, t).wait()
            return 0
        lax.fori_loop(0, nb, wait_k, 0)
        for b in seqs:
            put_row(kbuf, b, length[b], k_new[pl.ds(b, 1), :])

        def score(t, tops, seqs=seqs):
            out = []
            for n, b in enumerate(seqs):
                s = lax.dot_general(qbuf[b].astype(BF16), kbuf[b, block(t), :], (((1,), (1,)), ((), ())),
                                    preferred_element_type=F32) * scale
                pos = lax.broadcasted_iota(jnp.int32, (n_heads, BLK), 1) + t * BLK
                s = jnp.where(pos <= length[b], s, -jnp.inf)
                sbuf[n, :, block(t)] = s
                top = tops[n]
                for i in range(BLK // HD):
                    top = jnp.maximum(top, s[:, i * HD:(i + 1) * HD])
                out.append(top)
            return tuple(out)

        tops = lax.fori_loop(0, nb, score, tuple(jnp.full((n_heads, HD), -jnp.inf, F32) for _ in seqs))
        tops = [jnp.max(t, axis=1, keepdims=True) for t in tops]

        def expo(t, sums, tops=tops, seqs=seqs):
            out = []
            for n, b in enumerate(seqs):
                e = jnp.exp(sbuf[n, :, block(t)] - tops[n])
                sbuf[n, :, block(t)] = e
                total = sums[n]
                for i in range(BLK // HD):
                    total = total + e[:, i * HD:(i + 1) * HD]
                out.append(total)
            return tuple(out)

        sums = lax.fori_loop(0, nb, expo, tuple(jnp.zeros((n_heads, HD), F32) for _ in seqs))
        invs = [1.0 / jnp.sum(s, axis=1, keepdims=True) for s in sums]

        def wait_v(t, _, seqs=seqs):
            for b in seqs:
                v_copy(b, t).wait()
            return 0
        lax.fori_loop(0, nb, wait_v, 0)
        for b in seqs:
            put_row(vbuf, b, length[b], v_new[pl.ds(b, 1), :])

        def mix(t, accs, invs=invs, seqs=seqs):
            out = []
            for n, b in enumerate(seqs):
                p = (sbuf[n, :, block(t)] * invs[n]).astype(BF16)
                out.append(accs[n] + jnp.dot(p, vbuf[b, block(t), :], preferred_element_type=F32))
            return tuple(out)

        accs = lax.fori_loop(0, nb, mix, tuple(jnp.zeros((n_heads, HD), F32) for _ in seqs))
        for n, b in enumerate(seqs):
            cbuf[b] = accs[n]

    for i, c in enumerate((c0, c1, c2, c3)):
        for h in range(LH):
            c[:, h * HD:(h + 1) * HD] = cbuf[:, i * LH + h, :].astype(BF16)


def attend(layer, lens, rs, k_new, v_new, k_cache, v_cache):
    nt = SEQ // BLK
    return pl.pallas_call(
        functools.partial(attend_kernel, layer),
        out_shape=[sds((MINE, QW))] * 4,
        in_specs=[SSPEC] + [VSPEC] * 6 + [ASPEC] * 2,
        out_specs=[VSPEC] * 4,
        scratch_shapes=[
            VM((MINE, SEQ, HD), BF16),
            VM((MINE, SEQ, HD), BF16),
            VM((MINE, 4 * LH, HD), F32),
            VM((GRP, 4 * LH, SEQ), F32),
            VM((MINE, 4 * LH, HD), F32),
            pltpu.SemaphoreType.DMA((MINE, nt)),
            pltpu.SemaphoreType.DMA((MINE, nt)),
        ],
        compiler_params=pltpu.CompilerParams(vmem_limit_bytes=32 * MIB),
        cost_estimate=pl.CostEstimate(flops=5_000_000_000, bytes_accessed=8 * MIB, transcendentals=0),
        name=f"attend_{layer}",
    )(lens, *rs, k_new, v_new, k_cache, v_cache)


def out_kernel(layer, fuse, *refs):
    d_refs, (res, wo), refs = refs[:4], refs[4:6], refs[6:]
    if fuse:
        (wq, wk, wv), outs, refs = refs[:3], refs[3:10], refs[10:]
        q_outs, (k_new, v_new, res_out) = outs[:4], outs[4:]
        hid, qbuf, acc, q_sems = refs[:4]
        refs = refs[4:]
    else:
        hid, refs = refs[0], refs[1:]
    ctx, resv, wbuf, send_a, recv_a, send_c, recv_c, send_b, recv_b, own, w_sems, res_sem, ssems, rsems = refs

    me = lax.axis_index("model")
    partner, cross, diag = xor_id(me, 1), xor_id(me, 2), xor_id(me, 3)

    def cols(chunk):
        return pl.ds(pl.multiple_of(chunk * CH, CH), CH)

    def wo_copy(chunk, slot):
        return pltpu.make_async_copy(wo.at[layer, :, cols(chunk)], wbuf.at[slot], w_sems.at[slot])

    def q_copies(chunk, slot):
        return qkv_copies(layer + 1, chunk, slot, wq, wk, wv, qbuf, q_sems)

    def send(kind, j, src, dst, dev):
        return pltpu.make_async_remote_copy(
            src_ref=src, dst_ref=dst, send_sem=ssems.at[kind, j], recv_sem=rsems.at[kind, j],
            device_id={"model": dev}, device_id_type=pl.DeviceIdType.MESH)

    def pair_a(j):
        return send(0, j, send_a.at[j], recv_a.at[j], partner)

    def pair_b(j):
        return send(1, j, send_b.at[j], recv_b.at[j], partner)

    def across(j):
        return send(2, j, send_c.at[j], recv_c.at[j], cross)

    def hidden(kind, j, owner, dev):
        part = hid.at[:, cols(owner * NJ + j)]
        return send(kind, j, part, part, dev)

    for j in range(NJ):
        wo_copy(diag * NJ + j, 2 * j).start()
        wo_copy(cross * NJ + j, 2 * j + 1).start()
    if fuse:
        res_copy = pltpu.make_async_copy(
            res.at[:, pl.ds(pl.multiple_of(me * QW, QW), QW)], resv, res_sem)
    else:
        res_copy = pltpu.make_async_copy(res, resv, res_sem)
    res_copy.start()

    for i, d in enumerate(d_refs):
        ctx[pl.ds(pl.multiple_of(xor_id(me, i) * MINE, MINE), MINE), :] = d[...]
    if fuse:
        acc[...] = jnp.zeros_like(acc)

    barrier = pltpu.get_barrier_semaphore()
    for dev in (partner, cross):
        pl.semaphore_signal(barrier, inc=1, device_id={"model": dev}, device_id_type=pl.DeviceIdType.MESH)
    pl.semaphore_wait(barrier, 2)

    def part_sum(slot):
        return jnp.dot(ctx[...], wbuf[slot], preferred_element_type=F32)

    def phase_a(j, _):
        wo_copy(diag * NJ + j, 2 * j).wait()
        send_a[j] = part_sum(2 * j)
        pair_a(j).start()
        wo_copy(partner * NJ + j, 2 * j).start()
        wo_copy(cross * NJ + j, 2 * j + 1).wait()
        part = part_sum(2 * j + 1)
        wo_copy(me * NJ + j, 2 * j + 1).start()
        pair_a(j).wait_recv()
        send_c[j] = part + recv_a[j]
        across(j).start()
        return 0

    lax.fori_loop(0, NJ, phase_a, 0)

    def phase_b(j, _):
        if fuse:
            for i, owner in enumerate((me, partner)):
                for cp in q_copies(owner * NJ + j, 2 * j + i):
                    cp.start()
            for i, owner in enumerate((cross, diag)):
                for cp in q_copies(owner * NJ + j, 2 * NJ + 2 * j + i):
                    cp.start()
        wo_copy(partner * NJ + j, 2 * j).wait()
        send_b[j] = part_sum(2 * j)
        pair_b(j).start()
        wo_copy(me * NJ + j, 2 * j + 1).wait()
        part = part_sum(2 * j + 1)
        pair_b(j).wait_recv()
        own[j] = part + recv_b[j]
        return 0

    lax.fori_loop(0, NJ, phase_b, 0)
    res_copy.wait()

    def next_q(owner, j, slot):
        chunk = owner * NJ + j
        for cp in q_copies(chunk, slot):
            cp.wait()
        acc[...] += jnp.dot(hid[:, cols(chunk)], qbuf[slot], preferred_element_type=F32)

    def phase_c(j, _):
        across(j).wait_recv()
        total = own[j] + recv_c[j]
        part = (resv[:, cols(j)].astype(F32) + total).astype(BF16)
        hid[:, cols(me * NJ + j)] = part
        if fuse:
            res_out[:, cols(j)] = part
        hidden(4, j, me, cross).start()
        hidden(3, j, me, partner).start()
        if fuse:
            next_q(me, j, 2 * j)
        hidden(3, j, partner, partner).wait_recv()
        if fuse:
            next_q(partner, j, 2 * j + 1)
        return 0

    lax.fori_loop(0, NJ, phase_c, 0)

    def phase_d(j, _):
        hidden(4, j, cross, cross).wait_recv()
        hidden(5, j, cross, partner).start()
        if fuse:
            next_q(cross, j, 2 * NJ + 2 * j)
        hidden(5, j, diag, partner).wait_recv()
        if fuse:
            next_q(diag, j, 2 * NJ + 2 * j + 1)
        return 0

    lax.fori_loop(0, NJ, phase_d, 0)

    if fuse:
        write_qkv(me, acc, q_outs, k_new, v_new)

    def drain(j, _):
        pair_a(j).wait_send()
        pair_b(j).wait_send()
        across(j).wait_send()
        hidden(3, j, me, partner).wait_send()
        hidden(4, j, me, cross).wait_send()
        hidden(5, j, cross, partner).wait_send()
        return 0

    lax.fori_loop(0, NJ, drain, 0)


def out_product(layer, fuse, ds, res, w_out, qkv_weights):
    part = (NJ, ROWS, CH)
    shared = [
        VM((ROWS, QW), BF16),
        VM((ROWS, QW), BF16),
        VM((WO_SLOTS, QW, CH), BF16),
        VM(part, F32), VM(part, F32), VM(part, F32), VM(part, F32), VM(part, F32), VM(part, F32), VM(part, F32),
        pltpu.SemaphoreType.DMA((WO_SLOTS,)),
        pltpu.SemaphoreType.DMA,
        pltpu.SemaphoreType.DMA((6, NJ)),
        pltpu.SemaphoreType.DMA((6, NJ)),
    ]
    n = D // CH
    flops = 2 * ROWS * QW * D
    if fuse:
        out_shape = [sds((MINE, QW))] * 4 + [sds((MINE, HD))] * 2 + [sds((ROWS, QW))]
        out_specs = [VSPEC] * 7
        extra = [
            VM((ROWS, D), BF16),
            VM((n, CH, QKV), BF16),
            VM((ROWS, QKV), F32),
            pltpu.SemaphoreType.DMA((3, n)),
        ]
        args = (*ds, res, w_out, *qkv_weights)
        flops += 2 * ROWS * D * QKV
    else:
        out_shape = sds((ROWS, D))
        out_specs = VSPEC
        extra = []
        args = (*ds, res, w_out)
    return pl.pallas_call(
        functools.partial(out_kernel, layer, fuse),
        out_shape=out_shape,
        in_specs=[VSPEC] * 4 + [ASPEC] * (len(args) - 4),
        out_specs=out_specs,
        scratch_shapes=extra + shared,
        compiler_params=pltpu.CompilerParams(
            vmem_limit_bytes=63 * MIB if fuse else 32 * MIB, collective_id=layer, has_side_effects=True),
        cost_estimate=pl.CostEstimate(flops=flops, bytes_accessed=flops // ROWS, transcendentals=0),
        name=f"out_product_{layer}",
    )(*args)


def swap(parts):
    out = [parts[0]]
    for i in range(1, GROUPS):
        out.append(lax.ppermute(parts[i], "model", [(m, m ^ i) for m in range(GROUPS)]))
    return out


def solution(mesh):
    cache_spec = P(None, ("replica", "model"), None, None)

    def device_step(x, cache_len, w_query, w_key, w_value, w_out, k_cache, v_cache):
        *qs, k_new, v_new = first_qkv(x, w_query, w_key, w_value)
        rs = swap(qs)
        k_out = copy_cache(0, cache_len, k_new, k_cache, None)
        cs = attend(0, cache_len, rs, k_new, v_new, k_cache, v_cache)
        ds = swap(cs)
        v_out = copy_cache(0, cache_len, v_new, v_cache, None)
        *qs, k_new, v_new, res = out_product(0, True, ds, x, w_out, (w_query, w_key, w_value))
        rs = swap(qs)
        k_out = copy_cache(1, cache_len, k_new, k_cache, k_out)
        cs = attend(1, cache_len, rs, k_new, v_new, k_cache, v_cache)
        ds = swap(cs)
        v_out = copy_cache(1, cache_len, v_new, v_cache, v_out)
        out = out_product(1, False, ds, res, w_out, ())
        return out, k_out, v_out

    return jax.shard_map(
        device_step,
        mesh=mesh,
        in_specs=(P("replica", None), P("replica"), P(None, None, "model"), P(), P(), P(None, "model", None), cache_spec, cache_spec),
        out_specs=(P("replica", None), cache_spec, cache_spec),
        check_vma=False,
    )
```

```python
import functools

import jax
import jax.numpy as jnp
from jax import lax
from jax.experimental import pallas as pl
from jax.experimental.pallas import tpu as pltpu
from jax.sharding import PartitionSpec as P

F32 = jnp.float32
BF16 = jnp.bfloat16
MIB = 1 << 20
BIG = 50 * MIB

GROUPS = 4
ROWS = 64
MINE = 16
D = 8192
HD = 128
LH = 16
QW = LH * HD
SEQ = 2048
CH = 512
NJ = QW // CH
QKV = QW + 2 * HD
WO_SLOTS = 6
BLK = 256
VM = pltpu.VMEM
VSPEC = pl.BlockSpec(memory_space=pltpu.VMEM)
ASPEC = pl.BlockSpec(memory_space=pltpu.HBM)
SSPEC = pl.BlockSpec(memory_space=pltpu.SMEM)


def sds(shape, dtype=BF16):
    return jax.ShapeDtypeStruct(shape, dtype)


def qkv_copies(layer, chunk, slot, wq, wk, wv, buf, sems):
    rows = pl.ds(pl.multiple_of(chunk * CH, CH), CH)
    return (
        pltpu.make_async_copy(wq.at[layer, rows, :], buf.at[slot, :, pl.ds(0, QW)], sems.at[0, slot]),
        pltpu.make_async_copy(wk.at[layer, rows, :], buf.at[slot, :, pl.ds(QW, HD)], sems.at[1, slot]),
        pltpu.make_async_copy(wv.at[layer, rows, :], buf.at[slot, :, pl.ds(QW + HD, HD)], sems.at[2, slot]),
    )


def write_qkv(me, acc, q_outs, k_new, v_new):
    for i, q_out in enumerate(q_outs):
        other = xor_id(me, i)
        q_out[...] = acc[pl.ds(pl.multiple_of(other * MINE, MINE), MINE), 0:QW].astype(BF16)
    mine = pl.ds(pl.multiple_of(me * MINE, MINE), MINE)
    k_new[...] = acc[mine, QW:QW + HD].astype(BF16)
    v_new[...] = acc[mine, QW + HD:QKV].astype(BF16)


def xor_id(me, i):
    core = lax.rem(me, 2)
    other = me
    if i & 1:
        other = other + 1 - 2 * core
    if i & 2:
        other = lax.rem(other + 2, GROUPS)
    return other


def first_qkv_kernel(x, wq, wk, wv, q0, q1, q2, q3, k_new, v_new, buf, acc, xbuf, sems, x_sem):
    me = lax.axis_index("model")
    chunks = D // CH
    x_copy = pltpu.make_async_copy(x, xbuf, x_sem)
    x_copy.start()

    def start(c, _):
        for cp in qkv_copies(0, c, c, wq, wk, wv, buf, sems):
            cp.start()
        return 0

    lax.fori_loop(0, chunks, start, 0)
    acc[...] = jnp.zeros_like(acc)
    x_copy.wait()

    def step(c, _):
        for cp in qkv_copies(0, c, c, wq, wk, wv, buf, sems):
            cp.wait()
        cols = pl.ds(pl.multiple_of(c * CH, CH), CH)
        acc[...] += jnp.dot(xbuf[:, cols], buf[c], preferred_element_type=F32)
        return 0

    lax.fori_loop(0, chunks, step, 0)
    write_qkv(me, acc, (q0, q1, q2, q3), k_new, v_new)


def first_qkv(x, wq, wk, wv):
    n = D // CH
    return pl.pallas_call(
        first_qkv_kernel,
        out_shape=[sds((MINE, QW))] * 4 + [sds((MINE, HD))] * 2,
        in_specs=[ASPEC] * 4,
        out_specs=[VSPEC] * 6,
        scratch_shapes=[
            VM((n, CH, QKV), BF16),
            VM((ROWS, QKV), F32),
            VM((ROWS, D), BF16),
            pltpu.SemaphoreType.DMA((3, n)),
            pltpu.SemaphoreType.DMA,
        ],
        compiler_params=pltpu.CompilerParams(vmem_limit_bytes=BIG),
        cost_estimate=pl.CostEstimate(flops=2 * ROWS * D * QKV, bytes_accessed=2 * D * QKV, transcendentals=0),
        name="first_qkv",
    )(x, wq, wk, wv)


K_CUT = 6
V_CUT = 10


def put_row(buf, b, length, row):
    base = pl.multiple_of((length // 16) * 16, 16)
    here = lax.broadcasted_iota(jnp.int32, (16, HD), 0) == length - base
    buf[b, pl.ds(base, 16), :] = jnp.where(here, row, buf[b, pl.ds(base, 16), :])


class Share:
    def __init__(self, layer, first, last, lens, new, src, dst, buf, in_sems, out_sems):
        self.layer, self.first, self.count = layer, first, last - first
        self.lens, self.new, self.src, self.dst, self.buf = lens, new, src, dst, buf
        self.in_sems, self.out_sems = in_sems, out_sems

    def take(self, n):
        return pltpu.make_async_copy(self.src.at[self.layer, self.first + n], self.buf.at[n], self.in_sems.at[n])

    def give(self, n):
        return pltpu.make_async_copy(self.buf.at[n], self.dst.at[self.layer, self.first + n], self.out_sems.at[n])

    def start(self):
        for n in range(self.count):
            self.take(n).start()

    def forward(self):
        me = lax.axis_index("model")
        for n in range(self.count):
            self.take(n).wait()
            b = self.first + n
            put_row(self.buf, n, self.lens[me * MINE + b], self.new[pl.ds(b, 1), :])
            if n:
                self.give(n - 1).start()
        self.give(self.count - 1).start()

    def finish(self):
        for n in range(self.count):
            self.give(n).wait()

    @staticmethod
    def scratch(first, last):
        return [VM((last - first, SEQ, HD), BF16), pltpu.SemaphoreType.DMA((last - first,)),
                pltpu.SemaphoreType.DMA((last - first,))]


def copy_kernel(layer, first, last, n_in, *refs):
    lens, new, src = refs[:3]
    share = Share(layer, first, last, lens, new, src, *refs[n_in:])
    share.start()
    share.forward()
    share.finish()


def copy_cache(layer, first, last, lens, new, src, prior):
    args = [lens, new, src] + ([prior] if prior is not None else [])
    return pl.pallas_call(
        functools.partial(copy_kernel, layer, first, last, len(args)),
        out_shape=sds(src.shape),
        in_specs=[SSPEC, VSPEC, ASPEC] + ([ASPEC] if prior is not None else []),
        out_specs=ASPEC,
        input_output_aliases={3: 0} if prior is not None else {},
        scratch_shapes=Share.scratch(first, last),
        compiler_params=pltpu.CompilerParams(vmem_limit_bytes=BIG),
        cost_estimate=pl.CostEstimate(flops=5_000_000_000, bytes_accessed=4 * MINE * SEQ * HD, transcendentals=0),
        name=f"copy_cache_{layer}",
    )(*args)


GRP = 4
TIERS = (512, 1024, 2048)


def attend_kernel(layer, n_in, *refs):
    lens, r0, r1, r2, r3, k_new, v_new, k_cache, v_cache = refs[:9]
    c0, c1, c2, c3, k_out, v_out, kbuf, vbuf, qbuf, cbuf, new_kv, ksems, vsems = refs[n_in:n_in + 13]
    shares = refs[n_in + 13:]
    k_share = Share(layer, K_CUT, MINE, lens, k_new, k_cache, k_out, *shares[:3])
    v_share = Share(layer, 0, V_CUT, lens, v_new, v_cache, v_out, *shares[3:])
    me = lax.axis_index("model")
    n_heads = GROUPS * LH
    scale = HD ** -0.5

    def length(b):
        return lens[me * MINE + b]

    def tier_of(b, n):
        return jnp.logical_and(length(b) < TIERS[n], length(b) >= (TIERS[n - 1] if n else BLK))

    def copies(b, part):
        cut = pl.ds(*part)
        return (pltpu.make_async_copy(k_cache.at[layer, b, cut, :], kbuf.at[b, cut, :], ksems.at[b, part[0] // BLK]),
                pltpu.make_async_copy(v_cache.at[layer, b, cut, :], vbuf.at[b, cut, :], vsems.at[b, part[0] // BLK]))

    def start_first(b, _):
        for cp in copies(b, (0, BLK)):
            cp.start()
        return 0

    def start_rest(b, _):
        for n, size in enumerate(TIERS):
            @pl.when(tier_of(b, n))
            def _(size=size):
                for cp in copies(b, (BLK, size - BLK)):
                    cp.start()
        return 0

    lax.fori_loop(0, MINE, start_first, 0)
    lax.fori_loop(0, MINE, start_rest, 0)
    k_share.start()
    v_share.start()

    for i, r in enumerate((r0, r1, r2, r3)):
        qbuf[:, i * LH:(i + 1) * LH, :] = r[...].reshape(MINE, LH, HD)

    for b in range(MINE):
        new_kv[0, b] = k_new[b:b + 1, :].astype(F32)
        new_kv[1, b] = v_new[b:b + 1, :].astype(F32)

    def new_rows(b):
        put_row(kbuf, b, length(b), new_kv[0, b].astype(BF16))
        put_row(vbuf, b, length(b), new_kv[1, b].astype(BF16))

    def context(seqs, size):
        scores = []
        for b in seqs:
            s = lax.dot_general(qbuf[b], kbuf[b, 0:size, :], (((1,), (1,)), ((), ())),
                                preferred_element_type=F32)
            pos = lax.broadcasted_iota(jnp.int32, (n_heads, size), 1)
            scores.append(jnp.where(pos <= length(b), s * scale, -jnp.inf))
        expos = [jnp.exp(s - jnp.max(s, axis=1, keepdims=True)) for s in scores]
        probs = [(e * (1.0 / jnp.sum(e, axis=1, keepdims=True))).astype(BF16) for e in expos]
        for b, p in zip(seqs, probs):
            cbuf[b] = jnp.dot(p, vbuf[b, 0:size, :], preferred_element_type=F32).astype(BF16)

    def first_blocks(g, _):
        seqs = [g * GRP + i for i in range(GRP)]
        for b in seqs:
            for cp in copies(b, (0, BLK)):
                cp.wait()

            @pl.when(length(b) < BLK)
            def _(b=b):
                new_rows(b)
        context(seqs, BLK)
        return 0

    lax.fori_loop(0, MINE // GRP, first_blocks, 0)
    k_share.forward()
    v_share.forward()

    def rest(b, _):
        for n, size in enumerate(TIERS):
            @pl.when(tier_of(b, n))
            def _(size=size):
                for cp in copies(b, (BLK, size - BLK)):
                    cp.wait()
                new_rows(b)
                context((b,), size)
        return 0

    lax.fori_loop(0, MINE, rest, 0)

    for i, c in enumerate((c0, c1, c2, c3)):
        c[...] = cbuf[:, i * LH:(i + 1) * LH, :].reshape(MINE, QW)
    k_share.finish()
    v_share.finish()


def attend(layer, lens, rs, k_new, v_new, k_cache, v_cache, k_out, v_out):
    args = [lens, *rs, k_new, v_new, k_cache, v_cache, k_out] + ([v_out] if v_out is not None else [])
    return pl.pallas_call(
        functools.partial(attend_kernel, layer, len(args)),
        out_shape=[sds((MINE, QW))] * 4 + [sds(k_cache.shape)] * 2,
        in_specs=[SSPEC] + [VSPEC] * 6 + [ASPEC] * (len(args) - 7),
        out_specs=[VSPEC] * 4 + [ASPEC] * 2,
        input_output_aliases={9: 4} if v_out is None else {9: 4, 10: 5},
        scratch_shapes=[
            VM((MINE, SEQ, HD), BF16),
            VM((MINE, SEQ, HD), BF16),
            VM((MINE, GROUPS * LH, HD), BF16),
            VM((MINE, GROUPS * LH, HD), BF16),
            VM((2, MINE, 1, HD), F32),
            pltpu.SemaphoreType.DMA((MINE, 2)),
            pltpu.SemaphoreType.DMA((MINE, 2)),
            *Share.scratch(K_CUT, MINE),
            *Share.scratch(0, V_CUT),
        ],
        compiler_params=pltpu.CompilerParams(vmem_limit_bytes=BIG),
        cost_estimate=pl.CostEstimate(flops=5_000_000_000, bytes_accessed=8 * MIB, transcendentals=0),
        name=f"attend_{layer}",
    )(*args)


def out_kernel(layer, fuse, *refs):
    d_refs, (res, wo), refs = refs[:4], refs[4:6], refs[6:]
    if fuse:
        (wq, wk, wv), outs, refs = refs[:3], refs[3:10], refs[10:]
        q_outs, (k_new, v_new, res_out) = outs[:4], outs[4:]
        hid, qbuf, acc, q_sems = refs[:4]
        refs = refs[4:]
    else:
        hid, refs = refs[0], refs[1:]
    ctx, resv, wbuf, send_a, recv_a, send_c, recv_c, send_b, recv_b, own, w_sems, res_sem, ssems, rsems = refs

    me = lax.axis_index("model")
    partner, cross, diag = xor_id(me, 1), xor_id(me, 2), xor_id(me, 3)

    def cols(chunk):
        return pl.ds(pl.multiple_of(chunk * CH, CH), CH)

    def wo_copy(step):
        chip_of = lax.rem(lax.div(me, 2) + 1 - step // (2 * NJ), 2)
        core_of = lax.rem(lax.rem(me, 2) + 1 - step % 2, 2)
        chunk = (chip_of * 2 + core_of) * NJ + step % (2 * NJ) // 2
        slot = step % WO_SLOTS
        return pltpu.make_async_copy(wo.at[layer, :, cols(chunk)], wbuf.at[slot], w_sems.at[slot])

    def q_copies(chunk, slot):
        return qkv_copies(layer + 1, chunk, slot, wq, wk, wv, qbuf, q_sems)

    def send(kind, j, src, dst, dev):
        return pltpu.make_async_remote_copy(
            src_ref=src, dst_ref=dst, send_sem=ssems.at[kind, j], recv_sem=rsems.at[kind, j],
            device_id={"model": dev}, device_id_type=pl.DeviceIdType.MESH)

    def pair_a(j):
        return send(0, j, send_a.at[j], recv_a.at[j], partner)

    def pair_b(j):
        return send(1, j, send_b.at[j], recv_b.at[j], partner)

    def across(j):
        return send(2, j, send_c.at[j], recv_c.at[j], cross)

    def hidden(kind, j, owner, dev):
        part = hid.at[:, cols(owner * NJ + j)]
        return send(kind, j, part, part, dev)

    def start_wo(step, _):
        wo_copy(step).start()
        return 0

    lax.fori_loop(0, WO_SLOTS, start_wo, 0)
    if fuse:
        res_copy = pltpu.make_async_copy(
            res.at[:, pl.ds(pl.multiple_of(me * QW, QW), QW)], resv, res_sem)
    else:
        res_copy = pltpu.make_async_copy(res, resv, res_sem)
    res_copy.start()

    for i, d in enumerate(d_refs):
        ctx[pl.ds(pl.multiple_of(xor_id(me, i) * MINE, MINE), MINE), :] = d[...]
    if fuse:
        acc[...] = jnp.zeros_like(acc)

    barrier = pltpu.get_barrier_semaphore()
    for dev in (partner, cross):
        pl.semaphore_signal(barrier, inc=1, device_id={"model": dev}, device_id_type=pl.DeviceIdType.MESH)
    pl.semaphore_wait(barrier, 2)

    def part_sum(step):
        wo_copy(step).wait()
        return jnp.dot(ctx[...], wbuf[step % WO_SLOTS], preferred_element_type=F32)

    def refill(step):
        @pl.when(step + WO_SLOTS < 4 * NJ)
        def _():
            wo_copy(step + WO_SLOTS).start()

    def send_across(j):
        pair_a(j).wait_recv()
        send_c[j] += recv_a[j]
        across(j).start()

    def phase_a(j, _):
        send_a[j] = part_sum(2 * j)
        pair_a(j).start()
        refill(2 * j)

        @pl.when(j > 0)
        def _():
            send_across(j - 1)
        send_c[j] = part_sum(2 * j + 1)
        refill(2 * j + 1)
        return 0

    lax.fori_loop(0, NJ, phase_a, 0)
    send_across(NJ - 1)

    def phase_b(j, _):
        step = 2 * NJ + 2 * j
        send_b[j] = part_sum(step)
        pair_b(j).start()
        refill(step)
        own[j] = part_sum(step + 1)
        refill(step + 1)
        if fuse:
            for i, owner in enumerate((me, partner)):
                for cp in q_copies(owner * NJ + j, 2 * j + i):
                    cp.start()
        return 0

    lax.fori_loop(0, NJ, phase_b, 0)
    if fuse:
        def start_far(j, _):
            for i, owner in enumerate((cross, diag)):
                for cp in q_copies(owner * NJ + j, 2 * NJ + 2 * j + i):
                    cp.start()
            return 0

        lax.fori_loop(0, NJ, start_far, 0)
    res_copy.wait()

    def next_q(owner, j, slot):
        if fuse:
            chunk = owner * NJ + j
            for cp in q_copies(chunk, slot):
                cp.wait()
            acc[...] += jnp.dot(hid[:, cols(chunk)], qbuf[slot], preferred_element_type=F32)

    def from_partner(j):
        hidden(3, j, partner, partner).wait_recv()
        next_q(partner, j, 2 * j + 1)

    def phase_c(j, _):
        pair_b(j).wait_recv()
        across(j).wait_recv()
        total = own[j] + recv_b[j] + recv_c[j]
        part = (resv[:, cols(j)].astype(F32) + total).astype(BF16)
        hid[:, cols(me * NJ + j)] = part
        if fuse:
            res_out[:, cols(j)] = part
        hidden(4, j, me, cross).start()
        hidden(3, j, me, partner).start()
        next_q(me, j, 2 * j)

        @pl.when(j > 0)
        def _():
            from_partner(j - 1)
        return 0

    lax.fori_loop(0, NJ, phase_c, 0)
    from_partner(NJ - 1)

    def forwarded(j):
        hidden(5, j, diag, partner).wait_recv()
        next_q(diag, j, 2 * NJ + 2 * j + 1)

    def phase_d(j, _):
        hidden(4, j, cross, cross).wait_recv()
        hidden(5, j, cross, partner).start()
        next_q(cross, j, 2 * NJ + 2 * j)

        @pl.when(j > 0)
        def _():
            forwarded(j - 1)
        return 0

    lax.fori_loop(0, NJ, phase_d, 0)
    forwarded(NJ - 1)

    if fuse:
        write_qkv(me, acc, q_outs, k_new, v_new)

    def drain(j, _):
        pair_a(j).wait_send()
        pair_b(j).wait_send()
        across(j).wait_send()
        hidden(3, j, me, partner).wait_send()
        hidden(4, j, me, cross).wait_send()
        hidden(5, j, cross, partner).wait_send()
        return 0

    lax.fori_loop(0, NJ, drain, 0)


def out_product(layer, fuse, ds, res, w_out, qkv_weights):
    part = (NJ, ROWS, CH)
    shared = [
        VM((ROWS, QW), BF16),
        VM((ROWS, QW), BF16),
        VM((WO_SLOTS, QW, CH), BF16),
        VM(part, F32), VM(part, F32), VM(part, F32), VM(part, F32), VM(part, F32), VM(part, F32), VM(part, F32),
        pltpu.SemaphoreType.DMA((WO_SLOTS,)),
        pltpu.SemaphoreType.DMA,
        pltpu.SemaphoreType.DMA((6, NJ)),
        pltpu.SemaphoreType.DMA((6, NJ)),
    ]
    n = D // CH
    flops = 2 * ROWS * QW * D
    if fuse:
        out_shape = [sds((MINE, QW))] * 4 + [sds((MINE, HD))] * 2 + [sds((ROWS, QW))]
        out_specs = [VSPEC] * 7
        extra = [
            VM((ROWS, D), BF16),
            VM((n, CH, QKV), BF16),
            VM((ROWS, QKV), F32),
            pltpu.SemaphoreType.DMA((3, n)),
        ]
        args = (*ds, res, w_out, *qkv_weights)
        flops += 2 * ROWS * D * QKV
    else:
        out_shape = sds((ROWS, D))
        out_specs = VSPEC
        extra = []
        args = (*ds, res, w_out)
    return pl.pallas_call(
        functools.partial(out_kernel, layer, fuse),
        out_shape=out_shape,
        in_specs=[VSPEC] * 4 + [ASPEC] * (len(args) - 4),
        out_specs=out_specs,
        scratch_shapes=extra + shared,
        compiler_params=pltpu.CompilerParams(
            vmem_limit_bytes=58 * MIB if fuse else 32 * MIB, collective_id=layer, has_side_effects=True),
        cost_estimate=pl.CostEstimate(flops=flops, bytes_accessed=flops // ROWS, transcendentals=0),
        name=f"out_product_{layer}",
    )(*args)


def swap(parts):
    out = [parts[0]]
    for i in range(1, GROUPS):
        out.append(lax.ppermute(parts[i], "model", [(m, m ^ i) for m in range(GROUPS)]))
    return out


def solution(mesh):
    cache_spec = P(None, ("replica", "model"), None, None)

    def device_step(x, cache_len, w_query, w_key, w_value, w_out, k_cache, v_cache):
        *qs, k_new, v_new = first_qkv(x, w_query, w_key, w_value)
        k_out = v_out = None
        res = x
        for layer in range(2):
            rs = swap(qs)
            k_out = copy_cache(layer, 0, K_CUT, cache_len, k_new, k_cache, k_out)
            *cs, k_out, v_out = attend(layer, cache_len, rs, k_new, v_new, k_cache, v_cache, k_out, v_out)
            ds = swap(cs)
            v_out = copy_cache(layer, V_CUT, MINE, cache_len, v_new, v_cache, v_out)
            if layer == 0:
                *qs, k_new, v_new, res = out_product(0, True, ds, x, w_out, (w_query, w_key, w_value))
            else:
                out = out_product(1, False, ds, res, w_out, ())
        return out, k_out, v_out

    return jax.shard_map(
        device_step,
        mesh=mesh,
        in_specs=(P("replica", None), P("replica"), P(None, None, "model"), P(), P(), P(None, "model", None), cache_spec, cache_spec),
        out_specs=(P("replica", None), cache_spec, cache_spec),
        check_vma=False,
    )
```

```python
import functools

import jax
import jax.numpy as jnp
from jax import lax
from jax.experimental import pallas as pl
from jax.experimental.pallas import tpu as pltpu
from jax.sharding import PartitionSpec as P

F32 = jnp.float32
BF16 = jnp.bfloat16
MIB = 1 << 20
BIG = 50 * MIB

GROUPS = 4
ROWS = 64
MINE = 16
D = 8192
HD = 128
LH = 16
QW = LH * HD
SEQ = 2048
CH = 512
NJ = QW // CH
QKV = QW + 2 * HD
WO_SLOTS = 4
AHEAD = 4
Q_AHEAD = 6
BLK = 256
VM = pltpu.VMEM
VSPEC = pl.BlockSpec(memory_space=pltpu.VMEM)
ASPEC = pl.BlockSpec(memory_space=pltpu.HBM)
SSPEC = pl.BlockSpec(memory_space=pltpu.SMEM)


def sds(shape, dtype=BF16):
    return jax.ShapeDtypeStruct(shape, dtype)


def qkv_copies(layer, chunk, slot, wq, wk, wv, buf, sems):
    rows = pl.ds(pl.multiple_of(chunk * CH, CH), CH)
    return (
        pltpu.make_async_copy(wq.at[layer, rows, :], buf.at[slot, :, pl.ds(0, QW)], sems.at[0, slot]),
        pltpu.make_async_copy(wk.at[layer, rows, :], buf.at[slot, :, pl.ds(QW, HD)], sems.at[1, slot]),
        pltpu.make_async_copy(wv.at[layer, rows, :], buf.at[slot, :, pl.ds(QW + HD, HD)], sems.at[2, slot]),
    )


def write_qkv(me, acc, q_outs, k_new, v_new):
    for i, q_out in enumerate(q_outs):
        other = xor_id(me, i)
        q_out[...] = acc[pl.ds(pl.multiple_of(other * MINE, MINE), MINE), 0:QW].astype(BF16)
    mine = pl.ds(pl.multiple_of(me * MINE, MINE), MINE)
    k_new[...] = acc[mine, QW:QW + HD].astype(BF16)
    v_new[...] = acc[mine, QW + HD:QKV].astype(BF16)


def xor_id(me, i):
    core = lax.rem(me, 2)
    other = me
    if i & 1:
        other = other + 1 - 2 * core
    if i & 2:
        other = lax.rem(other + 2, GROUPS)
    return other


def first_qkv_kernel(x, wq, wk, wv, r0, r1, r2, r3, k_new, v_new,
                     xbuf, wbuf, kvbuf, acc, qbuf, rbuf, x_sem, w_sems, kv_sems, ssems, rsems):
    me = lax.axis_index("model")
    depth = D // NJ

    def cols(n):
        return pl.ds(pl.multiple_of(n * CH, CH), CH)

    def w_copy(step):
        rows = pl.ds(pl.multiple_of(step % NJ * depth, depth), depth)
        return pltpu.make_async_copy(wq.at[0, rows, cols(step // NJ)], wbuf.at[step], w_sems.at[step])

    def send(i, n):
        dev = xor_id(me, i)
        rows = pl.ds(pl.multiple_of(dev * MINE, MINE), MINE)
        return pltpu.make_async_remote_copy(
            src_ref=qbuf.at[rows, cols(n)], dst_ref=rbuf.at[i - 1, :, cols(n)],
            send_sem=ssems.at[i - 1, n], recv_sem=rsems.at[i - 1, n],
            device_id={"model": dev}, device_id_type=pl.DeviceIdType.MESH)

    x_copy = pltpu.make_async_copy(x, xbuf, x_sem)
    x_copy.start()
    kv_copies = [pltpu.make_async_copy(w.at[0], kvbuf.at[:, pl.ds(i * HD, HD)], kv_sems.at[i]) for i, w in enumerate((wk, wv))]

    def start(step, _):
        w_copy(step).start()
        return 0

    lax.fori_loop(0, AHEAD, start, 0)

    barrier = pltpu.get_barrier_semaphore()
    for i in range(1, GROUPS):
        pl.semaphore_signal(barrier, inc=1, device_id={"model": xor_id(me, i)}, device_id_type=pl.DeviceIdType.MESH)
    x_copy.wait()

    def group(n):
        acc[...] = jnp.zeros_like(acc)

        def step(k, _):
            w_copy(n * NJ + k).wait()

            @pl.when(n * NJ + k + AHEAD < NJ * NJ)
            def _():
                w_copy(n * NJ + k + AHEAD).start()
            part = xbuf[:, pl.ds(pl.multiple_of(k * depth, depth), depth)]
            acc[...] += jnp.dot(part, wbuf[n * NJ + k], preferred_element_type=F32)
            return 0

        lax.fori_loop(0, NJ, step, 0)
        qbuf[:, cols(n)] = acc[...].astype(BF16)

    def leave(n):
        for i in (3, 2, 1):
            send(i, n).start()

    group(0)
    pl.semaphore_wait(barrier, GROUPS - 1)
    leave(0)

    def later(n, _):
        @pl.when(n == NJ - 1)
        def _():
            for cp in kv_copies:
                cp.start()
        group(n)
        leave(n)
        return 0

    lax.fori_loop(1, NJ, later, 0)
    mine = pl.ds(pl.multiple_of(me * MINE, MINE), MINE)
    for cp in kv_copies:
        cp.wait()
    kv = jnp.zeros((MINE, 2 * HD), F32)
    for k in range(NJ):
        kv += jnp.dot(xbuf[mine, k * depth:(k + 1) * depth], kvbuf[k * depth:(k + 1) * depth, :], preferred_element_type=F32)
    k_new[...] = kv[:, :HD].astype(BF16)
    v_new[...] = kv[:, HD:].astype(BF16)
    r0[...] = qbuf[mine, :]
    for i, r in ((1, r1), (2, r2), (3, r3)):
        for n in range(NJ):
            send(i, n).wait_recv()
        r[...] = rbuf[i - 1]

    def drain(n, _):
        for i in range(1, GROUPS):
            send(i, n).wait_send()
        return 0

    lax.fori_loop(0, NJ, drain, 0)


def first_qkv(x, wq, wk, wv):
    return pl.pallas_call(
        first_qkv_kernel,
        out_shape=[sds((MINE, QW))] * 4 + [sds((MINE, HD))] * 2,
        in_specs=[ASPEC] * 4,
        out_specs=[VSPEC] * 6,
        scratch_shapes=[
            VM((ROWS, D), BF16),
            VM((NJ * NJ, D // NJ, CH), BF16),
            VM((D, 2 * HD), BF16),
            VM((ROWS, CH), F32),
            VM((ROWS, QW), BF16),
            VM((GROUPS - 1, MINE, QW), BF16),
            pltpu.SemaphoreType.DMA,
            pltpu.SemaphoreType.DMA((NJ * NJ,)),
            pltpu.SemaphoreType.DMA((2,)),
            pltpu.SemaphoreType.DMA((GROUPS - 1, NJ)),
            pltpu.SemaphoreType.DMA((GROUPS - 1, NJ)),
        ],
        compiler_params=pltpu.CompilerParams(vmem_limit_bytes=53 * MIB, collective_id=2, has_side_effects=True),
        cost_estimate=pl.CostEstimate(flops=2 * ROWS * D * QKV, bytes_accessed=2 * D * QKV, transcendentals=0),
        name="first_qkv",
    )(x, wq, wk, wv)


K_CUT = (0, 6)
V_CUT = (10, 10)
READ_AHEAD = 2


def put_row(buf, b, length, row):
    base = pl.multiple_of((length // 16) * 16, 16)
    here = lax.broadcasted_iota(jnp.int32, (16, HD), 0) == length - base
    buf[b, pl.ds(base, 16), :] = jnp.where(here, row, buf[b, pl.ds(base, 16), :])


class Share:
    def __init__(self, layer, first, last, lens, new, src, dst, buf, in_sems, out_sems):
        self.layer, self.first, self.count = layer, first, last - first
        self.lens, self.new, self.src, self.dst, self.buf = lens, new, src, dst, buf
        self.in_sems, self.out_sems = in_sems, out_sems

    def take(self, n):
        return pltpu.make_async_copy(self.src.at[self.layer, self.first + n], self.buf.at[n], self.in_sems.at[n])

    def give(self, n):
        return pltpu.make_async_copy(self.buf.at[n], self.dst.at[self.layer, self.first + n], self.out_sems.at[n])

    def start(self):
        for n in range(self.count):
            self.take(n).start()

    def forward(self, n):
        me = lax.axis_index("model")
        self.take(n).wait()
        b = self.first + n
        put_row(self.buf, n, self.lens[me * MINE + b], self.new[pl.ds(b, 1), :])
        if n:
            self.give(n - 1).start()
        if n == self.count - 1:
            self.give(n).start()

    def finish(self):
        for n in range(self.count):
            self.give(n).wait()

    @staticmethod
    def scratch(first, last):
        return [VM((last - first, SEQ, HD), BF16), pltpu.SemaphoreType.DMA((last - first,)),
                pltpu.SemaphoreType.DMA((last - first,))]


def copy_kernel(layer, first, last, n_in, *refs):
    lens, new, src = refs[:3]
    share = Share(layer, first, last, lens, new, src, *refs[n_in:])
    share.start()
    for n in range(share.count):
        share.forward(n)
    share.finish()


def copy_cache(layer, first, last, lens, new, src, prior):
    args = [lens, new, src] + ([prior] if prior is not None else [])
    return pl.pallas_call(
        functools.partial(copy_kernel, layer, first, last, len(args)),
        out_shape=sds(src.shape),
        in_specs=[SSPEC, VSPEC, ASPEC] + ([ASPEC] if prior is not None else []),
        out_specs=ASPEC,
        input_output_aliases={3: 0} if prior is not None else {},
        scratch_shapes=Share.scratch(first, last),
        compiler_params=pltpu.CompilerParams(vmem_limit_bytes=BIG),
        cost_estimate=pl.CostEstimate(flops=5_000_000_000, bytes_accessed=4 * MINE * SEQ * HD, transcendentals=0),
        name=f"copy_cache_{layer}",
    )(*args)


GRP = 4
TIERS = (512, 1024, 2048)


def attend_kernel(layer, n_in, *refs):
    lens, r0, r1, r2, r3, k_new, v_new, k_cache, v_cache = refs[:9]
    c0, c1, c2, c3, k_out, v_out, kbuf, vbuf, qbuf, cbuf, new_kv, ksems, vsems, ko_sems, vo_sems = refs[n_in:]
    me = lax.axis_index("model")
    n_heads = GROUPS * LH
    scale = HD ** -0.5
    caches = ((k_cache, kbuf, ksems, k_out, ko_sems, K_CUT[layer], MINE), (v_cache, vbuf, vsems, v_out, vo_sems, 0, V_CUT[layer]))

    def length(b):
        return lens[me * MINE + b]

    def tier_of(b, n):
        return jnp.logical_and(length(b) < TIERS[n], length(b) >= (TIERS[n - 1] if n else BLK))

    def reads(b, act):
        for cache, buf, sems, _, _, first, last in caches:
            def part(start, size, cache=cache, buf=buf, sems=sems):
                cut = pl.ds(start, size)
                return pltpu.make_async_copy(cache.at[layer, b, cut, :], buf.at[b, cut, :], sems.at[b, min(start, 1)])

            @pl.when(jnp.logical_and(b >= first, b < last))
            def _(part=part):
                act(part(0, SEQ))

            @pl.when(jnp.logical_or(b < first, b >= last))
            def _(part=part):
                act(part(0, BLK))
                for n, size in enumerate(TIERS):
                    @pl.when(tier_of(b, n))
                    def _(size=size):
                        act(part(BLK, size - BLK))

    def writes(b, act):
        for _, buf, _, out, sems, first, last in caches:
            @pl.when(jnp.logical_and(b >= first, b < last))
            def _(buf=buf, out=out, sems=sems):
                act(pltpu.make_async_copy(buf.at[b], out.at[layer, b], sems.at[b]))

    def each(g, do):
        for i in range(GRP):
            do(g * GRP + i)

    def start_group(g, _):
        each(g, lambda b: reads(b, lambda cp: cp.start()))
        return 0

    lax.fori_loop(0, READ_AHEAD, start_group, 0)
    for i, r in enumerate((r0, r1, r2, r3)):
        qbuf[:, i * LH:(i + 1) * LH, :] = r[...].reshape(MINE, LH, HD)
    for b in range(MINE):
        new_kv[0, b] = k_new[b:b + 1, :].astype(F32)
        new_kv[1, b] = v_new[b:b + 1, :].astype(F32)

    def context(seqs, size):
        scores = []
        for b in seqs:
            s = lax.dot_general(qbuf[b], kbuf[b, 0:size, :], (((1,), (1,)), ((), ())), preferred_element_type=F32)
            pos = lax.broadcasted_iota(jnp.int32, (n_heads, size), 1)
            scores.append(jnp.where(pos <= length(b), s * scale, -jnp.inf))
        expos = [jnp.exp(s - jnp.max(s, axis=1, keepdims=True)) for s in scores]
        probs = [(e * (1.0 / jnp.sum(e, axis=1, keepdims=True))).astype(BF16) for e in expos]
        for b, p in zip(seqs, probs):
            cbuf[b] = jnp.dot(p, vbuf[b, 0:size, :], preferred_element_type=F32).astype(BF16)

    def ready(b):
        reads(b, lambda cp: cp.wait())
        put_row(kbuf, b, length(b), new_kv[0, b].astype(BF16))
        put_row(vbuf, b, length(b), new_kv[1, b].astype(BF16))

    def long_one(b, _):
        for n, size in enumerate(TIERS):
            @pl.when(tier_of(b, n))
            def _(size=size):
                context((b,), size)
        return 0

    def group(g, _):
        each(g, ready)

        @pl.when(g + READ_AHEAD < MINE // GRP)
        def _():
            start_group(g + READ_AHEAD, 0)
        context([g * GRP + i for i in range(GRP)], BLK)
        each(g, lambda b: writes(b, lambda cp: cp.start()))
        lax.fori_loop(g * GRP, (g + 1) * GRP, long_one, 0)
        return 0

    lax.fori_loop(0, MINE // GRP, group, 0)
    for i, c in enumerate((c0, c1, c2, c3)):
        c[...] = cbuf[:, i * LH:(i + 1) * LH, :].reshape(MINE, QW)

    def finish(b, _):
        writes(b, lambda cp: cp.wait())
        return 0

    lax.fori_loop(0, MINE, finish, 0)


def attend(layer, lens, rs, k_new, v_new, k_cache, v_cache, priors):
    args = [lens, *rs, k_new, v_new, k_cache, v_cache, *priors]
    return pl.pallas_call(
        functools.partial(attend_kernel, layer, len(args)),
        out_shape=[sds((MINE, QW))] * 4 + [sds(k_cache.shape)] * 2,
        in_specs=[SSPEC] + [VSPEC] * 6 + [ASPEC] * (len(args) - 7),
        out_specs=[VSPEC] * 4 + [ASPEC] * 2,
        input_output_aliases={9: 4, 10: 5} if priors else {},
        scratch_shapes=[
            VM((MINE, SEQ, HD), BF16),
            VM((MINE, SEQ, HD), BF16),
            VM((MINE, GROUPS * LH, HD), BF16),
            VM((MINE, GROUPS * LH, HD), BF16),
            VM((2, MINE, 1, HD), F32),
            pltpu.SemaphoreType.DMA((MINE, 2)),
            pltpu.SemaphoreType.DMA((MINE, 2)),
            pltpu.SemaphoreType.DMA((MINE,)),
            pltpu.SemaphoreType.DMA((MINE,)),
        ],
        compiler_params=pltpu.CompilerParams(vmem_limit_bytes=BIG),
        cost_estimate=pl.CostEstimate(flops=5_000_000_000, bytes_accessed=8 * MIB, transcendentals=0),
        name=f"attend_{layer}",
    )(*args)


def out_kernel(layer, fuse, *refs):
    d_refs, (res, wo), refs = refs[:4], refs[4:6], refs[6:]
    if fuse:
        (wq, wk, wv), outs, refs = refs[:3], refs[3:10], refs[10:]
        q_outs, (k_new, v_new, res_out) = outs[:4], outs[4:]
        hid, qbuf, acc, q_sems = refs[:4]
        refs = refs[4:]
    else:
        hid, refs = refs[0], refs[1:]
    ctx, resv, wbuf, send_a, recv_a, send_c, recv_c, send_b, recv_b, own, w_sems, res_sem, ssems, rsems = refs

    me = lax.axis_index("model")
    partner, cross, diag = xor_id(me, 1), xor_id(me, 2), xor_id(me, 3)

    def cols(chunk):
        return pl.ds(pl.multiple_of(chunk * CH, CH), CH)

    def wo_copy(step):
        chip_of = lax.rem(lax.div(me, 2) + 1 - step // (2 * NJ), 2)
        core_of = lax.rem(lax.rem(me, 2) + 1 - step % 2, 2)
        chunk = (chip_of * 2 + core_of) * NJ + step % (2 * NJ) // 2
        slot = step % WO_SLOTS
        return pltpu.make_async_copy(wo.at[layer, :, cols(chunk)], wbuf.at[slot], w_sems.at[slot])

    def q_copies(slot):
        chip_of = lax.rem(lax.div(me, 2) + slot // (2 * NJ), 2)
        core_of = lax.rem(lax.rem(me, 2) + slot % 2, 2)
        chunk = (chip_of * 2 + core_of) * NJ + slot % (2 * NJ) // 2
        return qkv_copies(layer + 1, chunk, slot, wq, wk, wv, qbuf, q_sems)

    def start_q(slot):
        for cp in q_copies(slot):
            cp.start()

    def send(kind, j, src, dst, dev):
        return pltpu.make_async_remote_copy(
            src_ref=src, dst_ref=dst, send_sem=ssems.at[kind, j], recv_sem=rsems.at[kind, j],
            device_id={"model": dev}, device_id_type=pl.DeviceIdType.MESH)

    def pair_a(j):
        return send(0, j, send_a.at[j], recv_a.at[j], partner)

    def pair_b(j):
        return send(1, j, send_b.at[j], recv_b.at[j], partner)

    def across(j):
        return send(2, j, send_c.at[j], recv_c.at[j], cross)

    def hidden(kind, j, owner, dev):
        part = hid.at[:, cols(owner * NJ + j)]
        return send(kind, j, part, part, dev)

    def start_wo(step, _):
        wo_copy(step).start()
        return 0

    lax.fori_loop(0, WO_SLOTS - 1, start_wo, 0)
    if fuse:
        res_copy = pltpu.make_async_copy(
            res.at[:, pl.ds(pl.multiple_of(me * QW, QW), QW)], resv, res_sem)
    else:
        res_copy = pltpu.make_async_copy(res, resv, res_sem)
    res_copy.start()

    for i, d in enumerate(d_refs):
        ctx[pl.ds(pl.multiple_of(xor_id(me, i) * MINE, MINE), MINE), :] = d[...]
    if fuse:
        acc[...] = jnp.zeros_like(acc)

    barrier = pltpu.get_barrier_semaphore()
    for dev in (partner, cross):
        pl.semaphore_signal(barrier, inc=1, device_id={"model": dev}, device_id_type=pl.DeviceIdType.MESH)
    def part_sum(step):
        wo_copy(step).wait()

        @pl.when(step + WO_SLOTS - 1 < 4 * NJ)
        def _():
            wo_copy(step + WO_SLOTS - 1).start()
        return jnp.dot(ctx[...], wbuf[step % WO_SLOTS], preferred_element_type=F32)

    def send_across(j):
        pair_a(j).wait_recv()
        send_c[j] += recv_a[j]
        across(j).start()

    def phase_a(j, _):
        send_a[j] = part_sum(2 * j)

        @pl.when(j == 0)
        def _():
            pl.semaphore_wait(barrier, 2)
        pair_a(j).start()

        @pl.when(j > 0)
        def _():
            send_across(j - 1)
        send_c[j] = part_sum(2 * j + 1)
        return 0

    lax.fori_loop(0, NJ, phase_a, 0)
    send_across(NJ - 1)

    def phase_b(j, _):
        step = 2 * NJ + 2 * j
        send_b[j] = part_sum(step)
        pair_b(j).start()
        own[j] = part_sum(step + 1)
        if fuse:
            @pl.when(j >= NJ - 2)
            def _():
                start_q(2 * (j - NJ + 2))
                start_q(2 * (j - NJ + 2) + 1)

            @pl.when(j == NJ - 1)
            def _():
                start_q(4)
                start_q(5)
        return 0

    lax.fori_loop(0, NJ, phase_b, 0)
    res_copy.wait()

    def next_q(owner, j, slot):
        if fuse:
            chunk = owner * NJ + j
            for cp in q_copies(slot):
                cp.wait()

            @pl.when(slot + Q_AHEAD < 4 * NJ)
            def _():
                start_q(slot + Q_AHEAD)
            acc[...] += jnp.dot(hid[:, cols(chunk)], qbuf[slot], preferred_element_type=F32)

    def from_partner(j):
        hidden(3, j, partner, partner).wait_recv()
        next_q(partner, j, 2 * j + 1)

    def phase_c(j, _):
        pair_b(j).wait_recv()
        across(j).wait_recv()
        total = own[j] + recv_b[j] + recv_c[j]
        part = (resv[:, cols(j)].astype(F32) + total).astype(BF16)
        hid[:, cols(me * NJ + j)] = part
        if fuse:
            res_out[:, cols(j)] = part
        hidden(4, j, me, cross).start()
        hidden(3, j, me, partner).start()
        next_q(me, j, 2 * j)

        @pl.when(j > 0)
        def _():
            from_partner(j - 1)
        return 0

    lax.fori_loop(0, NJ, phase_c, 0)
    from_partner(NJ - 1)

    def forwarded(j):
        hidden(5, j, diag, partner).wait_recv()
        next_q(diag, j, 2 * NJ + 2 * j + 1)

    def phase_d(j, _):
        hidden(4, j, cross, cross).wait_recv()
        hidden(5, j, cross, partner).start()
        next_q(cross, j, 2 * NJ + 2 * j)

        @pl.when(j > 0)
        def _():
            forwarded(j - 1)
        return 0

    lax.fori_loop(0, NJ, phase_d, 0)
    forwarded(NJ - 1)

    if fuse:
        write_qkv(me, acc, q_outs, k_new, v_new)

    def drain(j, _):
        pair_a(j).wait_send()
        pair_b(j).wait_send()
        across(j).wait_send()
        hidden(3, j, me, partner).wait_send()
        hidden(4, j, me, cross).wait_send()
        hidden(5, j, cross, partner).wait_send()
        return 0

    lax.fori_loop(0, NJ, drain, 0)


def out_product(layer, fuse, ds, res, w_out, qkv_weights):
    part = (NJ, ROWS, CH)
    shared = [
        VM((ROWS, QW), BF16),
        VM((ROWS, QW), BF16),
        VM((WO_SLOTS, QW, CH), BF16),
        VM(part, F32), VM(part, F32), VM(part, F32), VM(part, F32), VM(part, F32), VM(part, F32), VM(part, F32),
        pltpu.SemaphoreType.DMA((WO_SLOTS,)),
        pltpu.SemaphoreType.DMA,
        pltpu.SemaphoreType.DMA((6, NJ)),
        pltpu.SemaphoreType.DMA((6, NJ)),
    ]
    n = D // CH
    flops = 2 * ROWS * QW * D
    if fuse:
        out_shape = [sds((MINE, QW))] * 4 + [sds((MINE, HD))] * 2 + [sds((ROWS, QW))]
        out_specs = [VSPEC] * 7
        extra = [
            VM((ROWS, D), BF16),
            VM((n, CH, QKV), BF16),
            VM((ROWS, QKV), F32),
            pltpu.SemaphoreType.DMA((3, n)),
        ]
        args = (*ds, res, w_out, *qkv_weights)
        flops += 2 * ROWS * D * QKV
    else:
        out_shape = sds((ROWS, D))
        out_specs = VSPEC
        extra = []
        args = (*ds, res, w_out)
    return pl.pallas_call(
        functools.partial(out_kernel, layer, fuse),
        out_shape=out_shape,
        in_specs=[VSPEC] * 4 + [ASPEC] * (len(args) - 4),
        out_specs=out_specs,
        scratch_shapes=extra + shared,
        compiler_params=pltpu.CompilerParams(
            vmem_limit_bytes=53 * MIB if fuse else 32 * MIB, collective_id=layer, has_side_effects=True),
        cost_estimate=pl.CostEstimate(flops=flops, bytes_accessed=flops // ROWS, transcendentals=0),
        name=f"out_product_{layer}",
    )(*args)


def swap(parts):
    out = [parts[0]]
    for i in range(1, GROUPS):
        out.append(lax.ppermute(parts[i], "model", [(m, m ^ i) for m in range(GROUPS)]))
    return out


def solution(mesh):
    cache_spec = P(None, ("replica", "model"), None, None)

    def device_step(x, cache_len, w_query, w_key, w_value, w_out, k_cache, v_cache):
        *rs, k_new, v_new = first_qkv(x, w_query, w_key, w_value)
        priors = ()
        for layer in range(2):
            if layer:
                k_out = copy_cache(layer, 0, K_CUT[layer], cache_len, k_new, k_cache, k_out)
                priors = (k_out, v_out)
            *cs, k_out, v_out = attend(layer, cache_len, rs, k_new, v_new, k_cache, v_cache, priors)
            ds = swap(cs)
            v_out = copy_cache(layer, V_CUT[layer], MINE, cache_len, v_new, v_cache, v_out)
            if layer == 0:
                *qs, k_new, v_new, res = out_product(0, True, ds, x, w_out, (w_query, w_key, w_value))
                rs = swap(qs)
            else:
                out = out_product(1, False, ds, res, w_out, ())
        return out, k_out, v_out

    return jax.shard_map(
        device_step,
        mesh=mesh,
        in_specs=(P("replica", None), P("replica"), P(None, None, "model"), P(), P(), P(None, "model", None), cache_spec, cache_spec),
        out_specs=(P("replica", None), cache_spec, cache_spec),
        check_vma=False,
    )
```

```python
import functools

import jax
import jax.numpy as jnp
from jax import lax
from jax.experimental import pallas as pl
from jax.experimental.pallas import tpu as pltpu
from jax.sharding import PartitionSpec as P

F32 = jnp.float32
BF16 = jnp.bfloat16
MIB = 1 << 20
BIG = 50 * MIB

GROUPS = 4
ROWS = 64
MINE = 16
D = 8192
HD = 128
LH = 16
QW = LH * HD
SEQ = 2048
CH = 512
NJ = QW // CH
QKV = QW + 2 * HD
WO_SLOTS = (8, 16)
Q_SLOTS = 12
AHEAD = 4
Q_FIRST = 4
BLK = 256
VM = pltpu.VMEM
VSPEC = pl.BlockSpec(memory_space=pltpu.VMEM)
ASPEC = pl.BlockSpec(memory_space=pltpu.HBM)
SSPEC = pl.BlockSpec(memory_space=pltpu.SMEM)


def sds(shape, dtype=BF16):
    return jax.ShapeDtypeStruct(shape, dtype)


def qkv_copies(layer, chunk, slot, wq, wk, wv, buf, sems):
    rows = pl.ds(pl.multiple_of(chunk * CH, CH), CH)
    return (
        pltpu.make_async_copy(wq.at[layer, rows, :], buf.at[slot, :, pl.ds(0, QW)], sems.at[0, slot]),
        pltpu.make_async_copy(wk.at[layer, rows, :], buf.at[slot, :, pl.ds(QW, HD)], sems.at[1, slot]),
        pltpu.make_async_copy(wv.at[layer, rows, :], buf.at[slot, :, pl.ds(QW + HD, HD)], sems.at[2, slot]),
    )


def write_qkv(me, acc, q_outs, k_new, v_new):
    for i, q_out in enumerate(q_outs):
        other = xor_id(me, i)
        q_out[...] = acc[pl.ds(pl.multiple_of(other * MINE, MINE), MINE), 0:QW].astype(BF16)
    mine = pl.ds(pl.multiple_of(me * MINE, MINE), MINE)
    k_new[...] = acc[mine, QW:QW + HD].astype(BF16)
    v_new[...] = acc[mine, QW + HD:QKV].astype(BF16)


def xor_id(me, i):
    core = lax.rem(me, 2)
    other = me
    if i & 1:
        other = other + 1 - 2 * core
    if i & 2:
        other = lax.rem(other + 2, GROUPS)
    return other


def first_qkv_kernel(x, wq, wk, wv, r0, r1, r2, r3, k_new, v_new,
                     xbuf, wbuf, kvbuf, acc, qbuf, rbuf, x_sem, w_sems, kv_sems, ssems, rsems):
    me = lax.axis_index("model")
    depth = D // NJ

    def cols(n):
        return pl.ds(pl.multiple_of(n * CH, CH), CH)

    def w_copy(step):
        rows = pl.ds(pl.multiple_of(step % NJ * depth, depth), depth)
        return pltpu.make_async_copy(wq.at[0, rows, cols(step // NJ)], wbuf.at[step], w_sems.at[step])

    def send(i, n):
        dev = xor_id(me, i)
        rows = pl.ds(pl.multiple_of(dev * MINE, MINE), MINE)
        return pltpu.make_async_remote_copy(
            src_ref=qbuf.at[rows, cols(n)], dst_ref=rbuf.at[i - 1, :, cols(n)],
            send_sem=ssems.at[i - 1, n], recv_sem=rsems.at[i - 1, n],
            device_id={"model": dev}, device_id_type=pl.DeviceIdType.MESH)

    x_copy = pltpu.make_async_copy(x, xbuf, x_sem)
    x_copy.start()
    kv_copies = [pltpu.make_async_copy(w.at[0], kvbuf.at[:, pl.ds(i * HD, HD)], kv_sems.at[i]) for i, w in enumerate((wk, wv))]

    def start(step, _):
        w_copy(step).start()
        return 0

    lax.fori_loop(0, AHEAD, start, 0)

    barrier = pltpu.get_barrier_semaphore()
    for i in range(1, GROUPS):
        pl.semaphore_signal(barrier, inc=1, device_id={"model": xor_id(me, i)}, device_id_type=pl.DeviceIdType.MESH)
    x_copy.wait()

    def group(n):
        acc[...] = jnp.zeros_like(acc)

        def step(k, _):
            w_copy(n * NJ + k).wait()

            @pl.when(n * NJ + k + AHEAD < NJ * NJ)
            def _():
                w_copy(n * NJ + k + AHEAD).start()
            part = xbuf[:, pl.ds(pl.multiple_of(k * depth, depth), depth)]
            acc[...] += jnp.dot(part, wbuf[n * NJ + k], preferred_element_type=F32)
            return 0

        lax.fori_loop(0, NJ, step, 0)
        qbuf[:, cols(n)] = acc[...].astype(BF16)

    def leave(n):
        for i in (3, 2, 1):
            send(i, n).start()

    group(0)
    pl.semaphore_wait(barrier, GROUPS - 1)
    leave(0)

    def later(n, _):
        @pl.when(n == NJ - 1)
        def _():
            for cp in kv_copies:
                cp.start()
        group(n)
        leave(n)
        return 0

    lax.fori_loop(1, NJ, later, 0)
    mine = pl.ds(pl.multiple_of(me * MINE, MINE), MINE)
    for cp in kv_copies:
        cp.wait()
    kv = jnp.zeros((MINE, 2 * HD), F32)
    for k in range(NJ):
        kv += jnp.dot(xbuf[mine, k * depth:(k + 1) * depth], kvbuf[k * depth:(k + 1) * depth, :], preferred_element_type=F32)
    k_new[...] = kv[:, :HD].astype(BF16)
    v_new[...] = kv[:, HD:].astype(BF16)
    r0[...] = qbuf[mine, :]
    for i, r in ((1, r1), (2, r2), (3, r3)):
        for n in range(NJ):
            send(i, n).wait_recv()
        r[...] = rbuf[i - 1]

    def drain(n, _):
        for i in range(1, GROUPS):
            send(i, n).wait_send()
        return 0

    lax.fori_loop(0, NJ, drain, 0)


def first_qkv(x, wq, wk, wv):
    return pl.pallas_call(
        first_qkv_kernel,
        out_shape=[sds((MINE, QW))] * 4 + [sds((MINE, HD))] * 2,
        in_specs=[ASPEC] * 4,
        out_specs=[VSPEC] * 6,
        scratch_shapes=[
            VM((ROWS, D), BF16),
            VM((NJ * NJ, D // NJ, CH), BF16),
            VM((D, 2 * HD), BF16),
            VM((ROWS, CH), F32),
            VM((ROWS, QW), BF16),
            VM((GROUPS - 1, MINE, QW), BF16),
            pltpu.SemaphoreType.DMA,
            pltpu.SemaphoreType.DMA((NJ * NJ,)),
            pltpu.SemaphoreType.DMA((2,)),
            pltpu.SemaphoreType.DMA((GROUPS - 1, NJ)),
            pltpu.SemaphoreType.DMA((GROUPS - 1, NJ)),
        ],
        compiler_params=pltpu.CompilerParams(vmem_limit_bytes=53 * MIB, collective_id=2, has_side_effects=True),
        cost_estimate=pl.CostEstimate(flops=2 * ROWS * D * QKV, bytes_accessed=2 * D * QKV, transcendentals=0),
        name="first_qkv",
    )(x, wq, wk, wv)


K_CUT = (0, 6)
V_CUT = (16, 16)
READ_AHEAD = 2


def put_row(buf, b, length, row):
    base = pl.multiple_of((length // 16) * 16, 16)
    here = lax.broadcasted_iota(jnp.int32, (16, HD), 0) == length - base
    buf[b, pl.ds(base, 16), :] = jnp.where(here, row, buf[b, pl.ds(base, 16), :])


class Share:
    def __init__(self, layer, first, last, lens, new, src, dst, buf, in_sems, out_sems):
        self.layer, self.first, self.count = layer, first, last - first
        self.lens, self.new, self.src, self.dst, self.buf = lens, new, src, dst, buf
        self.in_sems, self.out_sems = in_sems, out_sems

    def take(self, n):
        return pltpu.make_async_copy(self.src.at[self.layer, self.first + n], self.buf.at[n], self.in_sems.at[n])

    def give(self, n):
        return pltpu.make_async_copy(self.buf.at[n], self.dst.at[self.layer, self.first + n], self.out_sems.at[n])

    def start(self):
        for n in range(self.count):
            self.take(n).start()

    def forward(self, n):
        me = lax.axis_index("model")
        self.take(n).wait()
        b = self.first + n
        put_row(self.buf, n, self.lens[me * MINE + b], self.new[pl.ds(b, 1), :])
        if n:
            self.give(n - 1).start()
        if n == self.count - 1:
            self.give(n).start()

    def finish(self):
        for n in range(self.count):
            self.give(n).wait()

    @staticmethod
    def scratch(first, last):
        return [VM((last - first, SEQ, HD), BF16), pltpu.SemaphoreType.DMA((last - first,)),
                pltpu.SemaphoreType.DMA((last - first,))]


def copy_kernel(layer, first, last, n_in, *refs):
    lens, new, src = refs[:3]
    share = Share(layer, first, last, lens, new, src, *refs[n_in:])
    share.start()
    for n in range(share.count):
        share.forward(n)
    share.finish()


def copy_cache(layer, first, last, lens, new, src, prior):
    args = [lens, new, src] + ([prior] if prior is not None else [])
    return pl.pallas_call(
        functools.partial(copy_kernel, layer, first, last, len(args)),
        out_shape=sds(src.shape),
        in_specs=[SSPEC, VSPEC, ASPEC] + ([ASPEC] if prior is not None else []),
        out_specs=ASPEC,
        input_output_aliases={3: 0} if prior is not None else {},
        scratch_shapes=Share.scratch(first, last),
        compiler_params=pltpu.CompilerParams(vmem_limit_bytes=BIG),
        cost_estimate=pl.CostEstimate(flops=5_000_000_000, bytes_accessed=4 * MINE * SEQ * HD, transcendentals=0),
        name=f"copy_cache_{layer}",
    )(*args)


GRP = 8
TIERS = (512, 1024, 2048)


def attend_kernel(layer, n_in, *refs):
    lens, r0, r1, r2, r3, k_new, v_new, k_cache, v_cache = refs[:9]
    c0, c1, c2, c3, k_out, v_out, kbuf, vbuf, qbuf, cbuf, new_kv, ksems, vsems, ko_sems, vo_sems = refs[n_in:]
    me = lax.axis_index("model")
    n_heads = GROUPS * LH
    scale = HD ** -0.5
    caches = ((k_cache, kbuf, ksems, k_out, ko_sems, K_CUT[layer], MINE), (v_cache, vbuf, vsems, v_out, vo_sems, 0, V_CUT[layer]))

    def length(b):
        return lens[me * MINE + b]

    def tier_of(b, n):
        return jnp.logical_and(length(b) < TIERS[n], length(b) >= (TIERS[n - 1] if n else BLK))

    def reads(b, act):
        for cache, buf, sems, _, _, first, last in caches:
            def part(start, size, cache=cache, buf=buf, sems=sems):
                cut = pl.ds(start, size)
                return pltpu.make_async_copy(cache.at[layer, b, cut, :], buf.at[b, cut, :], sems.at[b, min(start, 1)])

            @pl.when(jnp.logical_and(b >= first, b < last))
            def _(part=part):
                act(part(0, SEQ))

            @pl.when(jnp.logical_or(b < first, b >= last))
            def _(part=part):
                act(part(0, BLK))
                for n, size in enumerate(TIERS):
                    @pl.when(tier_of(b, n))
                    def _(size=size):
                        act(part(BLK, size - BLK))

    def writes(b, act):
        for _, buf, _, out, sems, first, last in caches:
            @pl.when(jnp.logical_and(b >= first, b < last))
            def _(buf=buf, out=out, sems=sems):
                act(pltpu.make_async_copy(buf.at[b], out.at[layer, b], sems.at[b]))

    def each(g, do):
        for i in range(GRP):
            do(g * GRP + i)

    def start_group(g, _):
        each(g, lambda b: reads(b, lambda cp: cp.start()))
        return 0

    lax.fori_loop(0, READ_AHEAD, start_group, 0)
    for i, r in enumerate((r0, r1, r2, r3)):
        qbuf[:, i * LH:(i + 1) * LH, :] = r[...].reshape(MINE, LH, HD)
    for b in range(MINE):
        new_kv[0, b] = k_new[b:b + 1, :].astype(F32)
        new_kv[1, b] = v_new[b:b + 1, :].astype(F32)

    def context(seqs, size):
        scores = []
        for b in seqs:
            s = lax.dot_general(qbuf[b], kbuf[b, 0:size, :], (((1,), (1,)), ((), ())), preferred_element_type=F32)
            pos = lax.broadcasted_iota(jnp.int32, (n_heads, size), 1)
            scores.append(jnp.where(pos <= length(b), s * scale, -jnp.inf))
        expos = [jnp.exp(s - jnp.max(s, axis=1, keepdims=True)) for s in scores]
        probs = [(e * (1.0 / jnp.sum(e, axis=1, keepdims=True))).astype(BF16) for e in expos]
        for b, p in zip(seqs, probs):
            cbuf[b] = jnp.dot(p, vbuf[b, 0:size, :], preferred_element_type=F32).astype(BF16)

    def ready(b):
        reads(b, lambda cp: cp.wait())
        put_row(kbuf, b, length(b), new_kv[0, b].astype(BF16))
        put_row(vbuf, b, length(b), new_kv[1, b].astype(BF16))

    def long_one(b, _):
        for n, size in enumerate(TIERS):
            @pl.when(tier_of(b, n))
            def _(size=size):
                context((b,), size)
        return 0

    def group(g, _):
        each(g, ready)

        @pl.when(g + READ_AHEAD < MINE // GRP)
        def _():
            start_group(g + READ_AHEAD, 0)
        context([g * GRP + i for i in range(GRP)], BLK)
        each(g, lambda b: writes(b, lambda cp: cp.start()))
        lax.fori_loop(g * GRP, (g + 1) * GRP, long_one, 0)
        return 0

    lax.fori_loop(0, MINE // GRP, group, 0)
    for i, c in enumerate((c0, c1, c2, c3)):
        c[...] = cbuf[:, i * LH:(i + 1) * LH, :].reshape(MINE, QW)

    def finish(b, _):
        writes(b, lambda cp: cp.wait())
        return 0

    lax.fori_loop(0, MINE, finish, 0)


def attend(layer, lens, rs, k_new, v_new, k_cache, v_cache, priors):
    args = [lens, *rs, k_new, v_new, k_cache, v_cache, *priors]
    return pl.pallas_call(
        functools.partial(attend_kernel, layer, len(args)),
        out_shape=[sds((MINE, QW))] * 4 + [sds(k_cache.shape)] * 2,
        in_specs=[SSPEC] + [VSPEC] * 6 + [ASPEC] * (len(args) - 7),
        out_specs=[VSPEC] * 4 + [ASPEC] * 2,
        input_output_aliases={9: 4, 10: 5} if priors else {},
        scratch_shapes=[
            VM((MINE, SEQ, HD), BF16),
            VM((MINE, SEQ, HD), BF16),
            VM((MINE, GROUPS * LH, HD), BF16),
            VM((MINE, GROUPS * LH, HD), BF16),
            VM((2, MINE, 1, HD), F32),
            pltpu.SemaphoreType.DMA((MINE, 2)),
            pltpu.SemaphoreType.DMA((MINE, 2)),
            pltpu.SemaphoreType.DMA((MINE,)),
            pltpu.SemaphoreType.DMA((MINE,)),
        ],
        compiler_params=pltpu.CompilerParams(vmem_limit_bytes=BIG),
        cost_estimate=pl.CostEstimate(flops=5_000_000_000, bytes_accessed=8 * MIB, transcendentals=0),
        name=f"attend_{layer}",
    )(*args)


def out_kernel(layer, fuse, *refs):
    c_refs, (res, wo), refs = refs[:4], refs[4:6], refs[6:]
    if fuse:
        (wq, wk, wv), outs, refs = refs[:3], refs[3:10], refs[10:]
        q_outs, (k_new, v_new, res_out) = outs[:4], outs[4:]
        hid, qbuf, acc, q_sems = refs[:4]
        refs = refs[4:]
    else:
        hid, refs = refs[0], refs[1:]
    ctx, resv, wbuf, send_a, recv_a, send_c, recv_c, send_b, recv_b, own, w_sems, res_sem, ssems, rsems = refs

    me = lax.axis_index("model")
    n_wo = WO_SLOTS[layer]
    partner, cross, diag = xor_id(me, 1), xor_id(me, 2), xor_id(me, 3)

    def cols(chunk):
        return pl.ds(pl.multiple_of(chunk * CH, CH), CH)

    def wo_copy(step):
        chip_of = lax.rem(lax.div(me, 2) + 1 - step // (2 * NJ), 2)
        core_of = lax.rem(lax.rem(me, 2) + 1 - step % 2, 2)
        chunk = (chip_of * 2 + core_of) * NJ + step % (2 * NJ) // 2
        slot = step % n_wo
        return pltpu.make_async_copy(wo.at[layer, :, cols(chunk)], wbuf.at[slot], w_sems.at[slot])

    def q_copies(slot):
        chip_of = lax.rem(lax.div(me, 2) + slot // (2 * NJ), 2)
        core_of = lax.rem(lax.rem(me, 2) + slot % 2, 2)
        chunk = (chip_of * 2 + core_of) * NJ + slot % (2 * NJ) // 2
        return qkv_copies(layer + 1, chunk, slot % Q_SLOTS, wq, wk, wv, qbuf, q_sems)

    def start_q(slot):
        for cp in q_copies(slot):
            cp.start()

    def send(kind, j, src, dst, dev):
        return pltpu.make_async_remote_copy(
            src_ref=src, dst_ref=dst, send_sem=ssems.at[kind, j], recv_sem=rsems.at[kind, j],
            device_id={"model": dev}, device_id_type=pl.DeviceIdType.MESH)

    half = ROWS // 2

    def rows_of(h):
        return pl.ds(pl.multiple_of(lax.rem(lax.div(me, 2) + h, 2) * half, half), half)

    def context(i):
        there = ctx.at[pl.ds(pl.multiple_of(me * MINE, MINE), MINE), :]
        return send(6, i, c_refs[i], there, xor_id(me, i))

    def pair_a(t):
        part = (t % NJ, rows_of(t // NJ))
        return send(0, t, send_a.at[part], recv_a.at[part], partner)

    def pair_b(j):
        return send(1, j, send_b.at[j], recv_b.at[j], partner)

    def across(t):
        part = (t % NJ, rows_of(t // NJ))
        return send(2, t, send_c.at[part], recv_c.at[part], cross)

    def across_here(t):
        part = (t % NJ, rows_of(1 - t // NJ))
        return send(2, t, send_c.at[part], recv_c.at[part], cross)

    def hidden(kind, j, owner, dev):
        part = hid.at[:, cols(owner * NJ + j)]
        return send(kind, j, part, part, dev)

    def start_wo(step, _):
        wo_copy(step).start()
        return 0

    lax.fori_loop(0, n_wo, start_wo, 0)
    if fuse:
        res_copy = pltpu.make_async_copy(
            res.at[:, pl.ds(pl.multiple_of(me * QW, QW), QW)], resv, res_sem)
    else:
        res_copy = pltpu.make_async_copy(res, resv, res_sem)
    res_copy.start()

    ctx[pl.ds(pl.multiple_of(me * MINE, MINE), MINE), :] = c_refs[0][...]
    if fuse:
        acc[...] = jnp.zeros_like(acc)
        for slot in range(Q_FIRST):
            start_q(slot)

    barrier = pltpu.get_barrier_semaphore()
    for i in range(1, GROUPS):
        pl.semaphore_signal(barrier, inc=1, device_id={"model": xor_id(me, i)}, device_id_type=pl.DeviceIdType.MESH)
    pl.semaphore_wait(barrier, GROUPS - 1)
    for i in (1, 2, 3):
        context(i).start()

    def part_sum(step):
        wo_copy(step).wait()
        part = jnp.dot(ctx[...], wbuf[step % n_wo], preferred_element_type=F32)
        return part

    def refill(step):
        if n_wo < 4 * NJ:
            @pl.when(step + n_wo < 4 * NJ)
            def _():
                wo_copy(step + n_wo).start()
        if fuse:
            @pl.when(step >= 2 * NJ)
            def _():
                start_q(step - 2 * NJ + Q_FIRST)

    def send_across(t):
        part = (t % NJ, rows_of(t // NJ))
        pair_a(t).wait_recv()
        send_c[part] += recv_a[part]
        across(t).start()

    def half_sum(step, h):
        @pl.when(h == 0)
        def _():
            wo_copy(step).wait()
        return jnp.dot(ctx[rows_of(h), :], wbuf[step], preferred_element_type=F32)

    context(1).wait_recv()

    def phase_a(t, _):
        h, j = t // NJ, t % NJ

        @pl.when(t == NJ)
        def _():
            context(2).wait_recv()
            context(3).wait_recv()
        send_a[j, rows_of(h), :] = half_sum(2 * j, h)
        pair_a(t).start()

        @pl.when(t > 0)
        def _():
            send_across(t - 1)
        send_c[j, rows_of(h), :] = half_sum(2 * j + 1, h)

        @pl.when(h == 1)
        def _():
            refill(2 * j)
            refill(2 * j + 1)
        return 0

    lax.fori_loop(0, 2 * NJ, phase_a, 0)
    send_across(2 * NJ - 1)

    def phase_b(j, _):
        step = 2 * NJ + 2 * j
        send_b[j] = part_sum(step)
        pair_b(j).start()
        refill(step)
        own[j] = part_sum(step + 1)
        refill(step + 1)
        return 0

    lax.fori_loop(0, NJ, phase_b, 0)
    res_copy.wait()

    def next_q(owner, j, slot):
        if fuse:
            chunk = owner * NJ + j
            for cp in q_copies(slot):
                cp.wait()

            acc[...] += jnp.dot(hid[:, cols(chunk)], qbuf[slot % Q_SLOTS], preferred_element_type=F32)

            @pl.when(slot + Q_SLOTS < 4 * NJ)
            def _():
                start_q(slot + Q_SLOTS)

    def from_partner(j):
        hidden(3, j, partner, partner).wait_recv()
        next_q(partner, j, 2 * j + 1)

    def phase_c(j, _):
        pair_b(j).wait_recv()
        across_here(j).wait_recv()
        across_here(j + NJ).wait_recv()
        total = own[j] + recv_b[j] + recv_c[j]
        part = (resv[:, cols(j)].astype(F32) + total).astype(BF16)
        hid[:, cols(me * NJ + j)] = part
        if fuse:
            res_out[:, cols(j)] = part
        hidden(4, j, me, cross).start()
        hidden(3, j, me, partner).start()
        next_q(me, j, 2 * j)

        @pl.when(j > 0)
        def _():
            from_partner(j - 1)
        return 0

    lax.fori_loop(0, NJ, phase_c, 0)
    from_partner(NJ - 1)

    def forwarded(j):
        hidden(5, j, diag, partner).wait_recv()
        next_q(diag, j, 2 * NJ + 2 * j + 1)

    def phase_d(j, _):
        hidden(4, j, cross, cross).wait_recv()
        hidden(5, j, cross, partner).start()
        next_q(cross, j, 2 * NJ + 2 * j)

        @pl.when(j > 0)
        def _():
            forwarded(j - 1)
        return 0

    lax.fori_loop(0, NJ, phase_d, 0)
    forwarded(NJ - 1)

    if fuse:
        write_qkv(me, acc, q_outs, k_new, v_new)

    for i in (1, 2, 3):
        context(i).wait_send()

    def drain(j, _):
        for t in (j, j + NJ):
            pair_a(t).wait_send()
            across(t).wait_send()
        pair_b(j).wait_send()
        hidden(3, j, me, partner).wait_send()
        hidden(4, j, me, cross).wait_send()
        hidden(5, j, cross, partner).wait_send()
        return 0

    lax.fori_loop(0, NJ, drain, 0)


def out_product(layer, fuse, cs, res, w_out, qkv_weights):
    part = (NJ, ROWS, CH)
    shared = [
        VM((ROWS, QW), BF16),
        VM((ROWS, QW), BF16),
        VM((WO_SLOTS[layer], QW, CH), BF16),
        VM(part, F32), VM(part, F32), VM(part, F32), VM(part, F32), VM(part, F32), VM(part, F32), VM(part, F32),
        pltpu.SemaphoreType.DMA((WO_SLOTS[layer],)),
        pltpu.SemaphoreType.DMA,
        pltpu.SemaphoreType.DMA((7, 2 * NJ)),
        pltpu.SemaphoreType.DMA((7, 2 * NJ)),
    ]
    flops = 2 * ROWS * QW * D
    if fuse:
        out_shape = [sds((MINE, QW))] * 4 + [sds((MINE, HD))] * 2 + [sds((ROWS, QW))]
        out_specs = [VSPEC] * 7
        extra = [
            VM((ROWS, D), BF16),
            VM((Q_SLOTS, CH, QKV), BF16),
            VM((ROWS, QKV), F32),
            pltpu.SemaphoreType.DMA((3, Q_SLOTS)),
        ]
        args = (*cs, res, w_out, *qkv_weights)
        flops += 2 * ROWS * D * QKV
    else:
        out_shape = sds((ROWS, D))
        out_specs = VSPEC
        extra = []
        args = (*cs, res, w_out)
    return pl.pallas_call(
        functools.partial(out_kernel, layer, fuse),
        out_shape=out_shape,
        in_specs=[VSPEC] * 4 + [ASPEC] * (len(args) - 4),
        out_specs=out_specs,
        scratch_shapes=extra + shared,
        compiler_params=pltpu.CompilerParams(
            vmem_limit_bytes=53 * MIB if fuse else 44 * MIB, collective_id=layer, has_side_effects=True),
        cost_estimate=pl.CostEstimate(flops=flops, bytes_accessed=flops // ROWS, transcendentals=0),
        name=f"out_product_{layer}",
    )(*args)


def swap(parts):
    out = [parts[0]]
    for i in range(1, GROUPS):
        out.append(lax.ppermute(parts[i], "model", [(m, m ^ i) for m in range(GROUPS)]))
    return out


def solution(mesh):
    cache_spec = P(None, ("replica", "model"), None, None)

    def device_step(x, cache_len, w_query, w_key, w_value, w_out, k_cache, v_cache):
        *rs, k_new, v_new = first_qkv(x, w_query, w_key, w_value)
        priors = ()
        for layer in range(2):
            if layer:
                k_out = copy_cache(layer, 0, K_CUT[layer], cache_len, k_new, k_cache, k_out)
                priors = (k_out, v_out)
            *cs, k_out, v_out = attend(layer, cache_len, rs, k_new, v_new, k_cache, v_cache, priors)
            if layer == 0:
                *qs, k_new, v_new, res = out_product(0, True, cs, x, w_out, (w_query, w_key, w_value))
                rs = swap(qs)
            else:
                out = out_product(1, False, cs, res, w_out, ())
        return out, k_out, v_out

    return jax.shard_map(
        device_step,
        mesh=mesh,
        in_specs=(P("replica", None), P("replica"), P(None, None, "model"), P(), P(), P(None, "model", None), cache_spec, cache_spec),
        out_specs=(P("replica", None), cache_spec, cache_spec),
        check_vma=False,
    )
```

```python
import functools

import jax
import jax.numpy as jnp
from jax import lax
from jax.experimental import pallas as pl
from jax.experimental.pallas import tpu as pltpu
from jax.sharding import PartitionSpec as P

F32 = jnp.float32
BF16 = jnp.bfloat16
MIB = 1 << 20
BIG = 42 * MIB

GROUPS = 4
ROWS = 64
MINE = 16
D = 8192
HD = 128
LH = 16
QW = LH * HD
SEQ = 2048
CH = 512
NJ = QW // CH
QKV = QW + 2 * HD
WO_SLOTS = (8, 16)
Q_SLOTS = 8
AHEAD = 4
Q_FIRST = 4
BLK = 256
VM = pltpu.VMEM
VSPEC = pl.BlockSpec(memory_space=pltpu.VMEM)
ASPEC = pl.BlockSpec(memory_space=pltpu.HBM)
SSPEC = pl.BlockSpec(memory_space=pltpu.SMEM)


def sds(shape, dtype=BF16):
    return jax.ShapeDtypeStruct(shape, dtype)


def qkv_copies(layer, chunk, slot, wq, wk, wv, buf, sems):
    rows = pl.ds(pl.multiple_of(chunk * CH, CH), CH)
    return (
        pltpu.make_async_copy(wq.at[layer, rows, :], buf.at[slot, :, pl.ds(0, QW)], sems.at[0, slot]),
        pltpu.make_async_copy(wk.at[layer, rows, :], buf.at[slot, :, pl.ds(QW, HD)], sems.at[1, slot]),
        pltpu.make_async_copy(wv.at[layer, rows, :], buf.at[slot, :, pl.ds(QW + HD, HD)], sems.at[2, slot]),
    )


def xor_id(me, i):
    core = lax.rem(me, 2)
    other = me
    if i & 1:
        other = other + 1 - 2 * core
    if i & 2:
        other = lax.rem(other + 2, GROUPS)
    return other


def read_keys(layer, k_cache, keys, sems, act):
    for b in range(MINE):
        act(pltpu.make_async_copy(k_cache.at[layer, b], keys.at[b], sems.at[b]))


def first_qkv_kernel(x, wq, wk, wv, k_cache, r0, r1, r2, r3, k_new, v_new, keys,
                     xbuf, wbuf, kvbuf, acc, qbuf, rbuf, x_sem, w_sems, kv_sems, k_sems, ssems, rsems):
    me = lax.axis_index("model")
    depth = D // NJ

    def cols(n):
        return pl.ds(pl.multiple_of(n * CH, CH), CH)

    def w_copy(step):
        rows = pl.ds(pl.multiple_of(step % NJ * depth, depth), depth)
        return pltpu.make_async_copy(wq.at[0, rows, cols(step // NJ)], wbuf.at[step], w_sems.at[step])

    def send(i, n):
        dev = xor_id(me, i)
        rows = pl.ds(pl.multiple_of(dev * MINE, MINE), MINE)
        return pltpu.make_async_remote_copy(
            src_ref=qbuf.at[rows, cols(n)], dst_ref=rbuf.at[i - 1, :, cols(n)],
            send_sem=ssems.at[i - 1, n], recv_sem=rsems.at[i - 1, n],
            device_id={"model": dev}, device_id_type=pl.DeviceIdType.MESH)

    x_copy = pltpu.make_async_copy(x, xbuf, x_sem)
    x_copy.start()
    kv_copies = [pltpu.make_async_copy(w.at[0], kvbuf.at[:, pl.ds(i * HD, HD)], kv_sems.at[i]) for i, w in enumerate((wk, wv))]

    def start(step, _):
        w_copy(step).start()
        return 0

    lax.fori_loop(0, AHEAD, start, 0)

    barrier = pltpu.get_barrier_semaphore()
    for i in range(1, GROUPS):
        pl.semaphore_signal(barrier, inc=1, device_id={"model": xor_id(me, i)}, device_id_type=pl.DeviceIdType.MESH)
    x_copy.wait()

    def group(n):
        acc[...] = jnp.zeros_like(acc)

        def step(k, _):
            w_copy(n * NJ + k).wait()

            @pl.when(n * NJ + k + AHEAD < NJ * NJ)
            def _():
                w_copy(n * NJ + k + AHEAD).start()

            @pl.when(n * NJ + k == NJ * NJ - 1)
            def _():
                read_keys(0, k_cache, keys, k_sems, lambda cp: cp.start())
            part = xbuf[:, pl.ds(pl.multiple_of(k * depth, depth), depth)]
            acc[...] += jnp.dot(part, wbuf[n * NJ + k], preferred_element_type=F32)
            return 0

        lax.fori_loop(0, NJ, step, 0)
        qbuf[:, cols(n)] = acc[...].astype(BF16)

    def leave(n):
        for i in (3, 2, 1):
            send(i, n).start()

    group(0)
    pl.semaphore_wait(barrier, GROUPS - 1)
    leave(0)

    def later(n, _):
        @pl.when(n == NJ - 1)
        def _():
            for cp in kv_copies:
                cp.start()
        group(n)
        leave(n)
        return 0

    lax.fori_loop(1, NJ, later, 0)
    mine = pl.ds(pl.multiple_of(me * MINE, MINE), MINE)
    for cp in kv_copies:
        cp.wait()
    kv = jnp.zeros((MINE, 2 * HD), F32)
    for k in range(NJ):
        kv += jnp.dot(xbuf[mine, k * depth:(k + 1) * depth], kvbuf[k * depth:(k + 1) * depth, :], preferred_element_type=F32)
    k_new[...] = kv[:, :HD].astype(BF16)
    v_new[...] = kv[:, HD:].astype(BF16)
    r0[...] = qbuf[mine, :]
    for i, r in ((1, r1), (2, r2), (3, r3)):
        for n in range(NJ):
            send(i, n).wait_recv()
        r[...] = rbuf[i - 1]
    read_keys(0, k_cache, keys, k_sems, lambda cp: cp.wait())

    def drain(n, _):
        for i in range(1, GROUPS):
            send(i, n).wait_send()
        return 0

    lax.fori_loop(0, NJ, drain, 0)


def first_qkv(x, wq, wk, wv, k_cache):
    return pl.pallas_call(
        first_qkv_kernel,
        out_shape=[sds((MINE, QW))] * 4 + [sds((MINE, HD))] * 2 + [VM((MINE, SEQ, HD), BF16)],
        in_specs=[ASPEC] * 5,
        out_specs=[VSPEC] * 7,
        scratch_shapes=[
            VM((ROWS, D), BF16),
            VM((NJ * NJ, D // NJ, CH), BF16),
            VM((D, 2 * HD), BF16),
            VM((ROWS, CH), F32),
            VM((ROWS, QW), BF16),
            VM((GROUPS - 1, MINE, QW), BF16),
            pltpu.SemaphoreType.DMA,
            pltpu.SemaphoreType.DMA((NJ * NJ,)),
            pltpu.SemaphoreType.DMA((2,)),
            pltpu.SemaphoreType.DMA((MINE,)),
            pltpu.SemaphoreType.DMA((GROUPS - 1, NJ)),
            pltpu.SemaphoreType.DMA((GROUPS - 1, NJ)),
        ],
        compiler_params=pltpu.CompilerParams(vmem_limit_bytes=BIG, collective_id=2, has_side_effects=True),
        cost_estimate=pl.CostEstimate(flops=2 * ROWS * D * QKV, bytes_accessed=2 * D * QKV, transcendentals=0),
        name="first_qkv",
    )(x, wq, wk, wv, k_cache)


GRP = 8
TIERS = (512, 1024, 2048)


def aligned(length):
    return pl.ds(pl.multiple_of((length // 16) * 16, 16), 16)


def with_row(block, length, row):
    return jnp.where(lax.broadcasted_iota(jnp.int32, (16, HD), 0) == length % 16, row, block)


def attend_kernel(layer, n_in, *refs):
    lens, r0, r1, r2, r3, k_new, v_new, keys, v_cache = refs[:9]
    c0, c1, c2, c3, k_out, v_out, vbuf, qbuf, cbuf, new_kv, patch, v_sems, ko_sems, vo_sems, p_sems = refs[n_in:]
    me = lax.axis_index("model")
    n_heads = GROUPS * LH
    scale = HD ** -0.5

    def length(b):
        return lens[me * MINE + b]

    def tier_of(b, n):
        return jnp.logical_and(length(b) < TIERS[n], length(b) >= (TIERS[n - 1] if n else BLK))

    def v_read(b):
        return pltpu.make_async_copy(v_cache.at[layer, b], vbuf.at[b], v_sems.at[b])

    def v_write(b):
        return pltpu.make_async_copy(vbuf.at[b], v_out.at[layer, b], vo_sems.at[b])

    def k_write(b):
        return pltpu.make_async_copy(keys.at[b], k_out.at[layer, b], ko_sems.at[b])

    def k_patch(b):
        return pltpu.make_async_copy(patch.at[b], k_out.at[layer, b, aligned(length(b)), :], p_sems.at[b])

    def each(do):
        def step(b, _):
            do(b)
            return 0
        lax.fori_loop(0, MINE, step, 0)

    each(lambda b: v_read(b).start())
    each(lambda b: k_write(b).start())
    for i, r in enumerate((r0, r1, r2, r3)):
        qbuf[:, i * LH:(i + 1) * LH, :] = r[...].reshape(MINE, LH, HD)
    for b in range(MINE):
        new_kv[0, b] = k_new[b:b + 1, :].astype(F32)
        new_kv[1, b] = v_new[b:b + 1, :].astype(F32)

    def context(seqs, size):
        scores = []
        for b in seqs:
            s = lax.dot_general(qbuf[b], keys[b, 0:size, :], (((1,), (1,)), ((), ())), preferred_element_type=F32)
            s_new = jnp.sum(qbuf[b].astype(F32) * new_kv[0, b], axis=1, keepdims=True)
            pos = lax.broadcasted_iota(jnp.int32, (n_heads, size), 1)
            s = jnp.where(pos == length(b), s_new, s)
            scores.append(jnp.where(pos <= length(b), s * scale, -jnp.inf))
        expos = [jnp.exp(s - jnp.max(s, axis=1, keepdims=True)) for s in scores]
        probs = [(e * (1.0 / jnp.sum(e, axis=1, keepdims=True))).astype(BF16) for e in expos]
        for b, p in zip(seqs, probs):
            cbuf[b] = jnp.dot(p, vbuf[b, 0:size, :], preferred_element_type=F32).astype(BF16)

    def long_one(b, _):
        for n, size in enumerate(TIERS):
            @pl.when(tier_of(b, n))
            def _(size=size):
                context((b,), size)
        return 0

    def group(g, _):
        seqs = [g * GRP + i for i in range(GRP)]
        for b in seqs:
            rows = aligned(length(b))
            patch[b] = with_row(keys[b, rows, :], length(b), new_kv[0, b].astype(BF16))
            v_read(b).wait()
            vbuf[b, rows, :] = with_row(vbuf[b, rows, :], length(b), new_kv[1, b].astype(BF16))
        context(seqs, BLK)
        for b in seqs:
            v_write(b).start()
            k_write(b).wait()
            k_patch(b).start()
        lax.fori_loop(g * GRP, (g + 1) * GRP, long_one, 0)
        return 0

    lax.fori_loop(0, MINE // GRP, group, 0)
    for i, c in enumerate((c0, c1, c2, c3)):
        c[...] = cbuf[:, i * LH:(i + 1) * LH, :].reshape(MINE, QW)
    each(lambda b: v_write(b).wait())
    each(lambda b: k_patch(b).wait())


def attend(layer, lens, rs, k_new, v_new, keys, v_cache, priors):
    args = [lens, *rs, k_new, v_new, keys, v_cache, *priors]
    return pl.pallas_call(
        functools.partial(attend_kernel, layer, len(args)),
        out_shape=[sds((MINE, QW))] * 4 + [sds(v_cache.shape)] * 2,
        in_specs=[SSPEC] + [VSPEC] * 7 + [ASPEC] * (len(args) - 8),
        out_specs=[VSPEC] * 4 + [ASPEC] * 2,
        input_output_aliases={9: 4, 10: 5} if priors else {},
        scratch_shapes=[
            VM((MINE, SEQ, HD), BF16),
            VM((MINE, GROUPS * LH, HD), BF16),
            VM((MINE, GROUPS * LH, HD), BF16),
            VM((2, MINE, 1, HD), F32),
            VM((MINE, 16, HD), BF16),
            pltpu.SemaphoreType.DMA((MINE,)),
            pltpu.SemaphoreType.DMA((MINE,)),
            pltpu.SemaphoreType.DMA((MINE,)),
            pltpu.SemaphoreType.DMA((MINE,)),
        ],
        compiler_params=pltpu.CompilerParams(vmem_limit_bytes=BIG),
        cost_estimate=pl.CostEstimate(flops=5_000_000_000, bytes_accessed=24 * MIB, transcendentals=0),
        name=f"attend_{layer}",
    )(*args)


def out_kernel(layer, fuse, *refs):
    c_refs, (res, wo), refs = refs[:4], refs[4:6], refs[6:]
    if fuse:
        (wq, wk, wv, k_cache), outs, refs = refs[:4], refs[4:12], refs[12:]
        r_outs, (k_new, v_new, res_out, keys) = outs[:4], outs[4:]
        hid, qbuf, acc, q_all, rbuf, q_sems, k_sems = refs[:7]
        refs = refs[7:]
    else:
        hid, refs = refs[0], refs[1:]
    ctx, resv, wbuf, send_a, recv_a, send_c, recv_c, send_b, recv_b, own, w_sems, res_sem, ssems, rsems = refs

    me = lax.axis_index("model")
    n_wo = WO_SLOTS[layer]
    partner, cross, diag = xor_id(me, 1), xor_id(me, 2), xor_id(me, 3)

    def cols(chunk):
        return pl.ds(pl.multiple_of(chunk * CH, CH), CH)

    def wo_copy(step):
        chip_of = lax.rem(lax.div(me, 2) + 1 - step // (2 * NJ), 2)
        core_of = lax.rem(lax.rem(me, 2) + 1 - step % 2, 2)
        chunk = (chip_of * 2 + core_of) * NJ + step % (2 * NJ) // 2
        slot = step % n_wo
        return pltpu.make_async_copy(wo.at[layer, :, cols(chunk)], wbuf.at[slot], w_sems.at[slot])

    def q_copies(slot):
        chip_of = lax.rem(lax.div(me, 2) + slot // (2 * NJ), 2)
        core_of = lax.rem(lax.rem(me, 2) + slot % 2, 2)
        chunk = (chip_of * 2 + core_of) * NJ + slot % (2 * NJ) // 2
        return qkv_copies(layer + 1, chunk, slot % Q_SLOTS, wq, wk, wv, qbuf, q_sems)

    def start_q(slot):
        for cp in q_copies(slot):
            cp.start()

    def send(kind, j, src, dst, dev):
        return pltpu.make_async_remote_copy(
            src_ref=src, dst_ref=dst, send_sem=ssems.at[kind, j], recv_sem=rsems.at[kind, j],
            device_id={"model": dev}, device_id_type=pl.DeviceIdType.MESH)

    half = ROWS // 2

    def rows_of(h):
        return pl.ds(pl.multiple_of(lax.rem(lax.div(me, 2) + h, 2) * half, half), half)

    def context(i):
        there = ctx.at[pl.ds(pl.multiple_of(me * MINE, MINE), MINE), :]
        return send(6, i, c_refs[i], there, xor_id(me, i))

    def pair_a(t):
        part = (t % NJ, rows_of(t // NJ))
        return send(0, t, send_a.at[part], recv_a.at[part], partner)

    def pair_b(j):
        return send(1, j, send_b.at[j], recv_b.at[j], partner)

    def across(t):
        part = (t % NJ, rows_of(t // NJ))
        return send(2, t, send_c.at[part], recv_c.at[part], cross)

    def across_here(t):
        part = (t % NJ, rows_of(1 - t // NJ))
        return send(2, t, send_c.at[part], recv_c.at[part], cross)

    def hidden(kind, j, owner, dev):
        part = hid.at[:, cols(owner * NJ + j)]
        return send(kind, j, part, part, dev)

    def start_wo(step, _):
        wo_copy(step).start()
        return 0

    lax.fori_loop(0, n_wo, start_wo, 0)
    if fuse:
        res_copy = pltpu.make_async_copy(
            res.at[:, pl.ds(pl.multiple_of(me * QW, QW), QW)], resv, res_sem)
    else:
        res_copy = pltpu.make_async_copy(res, resv, res_sem)
    res_copy.start()

    ctx[pl.ds(pl.multiple_of(me * MINE, MINE), MINE), :] = c_refs[0][...]
    if fuse:
        acc[...] = jnp.zeros_like(acc)
        for slot in range(Q_FIRST):
            start_q(slot)

    barrier = pltpu.get_barrier_semaphore()
    for i in range(1, GROUPS):
        pl.semaphore_signal(barrier, inc=1, device_id={"model": xor_id(me, i)}, device_id_type=pl.DeviceIdType.MESH)
    pl.semaphore_wait(barrier, GROUPS - 1)
    for i in (1, 2, 3):
        context(i).start()

    def part_sum(step):
        wo_copy(step).wait()
        part = jnp.dot(ctx[...], wbuf[step % n_wo], preferred_element_type=F32)
        return part

    def refill(step):
        if n_wo < 4 * NJ:
            @pl.when(step + n_wo < 4 * NJ)
            def _():
                wo_copy(step + n_wo).start()
        if fuse:
            slot = step - 2 * NJ + Q_FIRST

            @pl.when(jnp.logical_and(step >= 2 * NJ, slot < Q_SLOTS))
            def _():
                start_q(slot)

    def send_across(t):
        part = (t % NJ, rows_of(t // NJ))
        pair_a(t).wait_recv()
        send_c[part] += recv_a[part]
        across(t).start()

    def half_sum(step, h):
        @pl.when(h == 0)
        def _():
            wo_copy(step).wait()
        return jnp.dot(ctx[rows_of(h), :], wbuf[step], preferred_element_type=F32)

    context(1).wait_recv()

    def phase_a(t, _):
        h, j = t // NJ, t % NJ

        @pl.when(t == NJ)
        def _():
            context(2).wait_recv()
            context(3).wait_recv()
        send_a[j, rows_of(h), :] = half_sum(2 * j, h)
        pair_a(t).start()

        @pl.when(t > 0)
        def _():
            send_across(t - 1)
        send_c[j, rows_of(h), :] = half_sum(2 * j + 1, h)

        @pl.when(h == 1)
        def _():
            refill(2 * j)
            refill(2 * j + 1)
        return 0

    lax.fori_loop(0, 2 * NJ, phase_a, 0)
    send_across(2 * NJ - 1)

    def phase_b(j, _):
        step = 2 * NJ + 2 * j
        send_b[j] = part_sum(step)
        pair_b(j).start()
        refill(step)
        own[j] = part_sum(step + 1)
        refill(step + 1)
        return 0

    lax.fori_loop(0, NJ, phase_b, 0)
    res_copy.wait()

    def next_q(owner, j, slot):
        if fuse:
            chunk = owner * NJ + j
            for cp in q_copies(slot):
                cp.wait()

            acc[...] += jnp.dot(hid[:, cols(chunk)], qbuf[slot % Q_SLOTS], preferred_element_type=F32)

            @pl.when(slot + Q_SLOTS < 4 * NJ)
            def _():
                start_q(slot + Q_SLOTS)

    def from_partner(j):
        hidden(3, j, partner, partner).wait_recv()
        next_q(partner, j, 2 * j + 1)

    def phase_c(j, _):
        pair_b(j).wait_recv()
        across_here(j).wait_recv()
        across_here(j + NJ).wait_recv()
        total = own[j] + recv_b[j] + recv_c[j]
        part = (resv[:, cols(j)].astype(F32) + total).astype(BF16)
        hid[:, cols(me * NJ + j)] = part
        if fuse:
            res_out[:, cols(j)] = part
        hidden(4, j, me, cross).start()
        hidden(3, j, me, partner).start()
        next_q(me, j, 2 * j)

        @pl.when(j > 0)
        def _():
            from_partner(j - 1)
        return 0

    lax.fori_loop(0, NJ, phase_c, 0)
    from_partner(NJ - 1)

    def forwarded(j):
        hidden(5, j, diag, partner).wait_recv()
        next_q(diag, j, 2 * NJ + 2 * j + 1)

    def phase_d(j, _):
        hidden(4, j, cross, cross).wait_recv()
        hidden(5, j, cross, partner).start()
        next_q(cross, j, 2 * NJ + 2 * j)

        @pl.when(j > 0)
        def _():
            forwarded(j - 1)
        return 0

    lax.fori_loop(0, NJ, phase_d, 0)
    if fuse:
        read_keys(layer + 1, k_cache, keys, k_sems, lambda cp: cp.start())
    forwarded(NJ - 1)

    if fuse:
        def query(i):
            dev = xor_id(me, i)
            rows = pl.ds(pl.multiple_of(dev * MINE, MINE), MINE)
            return send(6, GROUPS + i, q_all.at[rows, :], rbuf.at[i - 1], dev)

        q_all[...] = acc[:, 0:QW].astype(BF16)
        for i in (3, 2, 1):
            query(i).start()
        mine = pl.ds(pl.multiple_of(me * MINE, MINE), MINE)
        k_new[...] = acc[mine, QW:QW + HD].astype(BF16)
        v_new[...] = acc[mine, QW + HD:QKV].astype(BF16)
        r_outs[0][...] = q_all[mine, :]
        for i in (1, 2, 3):
            query(i).wait_recv()
            r_outs[i][...] = rbuf[i - 1]
        read_keys(layer + 1, k_cache, keys, k_sems, lambda cp: cp.wait())
        for i in (1, 2, 3):
            query(i).wait_send()
    for i in (1, 2, 3):
        context(i).wait_send()

    def drain(j, _):
        for t in (j, j + NJ):
            pair_a(t).wait_send()
            across(t).wait_send()
        pair_b(j).wait_send()
        hidden(3, j, me, partner).wait_send()
        hidden(4, j, me, cross).wait_send()
        hidden(5, j, cross, partner).wait_send()
        return 0

    lax.fori_loop(0, NJ, drain, 0)


def out_product(layer, fuse, cs, res, w_out, qkv_weights):
    part = (NJ, ROWS, CH)
    shared = [
        VM((ROWS, QW), BF16),
        VM((ROWS, QW), BF16),
        VM((WO_SLOTS[layer], QW, CH), BF16),
        VM(part, F32), VM(part, F32), VM(part, F32), VM(part, F32), VM(part, F32), VM(part, F32), VM(part, F32),
        pltpu.SemaphoreType.DMA((WO_SLOTS[layer],)),
        pltpu.SemaphoreType.DMA,
        pltpu.SemaphoreType.DMA((7, 2 * NJ)),
        pltpu.SemaphoreType.DMA((7, 2 * NJ)),
    ]
    flops = 2 * ROWS * QW * D
    if fuse:
        out_shape = [sds((MINE, QW))] * 4 + [sds((MINE, HD))] * 2 + [sds((ROWS, QW)), VM((MINE, SEQ, HD), BF16)]
        out_specs = [VSPEC] * 8
        extra = [
            VM((ROWS, D), BF16),
            VM((Q_SLOTS, CH, QKV), BF16),
            VM((ROWS, QKV), F32),
            VM((ROWS, QW), BF16),
            VM((GROUPS - 1, MINE, QW), BF16),
            pltpu.SemaphoreType.DMA((3, Q_SLOTS)),
            pltpu.SemaphoreType.DMA((MINE,)),
        ]
        args = (*cs, res, w_out, *qkv_weights)
        flops += 2 * ROWS * D * QKV
    else:
        out_shape = sds((ROWS, D))
        out_specs = VSPEC
        extra = []
        args = (*cs, res, w_out)
    return pl.pallas_call(
        functools.partial(out_kernel, layer, fuse),
        out_shape=out_shape,
        in_specs=[VSPEC] * 4 + [ASPEC] * (len(args) - 4),
        out_specs=out_specs,
        scratch_shapes=extra + shared,
        compiler_params=pltpu.CompilerParams(
            vmem_limit_bytes=44 * MIB, collective_id=layer, has_side_effects=True),
        cost_estimate=pl.CostEstimate(flops=flops, bytes_accessed=flops // ROWS, transcendentals=0),
        name=f"out_product_{layer}",
    )(*args)


def solution(mesh):
    cache_spec = P(None, ("replica", "model"), None, None)

    def device_step(x, cache_len, w_query, w_key, w_value, w_out, k_cache, v_cache):
        x = pltpu.with_memory_space_constraint(x, pltpu.HBM)
        *rs, k_new, v_new, keys = first_qkv(x, w_query, w_key, w_value, k_cache)
        *cs, k_out, v_out = attend(0, cache_len, rs, k_new, v_new, keys, v_cache, ())
        *rs, k_new, v_new, res, keys = out_product(0, True, cs, x, w_out, (w_query, w_key, w_value, k_cache))
        *cs, k_out, v_out = attend(1, cache_len, rs, k_new, v_new, keys, v_cache, (k_out, v_out))
        out = out_product(1, False, cs, res, w_out, ())
        return out, k_out, v_out

    return jax.shard_map(
        device_step,
        mesh=mesh,
        in_specs=(P("replica", None), P("replica"), P(None, None, "model"), P(), P(), P(None, "model", None), cache_spec, cache_spec),
        out_specs=(P("replica", None), cache_spec, cache_spec),
        check_vma=False,
    )
```

```python
import functools

import jax
import jax.numpy as jnp
from jax import lax
from jax.experimental import pallas as pl
from jax.experimental.pallas import tpu as pltpu
from jax.sharding import PartitionSpec as P

F32 = jnp.float32
BF16 = jnp.bfloat16
MIB = 1 << 20
BIG = 42 * MIB

GROUPS = 4
ROWS = 64
MINE = 16
D = 8192
HD = 128
LH = 16
QW = LH * HD
SEQ = 2048
CH = 512
NJ = QW // CH
QKV = QW + 2 * HD
WO_SLOTS = (8, 16)
Q_SLOTS = 6
AHEAD = 4
Q_FIRST = 4
KEYS_AT = 14
V_HELD = (0, 8)
CACHES_AT = 2
BLK = 256
VM = pltpu.VMEM
VSPEC = pl.BlockSpec(memory_space=pltpu.VMEM)
ASPEC = pl.BlockSpec(memory_space=pltpu.HBM)
SSPEC = pl.BlockSpec(memory_space=pltpu.SMEM)


def sds(shape, dtype=BF16):
    return jax.ShapeDtypeStruct(shape, dtype)


def qkv_copies(layer, chunk, slot, wq, wk, wv, buf, sems):
    rows = pl.ds(pl.multiple_of(chunk * CH, CH), CH)
    return (
        pltpu.make_async_copy(wq.at[layer, rows, :], buf.at[slot, :, pl.ds(0, QW)], sems.at[0, slot]),
        pltpu.make_async_copy(wk.at[layer, rows, :], buf.at[slot, :, pl.ds(QW, HD)], sems.at[1, slot]),
        pltpu.make_async_copy(wv.at[layer, rows, :], buf.at[slot, :, pl.ds(QW + HD, HD)], sems.at[2, slot]),
    )


def xor_id(me, i):
    core = lax.rem(me, 2)
    other = me
    if i & 1:
        other = other + 1 - 2 * core
    if i & 2:
        other = lax.rem(other + 2, GROUPS)
    return other


def read_cache(count, cache, held, sems, act):
    for b in range(count):
        act(pltpu.make_async_copy(cache.at[b], held.at[b], sems.at[b]))


def first_qkv_kernel(x, wq, wk, wv, k_cache, r0, r1, r2, r3, k_new, v_new, keys,
                     xbuf, wbuf, kvbuf, acc, qbuf, rbuf, kvrows, kvback, x_sem, w_sems, kv_sems, k_sems, ssems, rsems):
    me = lax.axis_index("model")
    depth = D // NJ

    def cols(n):
        return pl.ds(pl.multiple_of(n * CH, CH), CH)

    def w_copy(step):
        rows = pl.ds(pl.multiple_of(step % NJ * depth, depth), depth)
        return pltpu.make_async_copy(wq.at[0, rows, cols(step // NJ)], wbuf.at[step], w_sems.at[step])

    def send(i, n):
        dev = xor_id(me, i)
        rows = pl.ds(pl.multiple_of(dev * MINE, MINE), MINE)
        return pltpu.make_async_remote_copy(
            src_ref=qbuf.at[rows, cols(n)], dst_ref=rbuf.at[i - 1, :, cols(n)],
            send_sem=ssems.at[i - 1, n], recv_sem=rsems.at[i - 1, n],
            device_id={"model": dev}, device_id_type=pl.DeviceIdType.MESH)

    x_copy = pltpu.make_async_copy(x, xbuf, x_sem)
    x_copy.start()
    core = lax.rem(me, 2)

    def kv_weight(act):
        for i, w in enumerate((wk, wv)):
            @pl.when(core == i)
            def _(w=w):
                act(pltpu.make_async_copy(w.at[0], kvbuf, kv_sems.at[0]))

    def kv_send():
        rows = pl.ds(pl.multiple_of((1 - core) * MINE, MINE), MINE)
        return pltpu.make_async_remote_copy(
            src_ref=kvrows.at[rows, :], dst_ref=kvback, send_sem=kv_sems.at[1], recv_sem=kv_sems.at[2],
            device_id={"model": xor_id(me, 1)}, device_id_type=pl.DeviceIdType.MESH)


    def start(step, _):
        w_copy(step).start()
        return 0

    lax.fori_loop(0, AHEAD, start, 0)

    barrier = pltpu.get_barrier_semaphore()
    for i in range(1, GROUPS):
        pl.semaphore_signal(barrier, inc=1, device_id={"model": xor_id(me, i)}, device_id_type=pl.DeviceIdType.MESH)
    x_copy.wait()

    def group(n):
        acc[...] = jnp.zeros_like(acc)

        def step(k, _):
            w_copy(n * NJ + k).wait()

            @pl.when(n * NJ + k + AHEAD < NJ * NJ)
            def _():
                w_copy(n * NJ + k + AHEAD).start()

            @pl.when(n * NJ + k == KEYS_AT)
            def _():
                read_cache(MINE, k_cache.at[0], keys, k_sems, lambda cp: cp.start())
            part = xbuf[:, pl.ds(pl.multiple_of(k * depth, depth), depth)]
            acc[...] += jnp.dot(part, wbuf[n * NJ + k], preferred_element_type=F32)
            return 0

        lax.fori_loop(0, NJ, step, 0)
        qbuf[:, cols(n)] = acc[...].astype(BF16)

    def leave(n):
        for i in (3, 2, 1):
            send(i, n).start()

    group(0)
    pl.semaphore_wait(barrier, GROUPS - 1)
    leave(0)

    def later(n, _):
        @pl.when(n == NJ - 1)
        def _():
            kv_weight(lambda cp: cp.start())
        group(n)
        leave(n)
        return 0

    lax.fori_loop(1, NJ, later, 0)
    mine = pl.ds(pl.multiple_of(me * MINE, MINE), MINE)
    kv_weight(lambda cp: cp.wait())
    chip_rows = pl.ds(pl.multiple_of(lax.div(me, 2) * 2 * MINE, 2 * MINE), 2 * MINE)
    kv = jnp.zeros((2 * MINE, HD), F32)
    for k in range(NJ):
        kv += jnp.dot(xbuf[chip_rows, k * depth:(k + 1) * depth], kvbuf[k * depth:(k + 1) * depth, :], preferred_element_type=F32)
    kvrows[...] = kv.astype(BF16)
    kv_send().start()
    r0[...] = qbuf[mine, :]
    for i, r in ((1, r1), (2, r2), (3, r3)):
        for n in range(NJ):
            send(i, n).wait_recv()
        r[...] = rbuf[i - 1]
    kv_send().wait()
    here = kvrows[pl.ds(pl.multiple_of(core * MINE, MINE), MINE), :]
    k_new[...] = jnp.where(core == 0, here, kvback[...])
    v_new[...] = jnp.where(core == 0, kvback[...], here)
    read_cache(MINE, k_cache.at[0], keys, k_sems, lambda cp: cp.wait())

    def drain(n, _):
        for i in range(1, GROUPS):
            send(i, n).wait_send()
        return 0

    lax.fori_loop(0, NJ, drain, 0)


def first_qkv(x, wq, wk, wv, k_cache):
    return pl.pallas_call(
        first_qkv_kernel,
        out_shape=[sds((MINE, QW))] * 4 + [sds((MINE, HD))] * 2 + [VM((MINE, SEQ, HD), BF16)],
        in_specs=[ASPEC] * 5,
        out_specs=[VSPEC] * 7,
        scratch_shapes=[
            VM((ROWS, D), BF16),
            VM((NJ * NJ, D // NJ, CH), BF16),
            VM((D, HD), BF16),
            VM((ROWS, CH), F32),
            VM((ROWS, QW), BF16),
            VM((GROUPS - 1, MINE, QW), BF16),
            VM((2 * MINE, HD), BF16),
            VM((MINE, HD), BF16),
            pltpu.SemaphoreType.DMA,
            pltpu.SemaphoreType.DMA((NJ * NJ,)),
            pltpu.SemaphoreType.DMA((3,)),
            pltpu.SemaphoreType.DMA((MINE,)),
            pltpu.SemaphoreType.DMA((GROUPS - 1, NJ)),
            pltpu.SemaphoreType.DMA((GROUPS - 1, NJ)),
        ],
        compiler_params=pltpu.CompilerParams(vmem_limit_bytes=BIG, collective_id=2, has_side_effects=True),
        cost_estimate=pl.CostEstimate(flops=2 * ROWS * D * QKV, bytes_accessed=2 * D * QKV, transcendentals=0),
        name="first_qkv",
    )(x, wq, wk, wv, k_cache)


GRP = 8
TIERS = (512, 1024, 2048)


def aligned(length):
    return pl.ds(pl.multiple_of((length // 16) * 16, 16), 16)


def with_row(block, length, row):
    return jnp.where(lax.broadcasted_iota(jnp.int32, (16, HD), 0) == length % 16, row, block)


def attend_kernel(layer, n_in, *refs):
    lens, r0, r1, r2, r3, k_new, v_new = refs[:7]
    c0, c1, c2, c3, k_out, v_out, qbuf, cbuf, new_kv, patch, out_sems, patch_sems = refs[n_in:n_in + 12]
    keys = refs[7].at[pl.ds(0, MINE)]
    v_cache = refs[8]
    vbuf, v_sems = refs[n_in + 12:]
    held = V_HELD[layer]
    me = lax.axis_index("model")
    n_heads = GROUPS * LH
    scale = HD ** -0.5

    def value(b, held_group):
        return refs[7].at[MINE + b] if held_group else vbuf.at[b - held]

    def length(b):
        return lens[me * MINE + b]

    def tier_of(b, n):
        return jnp.logical_and(length(b) < TIERS[n], length(b) >= (TIERS[n - 1] if n else BLK))

    def v_read(b):
        return pltpu.make_async_copy(v_cache.at[layer, b], vbuf.at[b - held], v_sems.at[b])

    def k_write(b):
        return pltpu.make_async_copy(keys.at[b], k_out.at[layer, b], out_sems.at[0, b])

    def v_write(b, held_group):
        return pltpu.make_async_copy(value(b, held_group), v_out.at[layer, b], out_sems.at[1, b])

    def put(i, b):
        out = (k_out, v_out)[i]
        return pltpu.make_async_copy(patch.at[i, b], out.at[layer, b, aligned(length(b)), :], patch_sems.at[i, b])

    def each(do, first=0, last=MINE):
        def step(b, _):
            do(b)
            return 0
        lax.fori_loop(first, last, step, 0)

    each(lambda b: v_read(b).start(), held, held + GRP)
    each(lambda b: k_write(b).start())
    if held:
        each(lambda b: v_write(b, True).start(), 0, held)
    each(lambda b: v_read(b).start(), held + GRP, MINE)
    for i, r in enumerate((r0, r1, r2, r3)):
        qbuf[:, i * LH:(i + 1) * LH, :] = r[...].reshape(MINE, LH, HD)
    for b in range(MINE):
        new_kv[0, b] = k_new[b:b + 1, :].astype(F32)
        new_kv[1, b] = v_new[b:b + 1, :].astype(F32)

    def context(seqs, size, held_group):
        scores, news = [], []
        for b in seqs:
            s = lax.dot_general(qbuf[b], keys[b, 0:size, :], (((1,), (1,)), ((), ())), preferred_element_type=F32)
            pos = lax.broadcasted_iota(jnp.int32, (n_heads, size), 1)
            scores.append(jnp.where(pos < length(b), s * scale, -jnp.inf))
            news.append(jnp.sum(qbuf[b].astype(F32) * new_kv[0, b], axis=1, keepdims=True) * scale)
        tops = [jnp.maximum(jnp.max(s, axis=1, keepdims=True), n) for s, n in zip(scores, news)]
        expos = [jnp.exp(s - t) for s, t in zip(scores, tops)]
        news = [jnp.exp(n - t) for n, t in zip(news, tops)]
        invs = [1.0 / (jnp.sum(e, axis=1, keepdims=True) + n) for e, n in zip(expos, news)]
        probs = [(e * i).astype(BF16) for e, i in zip(expos, invs)]
        news = [(n * i).astype(BF16).astype(F32) for n, i in zip(news, invs)]
        for b, p, n in zip(seqs, probs, news):
            old = jnp.dot(p, value(b, held_group)[0:size, :], preferred_element_type=F32)
            cbuf[b] = (old + n * new_kv[1, b]).astype(BF16)

    def settle_keys(b):
        k_write(b).wait()
        put(0, b).start()

    def settle_values(b):
        v_write(b, True).wait()
        put(1, b).start()

    def group(g, held_group):
        seqs = [g * GRP + i for i in range(GRP)]
        for b in seqs:
            rows = aligned(length(b))
            patch[0, b] = with_row(keys[b, rows, :], length(b), new_kv[0, b].astype(BF16))
            if held_group:
                patch[1, b] = with_row(value(b, True)[rows, :], length(b), new_kv[1, b].astype(BF16))
            else:
                v_read(b).wait()
                value(b, False)[rows, :] = with_row(value(b, False)[rows, :], length(b), new_kv[1, b].astype(BF16))
        if not held_group:
            for b in seqs:
                v_write(b, False).start()
        context(seqs, BLK, held_group)
        if g == MINE // GRP - 1:
            each(settle_keys)
            if held:
                each(settle_values, 0, held)

        def long_one(b, _):
            for n, size in enumerate(TIERS):
                @pl.when(tier_of(b, n))
                def _(size=size):
                    context((b,), size, held_group)
            return 0

        lax.fori_loop(g * GRP, (g + 1) * GRP, long_one, 0)

    for g in range(MINE // GRP):
        group(g, g < held // GRP)
    for i, c in enumerate((c0, c1, c2, c3)):
        c[...] = cbuf[:, i * LH:(i + 1) * LH, :].reshape(MINE, QW)
    each(lambda b: v_write(b, False).wait(), held, MINE)
    each(lambda b: put(0, b).wait())
    if held:
        each(lambda b: put(1, b).wait(), 0, held)


def attend(layer, lens, rs, k_new, v_new, held, rest):
    args = [lens, *rs, k_new, v_new, held, *rest]
    return pl.pallas_call(
        functools.partial(attend_kernel, layer, len(args)),
        out_shape=[sds((MINE, QW))] * 4 + [sds((2, MINE, SEQ, HD))] * 2,
        in_specs=[SSPEC] + [VSPEC] * 7 + [ASPEC] * len(rest),
        out_specs=[VSPEC] * 4 + [ASPEC] * 2,
        input_output_aliases={9: 4, 10: 5} if layer else {},
        scratch_shapes=[
            VM((MINE, GROUPS * LH, HD), BF16),
            VM((MINE, GROUPS * LH, HD), BF16),
            VM((2, MINE, 1, HD), F32),
            VM((2, MINE, 16, HD), BF16),
            pltpu.SemaphoreType.DMA((2, MINE)),
            pltpu.SemaphoreType.DMA((2, MINE)),
            VM((MINE - V_HELD[layer], SEQ, HD), BF16),
            pltpu.SemaphoreType.DMA((MINE,)),
        ],
        compiler_params=pltpu.CompilerParams(vmem_limit_bytes=36 * MIB if layer else BIG),
        cost_estimate=pl.CostEstimate(flops=5_000_000_000, bytes_accessed=24 * MIB, transcendentals=0),
        name=f"attend_{layer}",
    )(*args)


def out_kernel(layer, fuse, *refs):
    c_refs, (res, wo), refs = refs[:4], refs[4:6], refs[6:]
    if fuse:
        (wq, wk, wv, k_cache, v_cache), outs, refs = refs[:5], refs[5:13], refs[13:]
        r_outs, (k_new, v_new, res_out, held) = outs[:4], outs[4:]
        hid, qbuf, acc, q_all, rbuf, q_sems, kv_sems = refs[:7]
        refs = refs[7:]
    else:
        hid, refs = refs[0], refs[1:]
    ctx, resv, wbuf, send_a, recv_a, send_c, recv_c, send_b, recv_b, own, w_sems, res_sem, ssems, rsems = refs

    me = lax.axis_index("model")
    n_wo = WO_SLOTS[layer]
    partner, cross, diag = xor_id(me, 1), xor_id(me, 2), xor_id(me, 3)

    def cols(chunk):
        return pl.ds(pl.multiple_of(chunk * CH, CH), CH)

    def wo_copy(step):
        chip_of = lax.rem(lax.div(me, 2) + 1 - step // (2 * NJ), 2)
        core_of = lax.rem(lax.rem(me, 2) + 1 - step % 2, 2)
        chunk = (chip_of * 2 + core_of) * NJ + step % (2 * NJ) // 2
        slot = step % n_wo
        return pltpu.make_async_copy(wo.at[layer, :, cols(chunk)], wbuf.at[slot], w_sems.at[slot])

    def q_copies(slot):
        chip_of = lax.rem(lax.div(me, 2) + slot // (2 * NJ), 2)
        core_of = lax.rem(lax.rem(me, 2) + slot % 2, 2)
        chunk = (chip_of * 2 + core_of) * NJ + slot % (2 * NJ) // 2
        return qkv_copies(layer + 1, chunk, slot % Q_SLOTS, wq, wk, wv, qbuf, q_sems)

    def start_q(slot):
        for cp in q_copies(slot):
            cp.start()

    def send(kind, j, src, dst, dev):
        return pltpu.make_async_remote_copy(
            src_ref=src, dst_ref=dst, send_sem=ssems.at[kind, j], recv_sem=rsems.at[kind, j],
            device_id={"model": dev}, device_id_type=pl.DeviceIdType.MESH)

    half = ROWS // 2

    def rows_of(h):
        return pl.ds(pl.multiple_of(lax.rem(lax.div(me, 2) + h, 2) * half, half), half)

    def context(i):
        there = ctx.at[pl.ds(pl.multiple_of(me * MINE, MINE), MINE), :]
        return send(6, i, c_refs[i], there, xor_id(me, i))

    def pair_a(t):
        part = (t % NJ, rows_of(t // NJ))
        return send(0, t, send_a.at[part], recv_a.at[part], partner)

    def pair_b(j):
        return send(1, j, send_b.at[j], recv_b.at[j], partner)

    def across(t):
        part = (t % NJ, rows_of(t // NJ))
        return send(2, t, send_c.at[part], recv_c.at[part], cross)

    def across_here(t):
        part = (t % NJ, rows_of(1 - t // NJ))
        return send(2, t, send_c.at[part], recv_c.at[part], cross)

    def hidden(kind, j, owner, dev):
        part = hid.at[:, cols(owner * NJ + j)]
        return send(kind, j, part, part, dev)

    def last_half(kind, p, owner, dev):
        part = hid.at[:, pl.ds(pl.multiple_of(owner * QW + QW - CH + p * (CH // 2), CH // 2), CH // 2)]
        return send(kind, NJ - 1 + p, part, part, dev)

    def start_wo(step, _):
        wo_copy(step).start()
        return 0

    lax.fori_loop(0, n_wo, start_wo, 0)
    if fuse:
        res_copy = pltpu.make_async_copy(
            res.at[:, pl.ds(pl.multiple_of(me * QW, QW), QW)], resv, res_sem)
    else:
        res_copy = pltpu.make_async_copy(res, resv, res_sem)
    res_copy.start()

    ctx[pl.ds(pl.multiple_of(me * MINE, MINE), MINE), :] = c_refs[0][...]
    if fuse:
        acc[...] = jnp.zeros_like(acc)
        for slot in range(Q_FIRST):
            start_q(slot)

    barrier = pltpu.get_barrier_semaphore()
    for i in range(1, GROUPS):
        pl.semaphore_signal(barrier, inc=1, device_id={"model": xor_id(me, i)}, device_id_type=pl.DeviceIdType.MESH)
    pl.semaphore_wait(barrier, GROUPS - 1)
    for i in (1, 2, 3):
        context(i).start()

    def part_sum(step):
        wo_copy(step).wait()
        part = jnp.dot(ctx[...], wbuf[step % n_wo], preferred_element_type=F32)
        return part

    def refill(step):
        if n_wo < 4 * NJ:
            @pl.when(step + n_wo < 4 * NJ)
            def _():
                wo_copy(step + n_wo).start()
        if fuse:
            slot = step - 2 * NJ + Q_FIRST

            @pl.when(jnp.logical_and(step >= 2 * NJ, slot < Q_SLOTS))
            def _():
                start_q(slot)

    def send_across(t):
        part = (t % NJ, rows_of(t // NJ))
        pair_a(t).wait_recv()
        send_c[part] += recv_a[part]
        across(t).start()

    def half_sum(step, h):
        @pl.when(h == 0)
        def _():
            wo_copy(step).wait()
        return jnp.dot(ctx[rows_of(h), :], wbuf[step], preferred_element_type=F32)

    context(1).wait_recv()

    def phase_a(t, _):
        h, j = t // NJ, t % NJ

        @pl.when(t == NJ)
        def _():
            context(2).wait_recv()
            context(3).wait_recv()
        send_a[j, rows_of(h), :] = half_sum(2 * j, h)
        pair_a(t).start()

        @pl.when(t > 0)
        def _():
            send_across(t - 1)
        send_c[j, rows_of(h), :] = half_sum(2 * j + 1, h)

        @pl.when(h == 1)
        def _():
            refill(2 * j)
            refill(2 * j + 1)
        return 0

    lax.fori_loop(0, 2 * NJ, phase_a, 0)
    send_across(2 * NJ - 1)

    def phase_b(j, _):
        step = 2 * NJ + 2 * j
        send_b[j] = part_sum(step)
        pair_b(j).start()
        refill(step)
        own[j] = part_sum(step + 1)
        refill(step + 1)
        return 0

    lax.fori_loop(0, NJ, phase_b, 0)
    res_copy.wait()

    def next_q(owner, j, slot):
        if fuse:
            chunk = owner * NJ + j
            for cp in q_copies(slot):
                cp.wait()

            acc[...] += jnp.dot(hid[:, cols(chunk)], qbuf[slot % Q_SLOTS], preferred_element_type=F32)

            @pl.when(slot + Q_SLOTS < 4 * NJ)
            def _():
                start_q(slot + Q_SLOTS)

    def from_partner(j):
        hidden(3, j, partner, partner).wait_recv()
        next_q(partner, j, 2 * j + 1)

    def phase_c(j, _):
        pair_b(j).wait_recv()
        across_here(j).wait_recv()
        across_here(j + NJ).wait_recv()
        total = own[j] + recv_b[j] + recv_c[j]
        part = (resv[:, cols(j)].astype(F32) + total).astype(BF16)
        hid[:, cols(me * NJ + j)] = part
        if fuse:
            res_out[:, cols(j)] = part
        @pl.when(j < NJ - 1)
        def _():
            hidden(4, j, me, cross).start()

        @pl.when(j == NJ - 1)
        def _():
            last_half(4, 0, me, cross).start()
            last_half(4, 1, me, cross).start()
            last_half(5, 1, me, diag).start()
        hidden(3, j, me, partner).start()
        next_q(me, j, 2 * j)

        @pl.when(j > 0)
        def _():
            from_partner(j - 1)
        return 0

    lax.fori_loop(0, NJ, phase_c, 0)
    from_partner(NJ - 1)

    def forwarded(j, last=False):
        if last:
            last_half(5, 0, diag, partner).wait_recv()
            last_half(5, 1, diag, diag).wait_recv()
        else:
            hidden(5, j, diag, partner).wait_recv()
        next_q(diag, j, 2 * NJ + 2 * j + 1)

    def next_caches(act):
        read_cache(MINE, k_cache.at[layer + 1], held, kv_sems.at[0], act)
        read_cache(V_HELD[layer + 1], v_cache.at[layer + 1], held.at[pl.ds(MINE, V_HELD[layer + 1])], kv_sems.at[1], act)

    def phase_d(j, _):
        if fuse:
            @pl.when(j == CACHES_AT)
            def _():
                next_caches(lambda cp: cp.start())
        @pl.when(j < NJ - 1)
        def _():
            hidden(4, j, cross, cross).wait_recv()
            hidden(5, j, cross, partner).start()

        @pl.when(j == NJ - 1)
        def _():
            last_half(4, 0, cross, cross).wait_recv()
            last_half(5, 0, cross, partner).start()
            last_half(4, 1, cross, cross).wait_recv()
        next_q(cross, j, 2 * NJ + 2 * j)

        @pl.when(j > 0)
        def _():
            forwarded(j - 1)
        return 0

    lax.fori_loop(0, NJ, phase_d, 0)
    forwarded(NJ - 1, last=True)

    if fuse:
        def query(i):
            dev = xor_id(me, i)
            rows = pl.ds(pl.multiple_of(dev * MINE, MINE), MINE)
            return send(6, GROUPS + i, q_all.at[rows, :], rbuf.at[i - 1], dev)

        q_all[...] = acc[:, 0:QW].astype(BF16)
        for i in (3, 2, 1):
            query(i).start()
        mine = pl.ds(pl.multiple_of(me * MINE, MINE), MINE)
        k_new[...] = acc[mine, QW:QW + HD].astype(BF16)
        v_new[...] = acc[mine, QW + HD:QKV].astype(BF16)
        r_outs[0][...] = q_all[mine, :]
        for i in (1, 2, 3):
            query(i).wait_recv()
            r_outs[i][...] = rbuf[i - 1]
        next_caches(lambda cp: cp.wait())
        for i in (1, 2, 3):
            query(i).wait_send()
    for i in (1, 2, 3):
        context(i).wait_send()

    def drain(j, _):
        for t in (j, j + NJ):
            pair_a(t).wait_send()
            across(t).wait_send()
        pair_b(j).wait_send()
        hidden(3, j, me, partner).wait_send()

        @pl.when(j < NJ - 1)
        def _():
            hidden(4, j, me, cross).wait_send()
            hidden(5, j, cross, partner).wait_send()
        return 0

    lax.fori_loop(0, NJ, drain, 0)
    last_half(4, 0, me, cross).wait_send()
    last_half(4, 1, me, cross).wait_send()
    last_half(5, 0, cross, partner).wait_send()
    last_half(5, 1, me, diag).wait_send()


def out_product(layer, fuse, cs, res, w_out, qkv_weights):
    part = (NJ, ROWS, CH)
    shared = [
        VM((ROWS, QW), BF16),
        VM((ROWS, QW), BF16),
        VM((WO_SLOTS[layer], QW, CH), BF16),
        VM(part, F32), VM(part, F32), VM(part, F32), VM(part, F32), VM(part, F32), VM(part, F32), VM(part, F32),
        pltpu.SemaphoreType.DMA((WO_SLOTS[layer],)),
        pltpu.SemaphoreType.DMA,
        pltpu.SemaphoreType.DMA((7, 2 * NJ)),
        pltpu.SemaphoreType.DMA((7, 2 * NJ)),
    ]
    flops = 2 * ROWS * QW * D
    if fuse:
        out_shape = [sds((MINE, QW))] * 4 + [sds((MINE, HD))] * 2 + [sds((ROWS, QW)), VM((MINE + V_HELD[1], SEQ, HD), BF16)]
        out_specs = [VSPEC] * 8
        extra = [
            VM((ROWS, D), BF16),
            VM((Q_SLOTS, CH, QKV), BF16),
            VM((ROWS, QKV), F32),
            VM((ROWS, QW), BF16),
            VM((GROUPS - 1, MINE, QW), BF16),
            pltpu.SemaphoreType.DMA((3, Q_SLOTS)),
            pltpu.SemaphoreType.DMA((2, MINE)),
        ]
        args = (*cs, res, w_out, *qkv_weights)
        flops += 2 * ROWS * D * QKV
    else:
        out_shape = sds((ROWS, D))
        out_specs = VSPEC
        extra = []
        args = (*cs, res, w_out)
    return pl.pallas_call(
        functools.partial(out_kernel, layer, fuse),
        out_shape=out_shape,
        in_specs=[VSPEC] * 4 + [ASPEC] * (len(args) - 4),
        out_specs=out_specs,
        scratch_shapes=extra + shared,
        compiler_params=pltpu.CompilerParams(
            vmem_limit_bytes=(39 if fuse else 44) * MIB, collective_id=layer, has_side_effects=True),
        cost_estimate=pl.CostEstimate(flops=flops, bytes_accessed=flops // ROWS, transcendentals=0),
        name=f"out_product_{layer}",
    )(*args)


def solution(mesh):
    cache_spec = P(None, ("replica", "model"), None, None)

    def device_step(x, cache_len, w_query, w_key, w_value, w_out, k_cache, v_cache):
        x, w_key, w_value = (pltpu.with_memory_space_constraint(a, pltpu.HBM) for a in (x, w_key, w_value))
        *rs, k_new, v_new, held = first_qkv(x, w_query, w_key, w_value, k_cache)
        *cs, k_out, v_out = attend(0, cache_len, rs, k_new, v_new, held, (v_cache,))
        *rs, k_new, v_new, res, held = out_product(0, True, cs, x, w_out, (w_query, w_key, w_value, k_cache, v_cache))
        *cs, k_out, v_out = attend(1, cache_len, rs, k_new, v_new, held, (v_cache, k_out, v_out))
        out = out_product(1, False, cs, res, w_out, ())
        return out, k_out, v_out

    return jax.shard_map(
        device_step,
        mesh=mesh,
        in_specs=(P("replica", None), P("replica"), P(None, None, "model"), P(), P(), P(None, "model", None), cache_spec, cache_spec),
        out_specs=(P("replica", None), cache_spec, cache_spec),
        check_vma=False,
    )
```

```python
import functools

import jax
import jax.numpy as jnp
from jax import lax
from jax.experimental import pallas as pl
from jax.experimental.pallas import tpu as pltpu
from jax.sharding import PartitionSpec as P

F32 = jnp.float32
BF16 = jnp.bfloat16
MIB = 1 << 20
BIG = 42 * MIB

GROUPS = 4
ROWS = 64
MINE = 16
D = 8192
HD = 128
LH = 16
QW = LH * HD
SEQ = 2048
CH = 512
NJ = QW // CH
QKV = QW + 2 * HD
WO_SLOTS = (8, 16)
Q_SLOTS = 6
AHEAD = 4
Q_FIRST = 4
KEYS_AT = 14
V_HELD = (0, 8)
CACHES_AT = 2
BLK = 256
VM = pltpu.VMEM
VSPEC = pl.BlockSpec(memory_space=pltpu.VMEM)
ASPEC = pl.BlockSpec(memory_space=pltpu.HBM)
SSPEC = pl.BlockSpec(memory_space=pltpu.SMEM)


def sds(shape, dtype=BF16):
    return jax.ShapeDtypeStruct(shape, dtype)


def qkv_copies(layer, chunk, slot, wq, wk, wv, buf, sems):
    rows = pl.ds(pl.multiple_of(chunk * CH, CH), CH)
    return (
        pltpu.make_async_copy(wq.at[layer, rows, :], buf.at[slot, :, pl.ds(0, QW)], sems.at[0, slot]),
        pltpu.make_async_copy(wk.at[layer, rows, :], buf.at[slot, :, pl.ds(QW, HD)], sems.at[1, slot]),
        pltpu.make_async_copy(wv.at[layer, rows, :], buf.at[slot, :, pl.ds(QW + HD, HD)], sems.at[2, slot]),
    )


def xor_id(me, i):
    core = lax.rem(me, 2)
    other = me
    if i & 1:
        other = other + 1 - 2 * core
    if i & 2:
        other = lax.rem(other + 2, GROUPS)
    return other


def read_cache(count, cache, held, sems, act):
    for b in range(count):
        act(pltpu.make_async_copy(cache.at[b], held.at[b], sems.at[b]))


def first_qkv_kernel(x, wq, wk, wv, k_cache, r0, r1, r2, r3, k_new, v_new, keys,
                     xbuf, wbuf, kvbuf, acc, qbuf, rbuf, kvrows, kvback, x_sem, w_sems, kv_sems, k_sems, ssems, rsems):
    me = lax.axis_index("model")
    depth = D // NJ

    def cols(n):
        return pl.ds(pl.multiple_of(n * CH, CH), CH)

    def w_copy(step):
        rows = pl.ds(pl.multiple_of(step % NJ * depth, depth), depth)
        return pltpu.make_async_copy(wq.at[0, rows, cols(step // NJ)], wbuf.at[step], w_sems.at[step])

    def send(i, n):
        dev = xor_id(me, i)
        rows = pl.ds(pl.multiple_of(dev * MINE, MINE), MINE)
        return pltpu.make_async_remote_copy(
            src_ref=qbuf.at[rows, cols(n)], dst_ref=rbuf.at[i - 1, :, cols(n)],
            send_sem=ssems.at[i - 1, n], recv_sem=rsems.at[i - 1, n],
            device_id={"model": dev}, device_id_type=pl.DeviceIdType.MESH)

    x_copy = pltpu.make_async_copy(x, xbuf, x_sem)
    x_copy.start()
    core = lax.rem(me, 2)

    def kv_weight(act):
        for i, w in enumerate((wk, wv)):
            @pl.when(core == i)
            def _(w=w):
                act(pltpu.make_async_copy(w.at[0], kvbuf, kv_sems.at[0]))

    def kv_send():
        rows = pl.ds(pl.multiple_of((1 - core) * MINE, MINE), MINE)
        return pltpu.make_async_remote_copy(
            src_ref=kvrows.at[rows, :], dst_ref=kvback, send_sem=kv_sems.at[1], recv_sem=kv_sems.at[2],
            device_id={"model": xor_id(me, 1)}, device_id_type=pl.DeviceIdType.MESH)


    def start(step, _):
        w_copy(step).start()
        return 0

    lax.fori_loop(0, AHEAD, start, 0)

    barrier = pltpu.get_barrier_semaphore()
    for i in range(1, GROUPS):
        pl.semaphore_signal(barrier, inc=1, device_id={"model": xor_id(me, i)}, device_id_type=pl.DeviceIdType.MESH)
    x_copy.wait()

    def group(n):
        acc[...] = jnp.zeros_like(acc)

        def step(k, _):
            w_copy(n * NJ + k).wait()

            @pl.when(n * NJ + k + AHEAD < NJ * NJ)
            def _():
                w_copy(n * NJ + k + AHEAD).start()

            @pl.when(n * NJ + k == KEYS_AT)
            def _():
                read_cache(MINE, k_cache.at[0], keys, k_sems, lambda cp: cp.start())
            part = xbuf[:, pl.ds(pl.multiple_of(k * depth, depth), depth)]
            acc[...] += jnp.dot(part, wbuf[n * NJ + k], preferred_element_type=F32)
            return 0

        lax.fori_loop(0, NJ, step, 0)
        qbuf[:, cols(n)] = acc[...].astype(BF16)

    def leave(n):
        for i in (3, 2, 1):
            send(i, n).start()

    group(0)
    pl.semaphore_wait(barrier, GROUPS - 1)
    leave(0)

    def later(n, _):
        @pl.when(n == NJ - 1)
        def _():
            kv_weight(lambda cp: cp.start())
        group(n)
        leave(n)
        return 0

    lax.fori_loop(1, NJ, later, 0)
    mine = pl.ds(pl.multiple_of(me * MINE, MINE), MINE)
    kv_weight(lambda cp: cp.wait())
    chip_rows = pl.ds(pl.multiple_of(lax.div(me, 2) * 2 * MINE, 2 * MINE), 2 * MINE)
    kv = jnp.zeros((2 * MINE, HD), F32)
    for k in range(NJ):
        kv += jnp.dot(xbuf[chip_rows, k * depth:(k + 1) * depth], kvbuf[k * depth:(k + 1) * depth, :], preferred_element_type=F32)
    kvrows[...] = kv.astype(BF16)
    kv_send().start()
    r0[...] = qbuf[mine, :]
    for i, r in ((1, r1), (2, r2), (3, r3)):
        for n in range(NJ):
            send(i, n).wait_recv()
        r[...] = rbuf[i - 1]
    kv_send().wait()
    here = kvrows[pl.ds(pl.multiple_of(core * MINE, MINE), MINE), :]
    k_new[...] = jnp.where(core == 0, here, kvback[...])
    v_new[...] = jnp.where(core == 0, kvback[...], here)
    read_cache(MINE, k_cache.at[0], keys, k_sems, lambda cp: cp.wait())

    def drain(n, _):
        for i in range(1, GROUPS):
            send(i, n).wait_send()
        return 0

    lax.fori_loop(0, NJ, drain, 0)


def first_qkv(x, wq, wk, wv, k_cache):
    return pl.pallas_call(
        first_qkv_kernel,
        out_shape=[sds((MINE, QW))] * 4 + [sds((MINE, HD))] * 2 + [VM((MINE, SEQ, HD), BF16)],
        in_specs=[ASPEC] * 5,
        out_specs=[VSPEC] * 7,
        scratch_shapes=[
            VM((ROWS, D), BF16),
            VM((NJ * NJ, D // NJ, CH), BF16),
            VM((D, HD), BF16),
            VM((ROWS, CH), F32),
            VM((ROWS, QW), BF16),
            VM((GROUPS - 1, MINE, QW), BF16),
            VM((2 * MINE, HD), BF16),
            VM((MINE, HD), BF16),
            pltpu.SemaphoreType.DMA,
            pltpu.SemaphoreType.DMA((NJ * NJ,)),
            pltpu.SemaphoreType.DMA((3,)),
            pltpu.SemaphoreType.DMA((MINE,)),
            pltpu.SemaphoreType.DMA((GROUPS - 1, NJ)),
            pltpu.SemaphoreType.DMA((GROUPS - 1, NJ)),
        ],
        compiler_params=pltpu.CompilerParams(vmem_limit_bytes=BIG, collective_id=2, has_side_effects=True),
        cost_estimate=pl.CostEstimate(flops=2 * ROWS * D * QKV, bytes_accessed=2 * D * QKV, transcendentals=0),
        name="first_qkv",
    )(x, wq, wk, wv, k_cache)


GRP = 8
TIERS = (512, 1024, 2048)


def aligned(length):
    return pl.ds(pl.multiple_of((length // 16) * 16, 16), 16)


def with_row(block, length, row):
    return jnp.where(lax.broadcasted_iota(jnp.int32, (16, HD), 0) == length % 16, row, block)


def attend_kernel(layer, n_in, *refs):
    lens, r0, r1, r2, r3, k_new, v_new = refs[:7]
    c0, c1, c2, c3, k_out, v_out, qbuf, cbuf, new_kv, patch, out_sems, patch_sems = refs[n_in:n_in + 12]
    keys = refs[7].at[pl.ds(0, MINE)]
    v_cache = refs[8]
    vbuf, v_sems = refs[n_in + 12:]
    held = V_HELD[layer]
    me = lax.axis_index("model")
    n_heads = GROUPS * LH
    scale = HD ** -0.5

    def value(b, held_group):
        return refs[7].at[MINE + b] if held_group else vbuf.at[b - held]

    def length(b):
        return lens[me * MINE + b]

    def tier_of(b, n):
        return jnp.logical_and(length(b) < TIERS[n], length(b) >= (TIERS[n - 1] if n else BLK))

    def v_read(b):
        return pltpu.make_async_copy(v_cache.at[layer, b], vbuf.at[b - held], v_sems.at[b])

    def k_write(b):
        return pltpu.make_async_copy(keys.at[b], k_out.at[layer, b], out_sems.at[0, b])

    def v_write(b, held_group):
        return pltpu.make_async_copy(value(b, held_group), v_out.at[layer, b], out_sems.at[1, b])

    def put(i, b):
        out = (k_out, v_out)[i]
        return pltpu.make_async_copy(patch.at[i, b], out.at[layer, b, aligned(length(b)), :], patch_sems.at[i, b])

    def each(do, first=0, last=MINE):
        def step(b, _):
            do(b)
            return 0
        lax.fori_loop(first, last, step, 0)

    each(lambda b: v_read(b).start(), held, MINE)
    if held:
        each(lambda b: k_write(b).start())
        each(lambda b: v_write(b, True).start(), 0, held)
    for i, r in enumerate((r0, r1, r2, r3)):
        qbuf[:, i * LH:(i + 1) * LH, :] = r[...].reshape(MINE, LH, HD)
    for b in range(MINE):
        new_kv[0, b] = k_new[b:b + 1, :].astype(F32)
        new_kv[1, b] = v_new[b:b + 1, :].astype(F32)

    def context(seqs, size, held_group):
        scores, news = [], []
        for b in seqs:
            s = lax.dot_general(qbuf[b], keys[b, 0:size, :], (((1,), (1,)), ((), ())), preferred_element_type=F32)
            pos = lax.broadcasted_iota(jnp.int32, (n_heads, size), 1)
            scores.append(jnp.where(pos < length(b), s * scale, -jnp.inf))
            news.append(jnp.sum(qbuf[b].astype(F32) * new_kv[0, b], axis=1, keepdims=True) * scale)
        tops = [jnp.maximum(jnp.max(s, axis=1, keepdims=True), n) for s, n in zip(scores, news)]
        expos = [jnp.exp(s - t) for s, t in zip(scores, tops)]
        news = [jnp.exp(n - t) for n, t in zip(news, tops)]
        invs = [1.0 / (jnp.sum(e, axis=1, keepdims=True) + n) for e, n in zip(expos, news)]
        probs = [(e * i).astype(BF16) for e, i in zip(expos, invs)]
        news = [(n * i).astype(BF16).astype(F32) for n, i in zip(news, invs)]
        for b, p, n in zip(seqs, probs, news):
            old = jnp.dot(p, value(b, held_group)[0:size, :], preferred_element_type=F32)
            cbuf[b] = (old + n * new_kv[1, b]).astype(BF16)

    def settle_keys(b):
        k_write(b).wait()
        put(0, b).start()

    def settle_values(b):
        v_write(b, True).wait()
        put(1, b).start()

    def group(g, held_group):
        seqs = [g * GRP + i for i in range(GRP)]
        for b in seqs:
            rows = aligned(length(b))
            patch[0, b] = with_row(keys[b, rows, :], length(b), new_kv[0, b].astype(BF16))
            if held_group:
                patch[1, b] = with_row(value(b, True)[rows, :], length(b), new_kv[1, b].astype(BF16))
            else:
                v_read(b).wait()
                value(b, False)[rows, :] = with_row(value(b, False)[rows, :], length(b), new_kv[1, b].astype(BF16))
        if not held_group:
            for b in seqs:
                v_write(b, False).start()
        if not held:
            for b in seqs:
                k_write(b).start()
        context(seqs, BLK, held_group)
        if g == MINE // GRP - 1 and held:
            each(settle_keys)
            each(settle_values, 0, held)

        def long_one(b, _):
            for n, size in enumerate(TIERS):
                @pl.when(tier_of(b, n))
                def _(size=size):
                    context((b,), size, held_group)
            return 0

        lax.fori_loop(g * GRP, (g + 1) * GRP, long_one, 0)

    for g in range(MINE // GRP):
        group(g, g < held // GRP)
    if not held:
        each(settle_keys)
    for i, c in enumerate((c0, c1, c2, c3)):
        c[...] = cbuf[:, i * LH:(i + 1) * LH, :].reshape(MINE, QW)
    each(lambda b: v_write(b, False).wait(), held, MINE)
    each(lambda b: put(0, b).wait())
    if held:
        each(lambda b: put(1, b).wait(), 0, held)


def attend(layer, lens, rs, k_new, v_new, held, rest):
    args = [lens, *rs, k_new, v_new, held, *rest]
    return pl.pallas_call(
        functools.partial(attend_kernel, layer, len(args)),
        out_shape=[sds((MINE, QW))] * 4 + [sds((2, MINE, SEQ, HD))] * 2,
        in_specs=[SSPEC] + [VSPEC] * 7 + [ASPEC] * len(rest),
        out_specs=[VSPEC] * 4 + [ASPEC] * 2,
        input_output_aliases={9: 4, 10: 5} if layer else {},
        scratch_shapes=[
            VM((MINE, GROUPS * LH, HD), BF16),
            VM((MINE, GROUPS * LH, HD), BF16),
            VM((2, MINE, 1, HD), F32),
            VM((2, MINE, 16, HD), BF16),
            pltpu.SemaphoreType.DMA((2, MINE)),
            pltpu.SemaphoreType.DMA((2, MINE)),
            VM((MINE - V_HELD[layer], SEQ, HD), BF16),
            pltpu.SemaphoreType.DMA((MINE,)),
        ],
        compiler_params=pltpu.CompilerParams(vmem_limit_bytes=36 * MIB if layer else BIG),
        cost_estimate=pl.CostEstimate(flops=5_000_000_000, bytes_accessed=24 * MIB, transcendentals=0),
        name=f"attend_{layer}",
    )(*args)


def out_kernel(layer, fuse, *refs):
    c_refs, (res, wo), refs = refs[:4], refs[4:6], refs[6:]
    if fuse:
        (wq, wk, wv, k_cache, v_cache), outs, refs = refs[:5], refs[5:13], refs[13:]
        r_outs, (k_new, v_new, res_out, held) = outs[:4], outs[4:]
        hid, qbuf, acc, q_all, rbuf, q_sems, kv_sems = refs[:7]
        refs = refs[7:]
    else:
        hid, refs = refs[0], refs[1:]
    ctx, resv, wbuf, send_a, recv_a, send_c, recv_c, send_b, recv_b, own, w_sems, res_sem, ssems, rsems = refs

    me = lax.axis_index("model")
    n_wo = WO_SLOTS[layer]
    partner, cross, diag = xor_id(me, 1), xor_id(me, 2), xor_id(me, 3)

    def cols(chunk):
        return pl.ds(pl.multiple_of(chunk * CH, CH), CH)

    def wo_copy(step):
        chip_of = lax.rem(lax.div(me, 2) + 1 - step // (2 * NJ), 2)
        core_of = lax.rem(lax.rem(me, 2) + 1 - step % 2, 2)
        chunk = (chip_of * 2 + core_of) * NJ + step % (2 * NJ) // 2
        slot = step % n_wo
        return pltpu.make_async_copy(wo.at[layer, :, cols(chunk)], wbuf.at[slot], w_sems.at[slot])

    def q_copies(slot):
        chip_of = lax.rem(lax.div(me, 2) + slot // (2 * NJ), 2)
        core_of = lax.rem(lax.rem(me, 2) + slot % 2, 2)
        chunk = (chip_of * 2 + core_of) * NJ + slot % (2 * NJ) // 2
        return qkv_copies(layer + 1, chunk, slot % Q_SLOTS, wq, wk, wv, qbuf, q_sems)

    def start_q(slot):
        for cp in q_copies(slot):
            cp.start()

    def send(kind, j, src, dst, dev):
        return pltpu.make_async_remote_copy(
            src_ref=src, dst_ref=dst, send_sem=ssems.at[kind, j], recv_sem=rsems.at[kind, j],
            device_id={"model": dev}, device_id_type=pl.DeviceIdType.MESH)

    half = ROWS // 2

    def rows_of(h):
        return pl.ds(pl.multiple_of(lax.rem(lax.div(me, 2) + h, 2) * half, half), half)

    def context(i):
        there = ctx.at[pl.ds(pl.multiple_of(me * MINE, MINE), MINE), :]
        return send(6, i, c_refs[i], there, xor_id(me, i))

    def pair_a(t):
        part = (t % NJ, rows_of(t // NJ))
        return send(0, t, send_a.at[part], recv_a.at[part], partner)

    def pair_b(j):
        return send(1, j, send_b.at[j], recv_b.at[j], partner)

    def across(t):
        part = (t % NJ, rows_of(t // NJ))
        return send(2, t, send_c.at[part], recv_c.at[part], cross)

    def across_here(t):
        part = (t % NJ, rows_of(1 - t // NJ))
        return send(2, t, send_c.at[part], recv_c.at[part], cross)

    def hidden(kind, j, owner, dev):
        part = hid.at[:, cols(owner * NJ + j)]
        return send(kind, j, part, part, dev)

    def last_half(kind, p, owner, dev):
        part = hid.at[:, pl.ds(pl.multiple_of(owner * QW + QW - CH + p * (CH // 2), CH // 2), CH // 2)]
        return send(kind, NJ - 1 + p, part, part, dev)

    def start_wo(step, _):
        wo_copy(step).start()
        return 0

    lax.fori_loop(0, n_wo, start_wo, 0)
    if fuse:
        res_copy = pltpu.make_async_copy(
            res.at[:, pl.ds(pl.multiple_of(me * QW, QW), QW)], resv, res_sem)
    else:
        res_copy = pltpu.make_async_copy(res, resv, res_sem)
    res_copy.start()

    ctx[pl.ds(pl.multiple_of(me * MINE, MINE), MINE), :] = c_refs[0][...]
    if fuse:
        acc[...] = jnp.zeros_like(acc)
        for slot in range(Q_FIRST):
            start_q(slot)

    barrier = pltpu.get_barrier_semaphore()
    for i in range(1, GROUPS):
        pl.semaphore_signal(barrier, inc=1, device_id={"model": xor_id(me, i)}, device_id_type=pl.DeviceIdType.MESH)
    pl.semaphore_wait(barrier, GROUPS - 1)
    for i in (1, 2, 3):
        context(i).start()

    def part_sum(step):
        wo_copy(step).wait()
        part = jnp.dot(ctx[...], wbuf[step % n_wo], preferred_element_type=F32)
        return part

    def refill(step):
        if n_wo < 4 * NJ:
            @pl.when(step + n_wo < 4 * NJ)
            def _():
                wo_copy(step + n_wo).start()
        if fuse:
            slot = step - 2 * NJ + Q_FIRST

            @pl.when(jnp.logical_and(step >= 2 * NJ, slot < Q_SLOTS))
            def _():
                start_q(slot)

    def send_across(t):
        part = (t % NJ, rows_of(t // NJ))
        pair_a(t).wait_recv()
        send_c[part] += recv_a[part]
        across(t).start()

    def half_sum(step, h):
        @pl.when(h == 0)
        def _():
            wo_copy(step).wait()
        return jnp.dot(ctx[rows_of(h), :], wbuf[step], preferred_element_type=F32)

    context(1).wait_recv()

    def phase_a(t, _):
        h, j = t // NJ, t % NJ

        @pl.when(t == NJ)
        def _():
            context(2).wait_recv()
            context(3).wait_recv()
        send_a[j, rows_of(h), :] = half_sum(2 * j, h)
        pair_a(t).start()

        @pl.when(t > 0)
        def _():
            send_across(t - 1)
        send_c[j, rows_of(h), :] = half_sum(2 * j + 1, h)

        @pl.when(h == 1)
        def _():
            refill(2 * j)
            refill(2 * j + 1)
        return 0

    lax.fori_loop(0, 2 * NJ, phase_a, 0)
    send_across(2 * NJ - 1)

    def phase_b(j, _):
        step = 2 * NJ + 2 * j
        send_b[j] = part_sum(step)
        pair_b(j).start()
        refill(step)
        own[j] = part_sum(step + 1)
        refill(step + 1)
        return 0

    lax.fori_loop(0, NJ, phase_b, 0)
    res_copy.wait()

    def next_q(owner, j, slot):
        if fuse:
            chunk = owner * NJ + j
            for cp in q_copies(slot):
                cp.wait()

            acc[...] += jnp.dot(hid[:, cols(chunk)], qbuf[slot % Q_SLOTS], preferred_element_type=F32)

            @pl.when(slot + Q_SLOTS < 4 * NJ)
            def _():
                start_q(slot + Q_SLOTS)

    def from_partner(j):
        hidden(3, j, partner, partner).wait_recv()
        next_q(partner, j, 2 * j + 1)

    def phase_c(j, _):
        pair_b(j).wait_recv()
        across_here(j).wait_recv()
        across_here(j + NJ).wait_recv()
        total = own[j] + recv_b[j] + recv_c[j]
        part = (resv[:, cols(j)].astype(F32) + total).astype(BF16)
        hid[:, cols(me * NJ + j)] = part
        if fuse:
            res_out[:, cols(j)] = part
        @pl.when(j < NJ - 1)
        def _():
            hidden(4, j, me, cross).start()

        @pl.when(j == NJ - 1)
        def _():
            last_half(4, 0, me, cross).start()
            last_half(4, 1, me, cross).start()
            last_half(5, 1, me, diag).start()
        hidden(3, j, me, partner).start()
        next_q(me, j, 2 * j)

        @pl.when(j > 0)
        def _():
            from_partner(j - 1)
        return 0

    lax.fori_loop(0, NJ, phase_c, 0)
    from_partner(NJ - 1)

    def forwarded(j, last=False):
        if last:
            last_half(5, 0, diag, partner).wait_recv()
            last_half(5, 1, diag, diag).wait_recv()
        else:
            hidden(5, j, diag, partner).wait_recv()
        next_q(diag, j, 2 * NJ + 2 * j + 1)

    def next_caches(act):
        read_cache(MINE, k_cache.at[layer + 1], held, kv_sems.at[0], act)
        read_cache(V_HELD[layer + 1], v_cache.at[layer + 1], held.at[pl.ds(MINE, V_HELD[layer + 1])], kv_sems.at[1], act)

    def phase_d(j, _):
        if fuse:
            @pl.when(j == CACHES_AT)
            def _():
                next_caches(lambda cp: cp.start())
        @pl.when(j < NJ - 1)
        def _():
            hidden(4, j, cross, cross).wait_recv()
            hidden(5, j, cross, partner).start()

        @pl.when(j == NJ - 1)
        def _():
            last_half(4, 0, cross, cross).wait_recv()
            last_half(5, 0, cross, partner).start()
            last_half(4, 1, cross, cross).wait_recv()
        next_q(cross, j, 2 * NJ + 2 * j)

        @pl.when(j > 0)
        def _():
            forwarded(j - 1)
        return 0

    lax.fori_loop(0, NJ, phase_d, 0)
    forwarded(NJ - 1, last=True)

    if fuse:
        def query(i):
            dev = xor_id(me, i)
            rows = pl.ds(pl.multiple_of(dev * MINE, MINE), MINE)
            return send(6, GROUPS + i, q_all.at[rows, :], rbuf.at[i - 1], dev)

        q_all[...] = acc[:, 0:QW].astype(BF16)
        for i in (3, 2, 1):
            query(i).start()
        mine = pl.ds(pl.multiple_of(me * MINE, MINE), MINE)
        k_new[...] = acc[mine, QW:QW + HD].astype(BF16)
        v_new[...] = acc[mine, QW + HD:QKV].astype(BF16)
        r_outs[0][...] = q_all[mine, :]
        for i in (1, 2, 3):
            query(i).wait_recv()
            r_outs[i][...] = rbuf[i - 1]
        next_caches(lambda cp: cp.wait())
        for i in (1, 2, 3):
            query(i).wait_send()
    for i in (1, 2, 3):
        context(i).wait_send()

    def drain(j, _):
        for t in (j, j + NJ):
            pair_a(t).wait_send()
            across(t).wait_send()
        pair_b(j).wait_send()
        hidden(3, j, me, partner).wait_send()

        @pl.when(j < NJ - 1)
        def _():
            hidden(4, j, me, cross).wait_send()
            hidden(5, j, cross, partner).wait_send()
        return 0

    lax.fori_loop(0, NJ, drain, 0)
    last_half(4, 0, me, cross).wait_send()
    last_half(4, 1, me, cross).wait_send()
    last_half(5, 0, cross, partner).wait_send()
    last_half(5, 1, me, diag).wait_send()


def out_product(layer, fuse, cs, res, w_out, qkv_weights):
    part = (NJ, ROWS, CH)
    shared = [
        VM((ROWS, QW), BF16),
        VM((ROWS, QW), BF16),
        VM((WO_SLOTS[layer], QW, CH), BF16),
        VM(part, F32), VM(part, F32), VM(part, F32), VM(part, F32), VM(part, F32), VM(part, F32), VM(part, F32),
        pltpu.SemaphoreType.DMA((WO_SLOTS[layer],)),
        pltpu.SemaphoreType.DMA,
        pltpu.SemaphoreType.DMA((7, 2 * NJ)),
        pltpu.SemaphoreType.DMA((7, 2 * NJ)),
    ]
    flops = 2 * ROWS * QW * D
    if fuse:
        out_shape = [sds((MINE, QW))] * 4 + [sds((MINE, HD))] * 2 + [sds((ROWS, QW)), VM((MINE + V_HELD[1], SEQ, HD), BF16)]
        out_specs = [VSPEC] * 8
        extra = [
            VM((ROWS, D), BF16),
            VM((Q_SLOTS, CH, QKV), BF16),
            VM((ROWS, QKV), F32),
            VM((ROWS, QW), BF16),
            VM((GROUPS - 1, MINE, QW), BF16),
            pltpu.SemaphoreType.DMA((3, Q_SLOTS)),
            pltpu.SemaphoreType.DMA((2, MINE)),
        ]
        args = (*cs, res, w_out, *qkv_weights)
        flops += 2 * ROWS * D * QKV
    else:
        out_shape = sds((ROWS, D))
        out_specs = VSPEC
        extra = []
        args = (*cs, res, w_out)
    return pl.pallas_call(
        functools.partial(out_kernel, layer, fuse),
        out_shape=out_shape,
        in_specs=[VSPEC] * 4 + [ASPEC] * (len(args) - 4),
        out_specs=out_specs,
        scratch_shapes=extra + shared,
        compiler_params=pltpu.CompilerParams(
            vmem_limit_bytes=(39 if fuse else 44) * MIB, collective_id=layer, has_side_effects=True),
        cost_estimate=pl.CostEstimate(flops=flops, bytes_accessed=flops // ROWS, transcendentals=0),
        name=f"out_product_{layer}",
    )(*args)


def solution(mesh):
    cache_spec = P(None, ("replica", "model"), None, None)

    def device_step(x, cache_len, w_query, w_key, w_value, w_out, k_cache, v_cache):
        x, w_key, w_value = (pltpu.with_memory_space_constraint(a, pltpu.HBM) for a in (x, w_key, w_value))
        *rs, k_new, v_new, held = first_qkv(x, w_query, w_key, w_value, k_cache)
        *cs, k_out, v_out = attend(0, cache_len, rs, k_new, v_new, held, (v_cache,))
        *rs, k_new, v_new, res, held = out_product(0, True, cs, x, w_out, (w_query, w_key, w_value, k_cache, v_cache))
        *cs, k_out, v_out = attend(1, cache_len, rs, k_new, v_new, held, (v_cache, k_out, v_out))
        out = out_product(1, False, cs, res, w_out, ())
        return out, k_out, v_out

    return jax.shard_map(
        device_step,
        mesh=mesh,
        in_specs=(P("replica", None), P("replica"), P(None, None, "model"), P(), P(), P(None, "model", None), cache_spec, cache_spec),
        out_specs=(P("replica", None), cache_spec, cache_spec),
        check_vma=False,
    )
```

```python
import functools

import jax
import jax.numpy as jnp
from jax import lax
from jax.experimental import pallas as pl
from jax.experimental.pallas import tpu as pltpu
from jax.sharding import PartitionSpec as P

F32 = jnp.float32
BF16 = jnp.bfloat16
MIB = 1 << 20
BIG = 42 * MIB

GROUPS = 4
ROWS = 64
MINE = 16
D = 8192
HD = 128
LH = 16
QW = LH * HD
SEQ = 2048
CH = 512
NJ = QW // CH
QKV = QW + 2 * HD
WO_SLOTS = (8, 16)
Q_SLOTS = 6
AHEAD = 4
Q_FIRST = 4
KEYS_AT = 14
V_HELD = (0, 8)
CACHES_AT = 2
BLK = 256
VM = pltpu.VMEM
VSPEC = pl.BlockSpec(memory_space=pltpu.VMEM)
ASPEC = pl.BlockSpec(memory_space=pltpu.HBM)
SSPEC = pl.BlockSpec(memory_space=pltpu.SMEM)


def sds(shape, dtype=BF16):
    return jax.ShapeDtypeStruct(shape, dtype)


def qkv_copies(layer, chunk, slot, wq, wk, wv, buf, sems):
    rows = pl.ds(pl.multiple_of(chunk * CH, CH), CH)
    return (
        pltpu.make_async_copy(wq.at[layer, rows, :], buf.at[slot, :, pl.ds(0, QW)], sems.at[0, slot]),
        pltpu.make_async_copy(wk.at[layer, rows, :], buf.at[slot, :, pl.ds(QW, HD)], sems.at[1, slot]),
        pltpu.make_async_copy(wv.at[layer, rows, :], buf.at[slot, :, pl.ds(QW + HD, HD)], sems.at[2, slot]),
    )


def xor_id(me, i):
    core = lax.rem(me, 2)
    other = me
    if i & 1:
        other = other + 1 - 2 * core
    if i & 2:
        other = lax.rem(other + 2, GROUPS)
    return other


def read_cache(count, cache, held, sems, act):
    for b in range(count):
        act(pltpu.make_async_copy(cache.at[b], held.at[b], sems.at[b]))


def first_qkv_kernel(x, wq, wk, wv, k_cache, r0, r1, r2, r3, k_new, v_new, keys,
                     xbuf, wbuf, kvbuf, acc, qbuf, rbuf, kvrows, kvback, x_sem, w_sems, kv_sems, k_sems, ssems, rsems):
    me = lax.axis_index("model")
    depth = D // NJ

    def cols(n):
        return pl.ds(pl.multiple_of(n * CH, CH), CH)

    def w_copy(step):
        rows = pl.ds(pl.multiple_of(step % NJ * depth, depth), depth)
        return pltpu.make_async_copy(wq.at[0, rows, cols(step // NJ)], wbuf.at[step], w_sems.at[step])

    def send(i, n):
        dev = xor_id(me, i)
        rows = pl.ds(pl.multiple_of(dev * MINE, MINE), MINE)
        return pltpu.make_async_remote_copy(
            src_ref=qbuf.at[rows, cols(n)], dst_ref=rbuf.at[i - 1, :, cols(n)],
            send_sem=ssems.at[i - 1, n], recv_sem=rsems.at[i - 1, n],
            device_id={"model": dev}, device_id_type=pl.DeviceIdType.MESH)

    x_copy = pltpu.make_async_copy(x, xbuf, x_sem)
    x_copy.start()
    core = lax.rem(me, 2)

    def kv_weight(act):
        for i, w in enumerate((wk, wv)):
            @pl.when(core == i)
            def _(w=w):
                act(pltpu.make_async_copy(w.at[0], kvbuf, kv_sems.at[0]))

    def kv_send():
        rows = pl.ds(pl.multiple_of((1 - core) * MINE, MINE), MINE)
        return pltpu.make_async_remote_copy(
            src_ref=kvrows.at[rows, :], dst_ref=kvback, send_sem=kv_sems.at[1], recv_sem=kv_sems.at[2],
            device_id={"model": xor_id(me, 1)}, device_id_type=pl.DeviceIdType.MESH)


    def start(step, _):
        w_copy(step).start()
        return 0

    lax.fori_loop(0, AHEAD, start, 0)

    barrier = pltpu.get_barrier_semaphore()
    for i in range(1, GROUPS):
        pl.semaphore_signal(barrier, inc=1, device_id={"model": xor_id(me, i)}, device_id_type=pl.DeviceIdType.MESH)
    x_copy.wait()

    def group(n):
        acc[...] = jnp.zeros_like(acc)

        def step(k, _):
            w_copy(n * NJ + k).wait()

            @pl.when(n * NJ + k + AHEAD < NJ * NJ)
            def _():
                w_copy(n * NJ + k + AHEAD).start()

            @pl.when(n * NJ + k == KEYS_AT)
            def _():
                read_cache(MINE, k_cache.at[0], keys, k_sems, lambda cp: cp.start())
            part = xbuf[:, pl.ds(pl.multiple_of(k * depth, depth), depth)]
            acc[...] += jnp.dot(part, wbuf[n * NJ + k], preferred_element_type=F32)
            return 0

        lax.fori_loop(0, NJ, step, 0)
        qbuf[:, cols(n)] = acc[...].astype(BF16)

    def leave(n):
        for i in (2, 3, 1):
            send(i, n).start()

    group(0)
    pl.semaphore_wait(barrier, GROUPS - 1)
    leave(0)

    def later(n, _):
        @pl.when(n == NJ - 1)
        def _():
            kv_weight(lambda cp: cp.start())
        group(n)
        leave(n)
        return 0

    lax.fori_loop(1, NJ, later, 0)
    mine = pl.ds(pl.multiple_of(me * MINE, MINE), MINE)
    kv_weight(lambda cp: cp.wait())
    chip_rows = pl.ds(pl.multiple_of(lax.div(me, 2) * 2 * MINE, 2 * MINE), 2 * MINE)
    kv = jnp.zeros((2 * MINE, HD), F32)
    for k in range(NJ):
        kv += jnp.dot(xbuf[chip_rows, k * depth:(k + 1) * depth], kvbuf[k * depth:(k + 1) * depth, :], preferred_element_type=F32)
    kvrows[...] = kv.astype(BF16)
    kv_send().start()
    r0[...] = qbuf[mine, :]
    for i, r in ((1, r1), (2, r2), (3, r3)):
        for n in range(NJ):
            send(i, n).wait_recv()
        r[...] = rbuf[i - 1]
    kv_send().wait()
    here = kvrows[pl.ds(pl.multiple_of(core * MINE, MINE), MINE), :]
    k_new[...] = jnp.where(core == 0, here, kvback[...])
    v_new[...] = jnp.where(core == 0, kvback[...], here)
    read_cache(MINE, k_cache.at[0], keys, k_sems, lambda cp: cp.wait())

    def drain(n, _):
        for i in range(1, GROUPS):
            send(i, n).wait_send()
        return 0

    lax.fori_loop(0, NJ, drain, 0)


def first_qkv(x, wq, wk, wv, k_cache):
    return pl.pallas_call(
        first_qkv_kernel,
        out_shape=[sds((MINE, QW))] * 4 + [sds((MINE, HD))] * 2 + [VM((MINE, SEQ, HD), BF16)],
        in_specs=[ASPEC] * 5,
        out_specs=[VSPEC] * 7,
        scratch_shapes=[
            VM((ROWS, D), BF16),
            VM((NJ * NJ, D // NJ, CH), BF16),
            VM((D, HD), BF16),
            VM((ROWS, CH), F32),
            VM((ROWS, QW), BF16),
            VM((GROUPS - 1, MINE, QW), BF16),
            VM((2 * MINE, HD), BF16),
            VM((MINE, HD), BF16),
            pltpu.SemaphoreType.DMA,
            pltpu.SemaphoreType.DMA((NJ * NJ,)),
            pltpu.SemaphoreType.DMA((3,)),
            pltpu.SemaphoreType.DMA((MINE,)),
            pltpu.SemaphoreType.DMA((GROUPS - 1, NJ)),
            pltpu.SemaphoreType.DMA((GROUPS - 1, NJ)),
        ],
        compiler_params=pltpu.CompilerParams(vmem_limit_bytes=BIG, collective_id=2, has_side_effects=True),
        cost_estimate=pl.CostEstimate(flops=2 * ROWS * D * QKV, bytes_accessed=2 * D * QKV, transcendentals=0),
        name="first_qkv",
    )(x, wq, wk, wv, k_cache)


GRP = 8
TIERS = (512, 1024, 2048)


def aligned(length):
    return pl.ds(pl.multiple_of((length // 16) * 16, 16), 16)


def with_row(block, length, row):
    return jnp.where(lax.broadcasted_iota(jnp.int32, (16, HD), 0) == length % 16, row, block)


def attend_kernel(layer, n_in, *refs):
    lens, r0, r1, r2, r3, k_new, v_new = refs[:7]
    c0, c1, c2, c3, k_out, v_out, qbuf, cbuf, new_kv, patch, out_sems, patch_sems = refs[n_in:n_in + 12]
    keys = refs[7].at[pl.ds(0, MINE)]
    v_cache = refs[8]
    vbuf, v_sems = refs[n_in + 12:]
    held = V_HELD[layer]
    me = lax.axis_index("model")
    n_heads = GROUPS * LH
    scale = HD ** -0.5

    def value(b, held_group):
        return refs[7].at[MINE + b] if held_group else vbuf.at[b - held]

    def length(b):
        return lens[me * MINE + b]

    def tier_of(b, n):
        return jnp.logical_and(length(b) < TIERS[n], length(b) >= (TIERS[n - 1] if n else BLK))

    def v_read(b):
        return pltpu.make_async_copy(v_cache.at[layer, b], vbuf.at[b - held], v_sems.at[b])

    def k_write(b):
        return pltpu.make_async_copy(keys.at[b], k_out.at[layer, b], out_sems.at[0, b])

    def v_write(b, held_group):
        return pltpu.make_async_copy(value(b, held_group), v_out.at[layer, b], out_sems.at[1, b])

    def put(i, b):
        out = (k_out, v_out)[i]
        return pltpu.make_async_copy(patch.at[i, b], out.at[layer, b, aligned(length(b)), :], patch_sems.at[i, b])

    def each(do, first=0, last=MINE):
        def step(b, _):
            do(b)
            return 0
        lax.fori_loop(first, last, step, 0)

    each(lambda b: v_read(b).start(), held, MINE)
    if held:
        each(lambda b: k_write(b).start())
        each(lambda b: v_write(b, True).start(), 0, held)
    for i, r in enumerate((r0, r1, r2, r3)):
        qbuf[:, i * LH:(i + 1) * LH, :] = r[...].reshape(MINE, LH, HD)
    for b in range(MINE):
        new_kv[0, b] = k_new[b:b + 1, :].astype(F32)
        new_kv[1, b] = v_new[b:b + 1, :].astype(F32)

    def context(seqs, size, held_group):
        scores, news = [], []
        for b in seqs:
            s = lax.dot_general(qbuf[b], keys[b, 0:size, :], (((1,), (1,)), ((), ())), preferred_element_type=F32)
            pos = lax.broadcasted_iota(jnp.int32, (n_heads, size), 1)
            scores.append(jnp.where(pos < length(b), s * scale, -jnp.inf))
            news.append(jnp.sum(qbuf[b].astype(F32) * new_kv[0, b], axis=1, keepdims=True) * scale)
        tops = [jnp.maximum(jnp.max(s, axis=1, keepdims=True), n) for s, n in zip(scores, news)]
        expos = [jnp.exp(s - t) for s, t in zip(scores, tops)]
        news = [jnp.exp(n - t) for n, t in zip(news, tops)]
        invs = [1.0 / (jnp.sum(e, axis=1, keepdims=True) + n) for e, n in zip(expos, news)]
        probs = [(e * i).astype(BF16) for e, i in zip(expos, invs)]
        news = [(n * i).astype(BF16).astype(F32) for n, i in zip(news, invs)]
        for b, p, n in zip(seqs, probs, news):
            old = jnp.dot(p, value(b, held_group)[0:size, :], preferred_element_type=F32)
            cbuf[b] = (old + n * new_kv[1, b]).astype(BF16)

    def settle_keys(b):
        k_write(b).wait()
        put(0, b).start()

    def settle_values(b):
        v_write(b, True).wait()
        put(1, b).start()

    def group(g, held_group):
        seqs = [g * GRP + i for i in range(GRP)]
        for b in seqs:
            rows = aligned(length(b))
            patch[0, b] = with_row(keys[b, rows, :], length(b), new_kv[0, b].astype(BF16))
            if held_group:
                patch[1, b] = with_row(value(b, True)[rows, :], length(b), new_kv[1, b].astype(BF16))
            else:
                v_read(b).wait()
                value(b, False)[rows, :] = with_row(value(b, False)[rows, :], length(b), new_kv[1, b].astype(BF16))
        if not held_group:
            for b in seqs:
                v_write(b, False).start()
        if not held:
            for b in seqs:
                k_write(b).start()
        context(seqs, BLK, held_group)
        if g == MINE // GRP - 1 and held:
            each(settle_keys)
            each(settle_values, 0, held)

        def long_one(b, _):
            for n, size in enumerate(TIERS):
                @pl.when(tier_of(b, n))
                def _(size=size):
                    context((b,), size, held_group)
            return 0

        lax.fori_loop(g * GRP, (g + 1) * GRP, long_one, 0)

    for g in range(MINE // GRP):
        group(g, g < held // GRP)
    if not held:
        each(settle_keys)
    for i, c in enumerate((c0, c1, c2, c3)):
        c[...] = cbuf[:, i * LH:(i + 1) * LH, :].reshape(MINE, QW)
    each(lambda b: v_write(b, False).wait(), held, MINE)
    each(lambda b: put(0, b).wait())
    if held:
        each(lambda b: put(1, b).wait(), 0, held)


def attend(layer, lens, rs, k_new, v_new, held, rest):
    args = [lens, *rs, k_new, v_new, held, *rest]
    return pl.pallas_call(
        functools.partial(attend_kernel, layer, len(args)),
        out_shape=[sds((MINE, QW))] * 4 + [sds((2, MINE, SEQ, HD))] * 2,
        in_specs=[SSPEC] + [VSPEC] * 7 + [ASPEC] * len(rest),
        out_specs=[VSPEC] * 4 + [ASPEC] * 2,
        input_output_aliases={9: 4, 10: 5} if layer else {},
        scratch_shapes=[
            VM((MINE, GROUPS * LH, HD), BF16),
            VM((MINE, GROUPS * LH, HD), BF16),
            VM((2, MINE, 1, HD), F32),
            VM((2, MINE, 16, HD), BF16),
            pltpu.SemaphoreType.DMA((2, MINE)),
            pltpu.SemaphoreType.DMA((2, MINE)),
            VM((MINE - V_HELD[layer], SEQ, HD), BF16),
            pltpu.SemaphoreType.DMA((MINE,)),
        ],
        compiler_params=pltpu.CompilerParams(vmem_limit_bytes=36 * MIB if layer else BIG),
        cost_estimate=pl.CostEstimate(flops=5_000_000_000, bytes_accessed=24 * MIB, transcendentals=0),
        name=f"attend_{layer}",
    )(*args)


def out_kernel(layer, fuse, *refs):
    c_refs, (res, wo), refs = refs[:4], refs[4:6], refs[6:]
    if fuse:
        (wq, wk, wv, k_cache, v_cache), outs, refs = refs[:5], refs[5:13], refs[13:]
        r_outs, (k_new, v_new, res_out, held) = outs[:4], outs[4:]
        hid, qbuf, acc, q_all, rbuf, q_sems, kv_sems = refs[:7]
        refs = refs[7:]
    else:
        hid, refs = refs[0], refs[1:]
    ctx, resv, wbuf, send_a, recv_a, send_c, recv_c, send_b, recv_b, own, w_sems, res_sem, ssems, rsems = refs

    me = lax.axis_index("model")
    n_wo = WO_SLOTS[layer]
    partner, cross, diag = xor_id(me, 1), xor_id(me, 2), xor_id(me, 3)

    def cols(chunk):
        return pl.ds(pl.multiple_of(chunk * CH, CH), CH)

    def wo_copy(step):
        chip_of = lax.rem(lax.div(me, 2) + 1 - step // (2 * NJ), 2)
        core_of = lax.rem(lax.rem(me, 2) + 1 - step % 2, 2)
        chunk = (chip_of * 2 + core_of) * NJ + step % (2 * NJ) // 2
        slot = step % n_wo
        return pltpu.make_async_copy(wo.at[layer, :, cols(chunk)], wbuf.at[slot], w_sems.at[slot])

    def q_copies(slot):
        chip_of = lax.rem(lax.div(me, 2) + slot // (2 * NJ), 2)
        core_of = lax.rem(lax.rem(me, 2) + slot % 2, 2)
        chunk = (chip_of * 2 + core_of) * NJ + slot % (2 * NJ) // 2
        return qkv_copies(layer + 1, chunk, slot % Q_SLOTS, wq, wk, wv, qbuf, q_sems)

    def start_q(slot):
        for cp in q_copies(slot):
            cp.start()

    def send(kind, j, src, dst, dev):
        return pltpu.make_async_remote_copy(
            src_ref=src, dst_ref=dst, send_sem=ssems.at[kind, j], recv_sem=rsems.at[kind, j],
            device_id={"model": dev}, device_id_type=pl.DeviceIdType.MESH)

    half = ROWS // 2

    def rows_of(h):
        return pl.ds(pl.multiple_of(lax.rem(lax.div(me, 2) + h, 2) * half, half), half)

    def context(i):
        there = ctx.at[pl.ds(pl.multiple_of(me * MINE, MINE), MINE), :]
        return send(6, i, c_refs[i], there, xor_id(me, i))

    def pair_a(t):
        part = (t % NJ, rows_of(t // NJ))
        return send(0, t, send_a.at[part], recv_a.at[part], partner)

    def pair_b(j):
        return send(1, j, send_b.at[j], recv_b.at[j], partner)

    def across(t):
        part = (t % NJ, rows_of(t // NJ))
        return send(2, t, send_c.at[part], recv_c.at[part], cross)

    def across_here(t):
        part = (t % NJ, rows_of(1 - t // NJ))
        return send(2, t, send_c.at[part], recv_c.at[part], cross)

    def hidden(kind, j, owner, dev):
        part = hid.at[:, cols(owner * NJ + j)]
        return send(kind, j, part, part, dev)

    def last_half(kind, p, owner, dev):
        part = hid.at[:, pl.ds(pl.multiple_of(owner * QW + QW - CH + p * (CH // 2), CH // 2), CH // 2)]
        return send(kind, NJ - 1 + p, part, part, dev)

    def start_wo(step, _):
        wo_copy(step).start()
        return 0

    lax.fori_loop(0, n_wo, start_wo, 0)
    if fuse:
        res_copy = pltpu.make_async_copy(
            res.at[:, pl.ds(pl.multiple_of(me * QW, QW), QW)], resv, res_sem)
    else:
        res_copy = pltpu.make_async_copy(res, resv, res_sem)
    res_copy.start()

    ctx[pl.ds(pl.multiple_of(me * MINE, MINE), MINE), :] = c_refs[0][...]
    if fuse:
        acc[...] = jnp.zeros_like(acc)
        for slot in range(Q_FIRST):
            start_q(slot)

    barrier = pltpu.get_barrier_semaphore()
    for i in range(1, GROUPS):
        pl.semaphore_signal(barrier, inc=1, device_id={"model": xor_id(me, i)}, device_id_type=pl.DeviceIdType.MESH)
    pl.semaphore_wait(barrier, GROUPS - 1)
    for i in (2, 3, 1):
        context(i).start()

    def part_sum(step):
        wo_copy(step).wait()
        part = jnp.dot(ctx[...], wbuf[step % n_wo], preferred_element_type=F32)
        return part

    def refill(step):
        if n_wo < 4 * NJ:
            @pl.when(step + n_wo < 4 * NJ)
            def _():
                wo_copy(step + n_wo).start()
        if fuse:
            slot = step - 2 * NJ + Q_FIRST

            @pl.when(jnp.logical_and(step >= 2 * NJ, slot < Q_SLOTS))
            def _():
                start_q(slot)

    def send_across(t):
        part = (t % NJ, rows_of(t // NJ))
        pair_a(t).wait_recv()
        send_c[part] += recv_a[part]
        across(t).start()

    def half_sum(step, h):
        @pl.when(h == 0)
        def _():
            wo_copy(step).wait()
        return jnp.dot(ctx[rows_of(h), :], wbuf[step], preferred_element_type=F32)

    context(1).wait_recv()

    def phase_a(t, _):
        h, j = t // NJ, t % NJ

        @pl.when(t == NJ)
        def _():
            context(2).wait_recv()
            context(3).wait_recv()
        send_a[j, rows_of(h), :] = half_sum(2 * j, h)
        pair_a(t).start()

        @pl.when(t > 0)
        def _():
            send_across(t - 1)
        send_c[j, rows_of(h), :] = half_sum(2 * j + 1, h)

        @pl.when(h == 1)
        def _():
            refill(2 * j)
            refill(2 * j + 1)
        return 0

    lax.fori_loop(0, 2 * NJ, phase_a, 0)
    send_across(2 * NJ - 1)

    def phase_b(j, _):
        step = 2 * NJ + 2 * j
        send_b[j] = part_sum(step)
        pair_b(j).start()
        refill(step)
        own[j] = part_sum(step + 1)
        refill(step + 1)
        return 0

    lax.fori_loop(0, NJ, phase_b, 0)
    res_copy.wait()

    def next_q(owner, j, slot):
        if fuse:
            chunk = owner * NJ + j
            for cp in q_copies(slot):
                cp.wait()

            acc[...] += jnp.dot(hid[:, cols(chunk)], qbuf[slot % Q_SLOTS], preferred_element_type=F32)

            @pl.when(slot + Q_SLOTS < 4 * NJ)
            def _():
                start_q(slot + Q_SLOTS)

    def from_partner(j):
        hidden(3, j, partner, partner).wait_recv()
        next_q(partner, j, 2 * j + 1)

    def phase_c(j, _):
        pair_b(j).wait_recv()
        across_here(j).wait_recv()
        across_here(j + NJ).wait_recv()
        total = own[j] + recv_b[j] + recv_c[j]
        part = (resv[:, cols(j)].astype(F32) + total).astype(BF16)
        hid[:, cols(me * NJ + j)] = part
        if fuse:
            res_out[:, cols(j)] = part
        @pl.when(j < NJ - 1)
        def _():
            hidden(4, j, me, cross).start()

        @pl.when(j == NJ - 1)
        def _():
            last_half(4, 0, me, cross).start()
            last_half(4, 1, me, cross).start()
            last_half(5, 1, me, diag).start()
        hidden(3, j, me, partner).start()
        next_q(me, j, 2 * j)

        @pl.when(j > 0)
        def _():
            from_partner(j - 1)
        return 0

    lax.fori_loop(0, NJ, phase_c, 0)
    from_partner(NJ - 1)

    def forwarded(j, last=False):
        if last:
            last_half(5, 0, diag, partner).wait_recv()
            last_half(5, 1, diag, diag).wait_recv()
        else:
            hidden(5, j, diag, partner).wait_recv()
        next_q(diag, j, 2 * NJ + 2 * j + 1)

    def next_caches(act):
        read_cache(MINE, k_cache.at[layer + 1], held, kv_sems.at[0], act)
        read_cache(V_HELD[layer + 1], v_cache.at[layer + 1], held.at[pl.ds(MINE, V_HELD[layer + 1])], kv_sems.at[1], act)

    def phase_d(j, _):
        if fuse:
            @pl.when(j == CACHES_AT)
            def _():
                next_caches(lambda cp: cp.start())
        @pl.when(j < NJ - 1)
        def _():
            hidden(4, j, cross, cross).wait_recv()
            hidden(5, j, cross, partner).start()

        @pl.when(j == NJ - 1)
        def _():
            last_half(4, 0, cross, cross).wait_recv()
            last_half(5, 0, cross, partner).start()
            last_half(4, 1, cross, cross).wait_recv()
        next_q(cross, j, 2 * NJ + 2 * j)

        @pl.when(j > 0)
        def _():
            forwarded(j - 1)
        return 0

    lax.fori_loop(0, NJ, phase_d, 0)
    forwarded(NJ - 1, last=True)

    if fuse:
        def query(i):
            dev = xor_id(me, i)
            rows = pl.ds(pl.multiple_of(dev * MINE, MINE), MINE)
            return send(6, GROUPS + i, q_all.at[rows, :], rbuf.at[i - 1], dev)

        q_all[...] = acc[:, 0:QW].astype(BF16)
        for i in (2, 3, 1):
            query(i).start()
        mine = pl.ds(pl.multiple_of(me * MINE, MINE), MINE)
        k_new[...] = acc[mine, QW:QW + HD].astype(BF16)
        v_new[...] = acc[mine, QW + HD:QKV].astype(BF16)
        r_outs[0][...] = q_all[mine, :]
        for i in (1, 2, 3):
            query(i).wait_recv()
            r_outs[i][...] = rbuf[i - 1]
        next_caches(lambda cp: cp.wait())
        for i in (1, 2, 3):
            query(i).wait_send()
    for i in (1, 2, 3):
        context(i).wait_send()

    def drain(j, _):
        for t in (j, j + NJ):
            pair_a(t).wait_send()
            across(t).wait_send()
        pair_b(j).wait_send()
        hidden(3, j, me, partner).wait_send()

        @pl.when(j < NJ - 1)
        def _():
            hidden(4, j, me, cross).wait_send()
            hidden(5, j, cross, partner).wait_send()
        return 0

    lax.fori_loop(0, NJ, drain, 0)
    last_half(4, 0, me, cross).wait_send()
    last_half(4, 1, me, cross).wait_send()
    last_half(5, 0, cross, partner).wait_send()
    last_half(5, 1, me, diag).wait_send()


def out_product(layer, fuse, cs, res, w_out, qkv_weights):
    part = (NJ, ROWS, CH)
    shared = [
        VM((ROWS, QW), BF16),
        VM((ROWS, QW), BF16),
        VM((WO_SLOTS[layer], QW, CH), BF16),
        VM(part, F32), VM(part, F32), VM(part, F32), VM(part, F32), VM(part, F32), VM(part, F32), VM(part, F32),
        pltpu.SemaphoreType.DMA((WO_SLOTS[layer],)),
        pltpu.SemaphoreType.DMA,
        pltpu.SemaphoreType.DMA((7, 2 * NJ)),
        pltpu.SemaphoreType.DMA((7, 2 * NJ)),
    ]
    flops = 2 * ROWS * QW * D
    if fuse:
        out_shape = [sds((MINE, QW))] * 4 + [sds((MINE, HD))] * 2 + [sds((ROWS, QW)), VM((MINE + V_HELD[1], SEQ, HD), BF16)]
        out_specs = [VSPEC] * 8
        extra = [
            VM((ROWS, D), BF16),
            VM((Q_SLOTS, CH, QKV), BF16),
            VM((ROWS, QKV), F32),
            VM((ROWS, QW), BF16),
            VM((GROUPS - 1, MINE, QW), BF16),
            pltpu.SemaphoreType.DMA((3, Q_SLOTS)),
            pltpu.SemaphoreType.DMA((2, MINE)),
        ]
        args = (*cs, res, w_out, *qkv_weights)
        flops += 2 * ROWS * D * QKV
    else:
        out_shape = sds((ROWS, D))
        out_specs = VSPEC
        extra = []
        args = (*cs, res, w_out)
    return pl.pallas_call(
        functools.partial(out_kernel, layer, fuse),
        out_shape=out_shape,
        in_specs=[VSPEC] * 4 + [ASPEC] * (len(args) - 4),
        out_specs=out_specs,
        scratch_shapes=extra + shared,
        compiler_params=pltpu.CompilerParams(
            vmem_limit_bytes=(39 if fuse else 44) * MIB, collective_id=layer, has_side_effects=True),
        cost_estimate=pl.CostEstimate(flops=flops, bytes_accessed=flops // ROWS, transcendentals=0),
        name=f"out_product_{layer}",
    )(*args)


def solution(mesh):
    cache_spec = P(None, ("replica", "model"), None, None)

    def device_step(x, cache_len, w_query, w_key, w_value, w_out, k_cache, v_cache):
        x, w_key, w_value = (pltpu.with_memory_space_constraint(a, pltpu.HBM) for a in (x, w_key, w_value))
        *rs, k_new, v_new, held = first_qkv(x, w_query, w_key, w_value, k_cache)
        *cs, k_out, v_out = attend(0, cache_len, rs, k_new, v_new, held, (v_cache,))
        *rs, k_new, v_new, res, held = out_product(0, True, cs, x, w_out, (w_query, w_key, w_value, k_cache, v_cache))
        *cs, k_out, v_out = attend(1, cache_len, rs, k_new, v_new, held, (v_cache, k_out, v_out))
        out = out_product(1, False, cs, res, w_out, ())
        return out, k_out, v_out

    return jax.shard_map(
        device_step,
        mesh=mesh,
        in_specs=(P("replica", None), P("replica"), P(None, None, "model"), P(), P(), P(None, "model", None), cache_spec, cache_spec),
        out_specs=(P("replica", None), cache_spec, cache_spec),
        check_vma=False,
    )
```

```python
import functools

import jax
import jax.numpy as jnp
from jax import lax
from jax.experimental import pallas as pl
from jax.experimental.pallas import tpu as pltpu
from jax.sharding import PartitionSpec as P

F32 = jnp.float32
BF16 = jnp.bfloat16
MIB = 1 << 20
BIG = 42 * MIB

GROUPS = 4
ROWS = 64
MINE = 16
D = 8192
HD = 128
LH = 16
QW = LH * HD
SEQ = 2048
CH = 512
NJ = QW // CH
QKV = QW + 2 * HD
WO_SLOTS = (8, 16)
Q_SLOTS = 6
AHEAD = 4
Q_FIRST = 4
KEYS_AT = 14
V_HELD = (0, 8)
CACHES_AT = 2
BLK = 256
VM = pltpu.VMEM
VSPEC = pl.BlockSpec(memory_space=pltpu.VMEM)
ASPEC = pl.BlockSpec(memory_space=pltpu.HBM)
SSPEC = pl.BlockSpec(memory_space=pltpu.SMEM)


def sds(shape, dtype=BF16):
    return jax.ShapeDtypeStruct(shape, dtype)


def qkv_copies(layer, chunk, slot, wq, wk, wv, buf, sems):
    rows = pl.ds(pl.multiple_of(chunk * CH, CH), CH)
    return (
        pltpu.make_async_copy(wq.at[layer, rows, :], buf.at[slot, :, pl.ds(0, QW)], sems.at[0, slot]),
        pltpu.make_async_copy(wk.at[layer, rows, :], buf.at[slot, :, pl.ds(QW, HD)], sems.at[1, slot]),
        pltpu.make_async_copy(wv.at[layer, rows, :], buf.at[slot, :, pl.ds(QW + HD, HD)], sems.at[2, slot]),
    )


def xor_id(me, i):
    core = lax.rem(me, 2)
    other = me
    if i & 1:
        other = other + 1 - 2 * core
    if i & 2:
        other = lax.rem(other + 2, GROUPS)
    return other


def read_cache(count, cache, held, sems, act):
    for b in range(count):
        act(pltpu.make_async_copy(cache.at[b], held.at[b], sems.at[b]))


def first_qkv_kernel(x, wq, wk, wv, k_cache, r0, r1, r2, r3, k_new, v_new, keys,
                     xbuf, wbuf, kvbuf, acc, qbuf, rbuf, kvrows, kvback, x_sem, w_sems, kv_sems, k_sems, ssems, rsems):
    me = lax.axis_index("model")
    barrier = pltpu.get_barrier_semaphore()
    for i in range(1, GROUPS):
        pl.semaphore_signal(barrier, inc=1, device_id={"model": xor_id(me, i)}, device_id_type=pl.DeviceIdType.MESH)
    depth = D // NJ

    def cols(n):
        return pl.ds(pl.multiple_of(n * CH, CH), CH)

    def w_copy(step):
        rows = pl.ds(pl.multiple_of(step % NJ * depth, depth), depth)
        return pltpu.make_async_copy(wq.at[0, rows, cols(step // NJ)], wbuf.at[step], w_sems.at[step])

    def send(i, n):
        dev = xor_id(me, i)
        rows = pl.ds(pl.multiple_of(dev * MINE, MINE), MINE)
        return pltpu.make_async_remote_copy(
            src_ref=qbuf.at[rows, cols(n)], dst_ref=rbuf.at[i - 1, :, cols(n)],
            send_sem=ssems.at[i - 1, n], recv_sem=rsems.at[i - 1, n],
            device_id={"model": dev}, device_id_type=pl.DeviceIdType.MESH)

    x_copy = pltpu.make_async_copy(x, xbuf, x_sem)
    x_copy.start()
    core = lax.rem(me, 2)

    def kv_weight(act):
        for i, w in enumerate((wk, wv)):
            @pl.when(core == i)
            def _(w=w):
                act(pltpu.make_async_copy(w.at[0], kvbuf, kv_sems.at[0]))

    def kv_send():
        rows = pl.ds(pl.multiple_of((1 - core) * MINE, MINE), MINE)
        return pltpu.make_async_remote_copy(
            src_ref=kvrows.at[rows, :], dst_ref=kvback, send_sem=kv_sems.at[1], recv_sem=kv_sems.at[2],
            device_id={"model": xor_id(me, 1)}, device_id_type=pl.DeviceIdType.MESH)


    def start(step, _):
        w_copy(step).start()
        return 0

    lax.fori_loop(0, AHEAD, start, 0)

    x_copy.wait()

    def group(n):
        acc[...] = jnp.zeros_like(acc)

        def step(k, _):
            w_copy(n * NJ + k).wait()

            @pl.when(n * NJ + k + AHEAD < NJ * NJ)
            def _():
                w_copy(n * NJ + k + AHEAD).start()

            @pl.when(n * NJ + k == KEYS_AT)
            def _():
                read_cache(MINE, k_cache.at[0], keys, k_sems, lambda cp: cp.start())
            part = xbuf[:, pl.ds(pl.multiple_of(k * depth, depth), depth)]
            acc[...] += jnp.dot(part, wbuf[n * NJ + k], preferred_element_type=F32)
            return 0

        lax.fori_loop(0, NJ, step, 0)
        qbuf[:, cols(n)] = acc[...].astype(BF16)

    def leave(n):
        for i in (2, 3, 1):
            send(i, n).start()

    group(0)
    pl.semaphore_wait(barrier, GROUPS - 1)
    leave(0)

    def later(n, _):
        @pl.when(n == NJ - 1)
        def _():
            kv_weight(lambda cp: cp.start())
        group(n)
        leave(n)
        return 0

    lax.fori_loop(1, NJ, later, 0)
    mine = pl.ds(pl.multiple_of(me * MINE, MINE), MINE)
    kv_weight(lambda cp: cp.wait())
    chip_rows = pl.ds(pl.multiple_of(lax.div(me, 2) * 2 * MINE, 2 * MINE), 2 * MINE)
    kv = jnp.zeros((2 * MINE, HD), F32)
    for k in range(NJ):
        kv += jnp.dot(xbuf[chip_rows, k * depth:(k + 1) * depth], kvbuf[k * depth:(k + 1) * depth, :], preferred_element_type=F32)
    kvrows[...] = kv.astype(BF16)
    kv_send().start()
    r0[...] = qbuf[mine, :]
    for i, r in ((1, r1), (2, r2), (3, r3)):
        for n in range(NJ):
            send(i, n).wait_recv()
        r[...] = rbuf[i - 1]
    kv_send().wait()
    here = kvrows[pl.ds(pl.multiple_of(core * MINE, MINE), MINE), :]
    k_new[...] = jnp.where(core == 0, here, kvback[...])
    v_new[...] = jnp.where(core == 0, kvback[...], here)
    read_cache(MINE, k_cache.at[0], keys, k_sems, lambda cp: cp.wait())

    def drain(n, _):
        for i in range(1, GROUPS):
            send(i, n).wait_send()
        return 0

    lax.fori_loop(0, NJ, drain, 0)


def first_qkv(x, wq, wk, wv, k_cache):
    return pl.pallas_call(
        first_qkv_kernel,
        out_shape=[sds((MINE, QW))] * 4 + [sds((MINE, HD))] * 2 + [VM((MINE, SEQ, HD), BF16)],
        in_specs=[ASPEC] * 5,
        out_specs=[VSPEC] * 7,
        scratch_shapes=[
            VM((ROWS, D), BF16),
            VM((NJ * NJ, D // NJ, CH), BF16),
            VM((D, HD), BF16),
            VM((ROWS, CH), F32),
            VM((ROWS, QW), BF16),
            VM((GROUPS - 1, MINE, QW), BF16),
            VM((2 * MINE, HD), BF16),
            VM((MINE, HD), BF16),
            pltpu.SemaphoreType.DMA,
            pltpu.SemaphoreType.DMA((NJ * NJ,)),
            pltpu.SemaphoreType.DMA((3,)),
            pltpu.SemaphoreType.DMA((MINE,)),
            pltpu.SemaphoreType.DMA((GROUPS - 1, NJ)),
            pltpu.SemaphoreType.DMA((GROUPS - 1, NJ)),
        ],
        compiler_params=pltpu.CompilerParams(vmem_limit_bytes=BIG, collective_id=2, has_side_effects=True),
        cost_estimate=pl.CostEstimate(flops=2 * ROWS * D * QKV, bytes_accessed=2 * D * QKV, transcendentals=0),
        name="first_qkv",
    )(x, wq, wk, wv, k_cache)


GRP = 8
TIERS = (512, 1024, 2048)


def aligned(length):
    return pl.ds(pl.multiple_of((length // 16) * 16, 16), 16)


def with_row(block, length, row):
    return jnp.where(lax.broadcasted_iota(jnp.int32, (16, HD), 0) == length % 16, row, block)


def attend_kernel(layer, n_in, *refs):
    lens, r0, r1, r2, r3, k_new, v_new = refs[:7]
    c0, c1, c2, c3, k_out, v_out, qbuf, cbuf, new_kv, patch, out_sems, patch_sems = refs[n_in:n_in + 12]
    keys = refs[7].at[pl.ds(0, MINE)]
    v_cache = refs[8]
    vbuf, v_sems = refs[n_in + 12:]
    held = V_HELD[layer]
    me = lax.axis_index("model")
    n_heads = GROUPS * LH
    scale = HD ** -0.5

    def value(b, held_group):
        return refs[7].at[MINE + b] if held_group else vbuf.at[b - held]

    def length(b):
        return lens[me * MINE + b]

    def tier_of(b, n):
        return jnp.logical_and(length(b) < TIERS[n], length(b) >= (TIERS[n - 1] if n else BLK))

    def v_read(b):
        return pltpu.make_async_copy(v_cache.at[layer, b], vbuf.at[b - held], v_sems.at[b])

    def k_write(b):
        return pltpu.make_async_copy(keys.at[b], k_out.at[layer, b], out_sems.at[0, b])

    def v_write(b, held_group):
        return pltpu.make_async_copy(value(b, held_group), v_out.at[layer, b], out_sems.at[1, b])

    def put(i, b):
        out = (k_out, v_out)[i]
        return pltpu.make_async_copy(patch.at[i, b], out.at[layer, b, aligned(length(b)), :], patch_sems.at[i, b])

    def each(do, first=0, last=MINE):
        def step(b, _):
            do(b)
            return 0
        lax.fori_loop(first, last, step, 0)

    each(lambda b: v_read(b).start(), held, MINE)
    if held:
        each(lambda b: k_write(b).start())
        each(lambda b: v_write(b, True).start(), 0, held)
    for i, r in enumerate((r0, r1, r2, r3)):
        qbuf[:, i * LH:(i + 1) * LH, :] = r[...].reshape(MINE, LH, HD)
    for b in range(MINE):
        new_kv[0, b] = k_new[b:b + 1, :].astype(F32)
        new_kv[1, b] = v_new[b:b + 1, :].astype(F32)

    def context(seqs, size, held_group):
        scores, news = [], []
        for b in seqs:
            s = lax.dot_general(qbuf[b], keys[b, 0:size, :], (((1,), (1,)), ((), ())), preferred_element_type=F32)
            pos = lax.broadcasted_iota(jnp.int32, (n_heads, size), 1)
            scores.append(jnp.where(pos < length(b), s * scale, -jnp.inf))
            news.append(jnp.sum(qbuf[b].astype(F32) * new_kv[0, b], axis=1, keepdims=True) * scale)
        tops = [jnp.maximum(jnp.max(s, axis=1, keepdims=True), n) for s, n in zip(scores, news)]
        expos = [jnp.exp(s - t) for s, t in zip(scores, tops)]
        news = [jnp.exp(n - t) for n, t in zip(news, tops)]
        invs = [1.0 / (jnp.sum(e, axis=1, keepdims=True) + n) for e, n in zip(expos, news)]
        probs = [(e * i).astype(BF16) for e, i in zip(expos, invs)]
        news = [(n * i).astype(BF16).astype(F32) for n, i in zip(news, invs)]
        for b, p, n in zip(seqs, probs, news):
            old = jnp.dot(p, value(b, held_group)[0:size, :], preferred_element_type=F32)
            cbuf[b] = (old + n * new_kv[1, b]).astype(BF16)

    def settle_keys(b):
        k_write(b).wait()
        put(0, b).start()

    def settle_values(b):
        v_write(b, True).wait()
        put(1, b).start()

    def group(g, held_group):
        seqs = [g * GRP + i for i in range(GRP)]
        for b in seqs:
            rows = aligned(length(b))
            patch[0, b] = with_row(keys[b, rows, :], length(b), new_kv[0, b].astype(BF16))
            if held_group:
                patch[1, b] = with_row(value(b, True)[rows, :], length(b), new_kv[1, b].astype(BF16))
            else:
                v_read(b).wait()
                value(b, False)[rows, :] = with_row(value(b, False)[rows, :], length(b), new_kv[1, b].astype(BF16))
        if not held_group:
            for b in seqs:
                v_write(b, False).start()
        if not held:
            for b in seqs:
                k_write(b).start()
        context(seqs, BLK, held_group)
        if g == MINE // GRP - 1 and held:
            each(settle_keys)
            each(settle_values, 0, held)

        def long_one(b, _):
            for n, size in enumerate(TIERS):
                @pl.when(tier_of(b, n))
                def _(size=size):
                    context((b,), size, held_group)
            return 0

        lax.fori_loop(g * GRP, (g + 1) * GRP, long_one, 0)

    for g in range(MINE // GRP):
        group(g, g < held // GRP)
    if not held:
        each(settle_keys)
    for i, c in enumerate((c0, c1, c2, c3)):
        c[...] = cbuf[:, i * LH:(i + 1) * LH, :].reshape(MINE, QW)
    each(lambda b: v_write(b, False).wait(), held, MINE)
    each(lambda b: put(0, b).wait())
    if held:
        each(lambda b: put(1, b).wait(), 0, held)


def attend(layer, lens, rs, k_new, v_new, held, rest):
    args = [lens, *rs, k_new, v_new, held, *rest]
    return pl.pallas_call(
        functools.partial(attend_kernel, layer, len(args)),
        out_shape=[sds((MINE, QW))] * 4 + [sds((2, MINE, SEQ, HD))] * 2,
        in_specs=[SSPEC] + [VSPEC] * 7 + [ASPEC] * len(rest),
        out_specs=[VSPEC] * 4 + [ASPEC] * 2,
        input_output_aliases={9: 4, 10: 5} if layer else {},
        scratch_shapes=[
            VM((MINE, GROUPS * LH, HD), BF16),
            VM((MINE, GROUPS * LH, HD), BF16),
            VM((2, MINE, 1, HD), F32),
            VM((2, MINE, 16, HD), BF16),
            pltpu.SemaphoreType.DMA((2, MINE)),
            pltpu.SemaphoreType.DMA((2, MINE)),
            VM((MINE - V_HELD[layer], SEQ, HD), BF16),
            pltpu.SemaphoreType.DMA((MINE,)),
        ],
        compiler_params=pltpu.CompilerParams(vmem_limit_bytes=36 * MIB if layer else BIG),
        cost_estimate=pl.CostEstimate(flops=5_000_000_000, bytes_accessed=24 * MIB, transcendentals=0),
        name=f"attend_{layer}",
    )(*args)


def out_kernel(layer, fuse, *refs):
    c_refs, (res, wo), refs = refs[:4], refs[4:6], refs[6:]
    if fuse:
        (wq, wk, wv, k_cache, v_cache), outs, refs = refs[:5], refs[5:13], refs[13:]
        r_outs, (k_new, v_new, res_out, held) = outs[:4], outs[4:]
        hid, qbuf, acc, q_all, rbuf, q_sems, kv_sems = refs[:7]
        refs = refs[7:]
    else:
        hid, refs = refs[0], refs[1:]
    ctx, resv, wbuf, send_a, recv_a, send_c, recv_c, send_b, recv_b, own, w_sems, res_sem, ssems, rsems = refs

    me = lax.axis_index("model")
    barrier = pltpu.get_barrier_semaphore()
    for i in range(1, GROUPS):
        pl.semaphore_signal(barrier, inc=1, device_id={"model": xor_id(me, i)}, device_id_type=pl.DeviceIdType.MESH)
    n_wo = WO_SLOTS[layer]
    partner, cross, diag = xor_id(me, 1), xor_id(me, 2), xor_id(me, 3)

    def cols(chunk):
        return pl.ds(pl.multiple_of(chunk * CH, CH), CH)

    def wo_copy(step):
        chip_of = lax.rem(lax.div(me, 2) + 1 - step // (2 * NJ), 2)
        core_of = lax.rem(lax.rem(me, 2) + 1 - step % 2, 2)
        chunk = (chip_of * 2 + core_of) * NJ + step % (2 * NJ) // 2
        slot = step % n_wo
        return pltpu.make_async_copy(wo.at[layer, :, cols(chunk)], wbuf.at[slot], w_sems.at[slot])

    def q_copies(slot):
        chip_of = lax.rem(lax.div(me, 2) + slot // (2 * NJ), 2)
        core_of = lax.rem(lax.rem(me, 2) + slot % 2, 2)
        chunk = (chip_of * 2 + core_of) * NJ + slot % (2 * NJ) // 2
        return qkv_copies(layer + 1, chunk, slot % Q_SLOTS, wq, wk, wv, qbuf, q_sems)

    def start_q(slot):
        for cp in q_copies(slot):
            cp.start()

    def send(kind, j, src, dst, dev):
        return pltpu.make_async_remote_copy(
            src_ref=src, dst_ref=dst, send_sem=ssems.at[kind, j], recv_sem=rsems.at[kind, j],
            device_id={"model": dev}, device_id_type=pl.DeviceIdType.MESH)

    half = ROWS // 2

    def rows_of(h):
        return pl.ds(pl.multiple_of(lax.rem(lax.div(me, 2) + h, 2) * half, half), half)

    def context(i):
        there = ctx.at[pl.ds(pl.multiple_of(me * MINE, MINE), MINE), :]
        return send(6, i, c_refs[i], there, xor_id(me, i))

    def pair_a(t):
        part = (t % NJ, rows_of(t // NJ))
        return send(0, t, send_a.at[part], recv_a.at[part], partner)

    def pair_b(j):
        return send(1, j, send_b.at[j], recv_b.at[j], partner)

    def across(t):
        part = (t % NJ, rows_of(t // NJ))
        return send(2, t, send_c.at[part], recv_c.at[part], cross)

    def across_here(t):
        part = (t % NJ, rows_of(1 - t // NJ))
        return send(2, t, send_c.at[part], recv_c.at[part], cross)

    def hidden(kind, j, owner, dev):
        part = hid.at[:, cols(owner * NJ + j)]
        return send(kind, j, part, part, dev)

    def last_half(kind, p, owner, dev):
        part = hid.at[:, pl.ds(pl.multiple_of(owner * QW + QW - CH + p * (CH // 2), CH // 2), CH // 2)]
        return send(kind, NJ - 1 + p, part, part, dev)

    def start_wo(step, _):
        wo_copy(step).start()
        return 0

    lax.fori_loop(0, n_wo, start_wo, 0)
    if fuse:
        res_copy = pltpu.make_async_copy(
            res.at[:, pl.ds(pl.multiple_of(me * QW, QW), QW)], resv, res_sem)
    else:
        res_copy = pltpu.make_async_copy(res, resv, res_sem)
    res_copy.start()

    ctx[pl.ds(pl.multiple_of(me * MINE, MINE), MINE), :] = c_refs[0][...]
    if fuse:
        for slot in range(Q_FIRST):
            start_q(slot)

    pl.semaphore_wait(barrier, GROUPS - 1)
    for i in (2, 3, 1):
        context(i).start()
    if fuse:
        acc[...] = jnp.zeros_like(acc)

    def part_sum(step):
        wo_copy(step).wait()
        part = jnp.dot(ctx[...], wbuf[step % n_wo], preferred_element_type=F32)
        return part

    def refill(step):
        if n_wo < 4 * NJ:
            @pl.when(step + n_wo < 4 * NJ)
            def _():
                wo_copy(step + n_wo).start()
        if fuse:
            slot = step - 2 * NJ + Q_FIRST

            @pl.when(jnp.logical_and(step >= 2 * NJ, slot < Q_SLOTS))
            def _():
                start_q(slot)

    def send_across(t):
        part = (t % NJ, rows_of(t // NJ))
        pair_a(t).wait_recv()
        send_c[part] += recv_a[part]
        across(t).start()

    def half_sum(step, h):
        @pl.when(h == 0)
        def _():
            wo_copy(step).wait()
        return jnp.dot(ctx[rows_of(h), :], wbuf[step], preferred_element_type=F32)

    context(1).wait_recv()

    def phase_a(t, _):
        h, j = t // NJ, t % NJ

        @pl.when(t == NJ)
        def _():
            context(2).wait_recv()
            context(3).wait_recv()
        send_a[j, rows_of(h), :] = half_sum(2 * j, h)
        pair_a(t).start()

        @pl.when(t > 0)
        def _():
            send_across(t - 1)
        send_c[j, rows_of(h), :] = half_sum(2 * j + 1, h)

        @pl.when(h == 1)
        def _():
            refill(2 * j)
            refill(2 * j + 1)
        return 0

    lax.fori_loop(0, 2 * NJ, phase_a, 0)
    send_across(2 * NJ - 1)

    def phase_b(j, _):
        step = 2 * NJ + 2 * j
        send_b[j] = part_sum(step)
        pair_b(j).start()
        refill(step)
        own[j] = part_sum(step + 1)
        refill(step + 1)
        return 0

    lax.fori_loop(0, NJ, phase_b, 0)
    res_copy.wait()

    def next_q(owner, j, slot):
        if fuse:
            chunk = owner * NJ + j
            for cp in q_copies(slot):
                cp.wait()

            acc[...] += jnp.dot(hid[:, cols(chunk)], qbuf[slot % Q_SLOTS], preferred_element_type=F32)

            @pl.when(slot + Q_SLOTS < 4 * NJ)
            def _():
                start_q(slot + Q_SLOTS)

    def from_partner(j):
        hidden(3, j, partner, partner).wait_recv()
        next_q(partner, j, 2 * j + 1)

    def phase_c(j, _):
        pair_b(j).wait_recv()
        across_here(j).wait_recv()
        across_here(j + NJ).wait_recv()
        total = own[j] + recv_b[j] + recv_c[j]
        part = (resv[:, cols(j)].astype(F32) + total).astype(BF16)
        hid[:, cols(me * NJ + j)] = part
        if fuse:
            res_out[:, cols(j)] = part
        @pl.when(j < NJ - 1)
        def _():
            hidden(4, j, me, cross).start()

        @pl.when(j == NJ - 1)
        def _():
            last_half(4, 0, me, cross).start()
            last_half(4, 1, me, cross).start()
            last_half(5, 1, me, diag).start()
        hidden(3, j, me, partner).start()
        next_q(me, j, 2 * j)

        @pl.when(j > 0)
        def _():
            from_partner(j - 1)
        return 0

    lax.fori_loop(0, NJ, phase_c, 0)
    from_partner(NJ - 1)

    def forwarded(j, last=False):
        if last:
            last_half(5, 0, diag, partner).wait_recv()
            last_half(5, 1, diag, diag).wait_recv()
        else:
            hidden(5, j, diag, partner).wait_recv()
        next_q(diag, j, 2 * NJ + 2 * j + 1)

    def next_caches(act):
        read_cache(MINE, k_cache.at[layer + 1], held, kv_sems.at[0], act)
        read_cache(V_HELD[layer + 1], v_cache.at[layer + 1], held.at[pl.ds(MINE, V_HELD[layer + 1])], kv_sems.at[1], act)

    def phase_d(j, _):
        if fuse:
            @pl.when(j == CACHES_AT)
            def _():
                next_caches(lambda cp: cp.start())
        @pl.when(j < NJ - 1)
        def _():
            hidden(4, j, cross, cross).wait_recv()
            hidden(5, j, cross, partner).start()

        @pl.when(j == NJ - 1)
        def _():
            last_half(4, 0, cross, cross).wait_recv()
            last_half(5, 0, cross, partner).start()
            last_half(4, 1, cross, cross).wait_recv()
        next_q(cross, j, 2 * NJ + 2 * j)

        @pl.when(j > 0)
        def _():
            forwarded(j - 1)
        return 0

    lax.fori_loop(0, NJ, phase_d, 0)
    forwarded(NJ - 1, last=True)

    if fuse:
        def query(i):
            dev = xor_id(me, i)
            rows = pl.ds(pl.multiple_of(dev * MINE, MINE), MINE)
            return send(6, GROUPS + i, q_all.at[rows, :], rbuf.at[i - 1], dev)

        q_all[...] = acc[:, 0:QW].astype(BF16)
        for i in (2, 3, 1):
            query(i).start()
        mine = pl.ds(pl.multiple_of(me * MINE, MINE), MINE)
        k_new[...] = acc[mine, QW:QW + HD].astype(BF16)
        v_new[...] = acc[mine, QW + HD:QKV].astype(BF16)
        r_outs[0][...] = q_all[mine, :]
        for i in (1, 2, 3):
            query(i).wait_recv()
            r_outs[i][...] = rbuf[i - 1]
        next_caches(lambda cp: cp.wait())
        for i in (1, 2, 3):
            query(i).wait_send()
    for i in (1, 2, 3):
        context(i).wait_send()

    def drain(j, _):
        for t in (j, j + NJ):
            pair_a(t).wait_send()
            across(t).wait_send()
        pair_b(j).wait_send()
        hidden(3, j, me, partner).wait_send()

        @pl.when(j < NJ - 1)
        def _():
            hidden(4, j, me, cross).wait_send()
            hidden(5, j, cross, partner).wait_send()
        return 0

    lax.fori_loop(0, NJ, drain, 0)
    last_half(4, 0, me, cross).wait_send()
    last_half(4, 1, me, cross).wait_send()
    last_half(5, 0, cross, partner).wait_send()
    last_half(5, 1, me, diag).wait_send()


def out_product(layer, fuse, cs, res, w_out, qkv_weights):
    part = (NJ, ROWS, CH)
    shared = [
        VM((ROWS, QW), BF16),
        VM((ROWS, QW), BF16),
        VM((WO_SLOTS[layer], QW, CH), BF16),
        VM(part, F32), VM(part, F32), VM(part, F32), VM(part, F32), VM(part, F32), VM(part, F32), VM(part, F32),
        pltpu.SemaphoreType.DMA((WO_SLOTS[layer],)),
        pltpu.SemaphoreType.DMA,
        pltpu.SemaphoreType.DMA((7, 2 * NJ)),
        pltpu.SemaphoreType.DMA((7, 2 * NJ)),
    ]
    flops = 2 * ROWS * QW * D
    if fuse:
        out_shape = [sds((MINE, QW))] * 4 + [sds((MINE, HD))] * 2 + [sds((ROWS, QW)), VM((MINE + V_HELD[1], SEQ, HD), BF16)]
        out_specs = [VSPEC] * 8
        extra = [
            VM((ROWS, D), BF16),
            VM((Q_SLOTS, CH, QKV), BF16),
            VM((ROWS, QKV), F32),
            VM((ROWS, QW), BF16),
            VM((GROUPS - 1, MINE, QW), BF16),
            pltpu.SemaphoreType.DMA((3, Q_SLOTS)),
            pltpu.SemaphoreType.DMA((2, MINE)),
        ]
        args = (*cs, res, w_out, *qkv_weights)
        flops += 2 * ROWS * D * QKV
    else:
        out_shape = sds((ROWS, D))
        out_specs = VSPEC
        extra = []
        args = (*cs, res, w_out)
    return pl.pallas_call(
        functools.partial(out_kernel, layer, fuse),
        out_shape=out_shape,
        in_specs=[VSPEC] * 4 + [ASPEC] * (len(args) - 4),
        out_specs=out_specs,
        scratch_shapes=extra + shared,
        compiler_params=pltpu.CompilerParams(
            vmem_limit_bytes=(39 if fuse else 44) * MIB, collective_id=layer, has_side_effects=True),
        cost_estimate=pl.CostEstimate(flops=flops, bytes_accessed=flops // ROWS, transcendentals=0),
        name=f"out_product_{layer}",
    )(*args)


def solution(mesh):
    cache_spec = P(None, ("replica", "model"), None, None)

    def device_step(x, cache_len, w_query, w_key, w_value, w_out, k_cache, v_cache):
        x, w_key, w_value = (pltpu.with_memory_space_constraint(a, pltpu.HBM) for a in (x, w_key, w_value))
        *rs, k_new, v_new, held = first_qkv(x, w_query, w_key, w_value, k_cache)
        *cs, k_out, v_out = attend(0, cache_len, rs, k_new, v_new, held, (v_cache,))
        *rs, k_new, v_new, res, held = out_product(0, True, cs, x, w_out, (w_query, w_key, w_value, k_cache, v_cache))
        *cs, k_out, v_out = attend(1, cache_len, rs, k_new, v_new, held, (v_cache, k_out, v_out))
        out = out_product(1, False, cs, res, w_out, ())
        return out, k_out, v_out

    return jax.shard_map(
        device_step,
        mesh=mesh,
        in_specs=(P("replica", None), P("replica"), P(None, None, "model"), P(), P(), P(None, "model", None), cache_spec, cache_spec),
        out_specs=(P("replica", None), cache_spec, cache_spec),
        check_vma=False,
    )
```
